32 devices in a mesh: dp: 16 (over z, x, core), tensor: 2 (over y).
Axes of the slice: x: 2, y: 2, z: 4, core: 2. Of those that a mesh axis runs over, the one named last changes fastest.
Arguments:
- hidden_in: float32 [2816, 2048], P('dp'), may hold values from -6 to 6
- segment_ids: int32 [16, 176], P('dp'), may hold values from 0 to 5, never falling along the last dimension, each value on 1 to 96 neighbouring positions
- gain_attn: bfloat16 [1, 2048], P(None, 'dp'), may hold values from 0.5 to 1.5
- w_query: bfloat16 [1, 2048, 2048], P(None, 'dp', 'tensor'), may hold values from -0.125 to 0.125
- w_key: bfloat16 [1, 2048, 256], P(None, 'dp', 'tensor'), may hold values from -0.125 to 0.125
- w_value: bfloat16 [1, 2048, 256], P(None, 'dp', 'tensor'), may hold values from -0.125 to 0.125
- w_out: bfloat16 [1, 2048, 2048], P(None, 'tensor', 'dp'), may hold values from -0.4375 to 0.4375
- gain_ffn: bfloat16 [1, 2048], P(None, 'dp'), may hold values from 0.5 to 1.5
- w_gate: bfloat16 [1, 2048, 5632], P(None, 'dp', 'tensor'), may hold values from -0.125 to 0.125
- w_up: bfloat16 [1, 2048, 5632], P(None, 'dp', 'tensor'), may hold values from -0.125 to 0.125
- w_down: bfloat16 [1, 5632, 2048], P(None, 'tensor', 'dp'), may hold values from -0.078125 to 0.078125
- cotangent: float32 [2816, 2048], P('dp'), may hold values from -6 to 6
Outputs:
- hidden_out: float32 [2816, 2048], P('dp')
- grad_in: float32 [2816, 2048], P('dp')
- grad_gain_attn: float32 [1, 2048], P(None, 'dp')
- grad_w_query: float32 [1, 2048, 2048], P(None, 'dp', 'tensor')
- grad_w_key: float32 [1, 2048, 256], P(None, 'dp', 'tensor')
- grad_w_value: float32 [1, 2048, 256], P(None, 'dp', 'tensor')
- grad_w_out: float32 [1, 2048, 2048], P(None, 'tensor', 'dp')
- grad_gain_ffn: float32 [1, 2048], P(None, 'dp')
- grad_w_gate: float32 [1, 2048, 5632], P(None, 'dp', 'tensor')
- grad_w_up: float32 [1, 2048, 5632], P(None, 'dp', 'tensor')
- grad_w_down: float32 [1, 5632, 2048], P(None, 'tensor', 'dp')
The draws below stay inside these ranges and needn't reach their ends.
Inputs may be any that keep to these rules, and one draw needn't show every extreme that they name: `segment_ids`: along a row of 176 tokens the ids never fall; a segment holds 1 to 96 tokens.
All inputs are finite; a program needn't handle non-finite values.
Results may differ from the reference program's by a relative error of at most 0.014.
Values may be sent and summed in bfloat16 or wider, within the bound.
A program may use at most 256 MiB of HBM per device.

```python
import math
import jax
import jax.numpy as jnp
import numpy as np
from jax import lax

D = 2048
HQ = 32
KV = 4
HD = 64
FF = 5632
LAYERS = 1
SEQ = 176
SEGMENTS = 6
SEG_MOST = 96
ROWS_DEV = 1
ROWS = 16
TOKENS = 2816
N_DP = 16


def raised(drawn, own_key, source, target, blocks, factor):
    def block_of(position):
        return (jnp.arange(drawn.shape[position]) // (drawn.shape[position] // blocks)).reshape((-1,) + (1,) * (drawn.ndim - 1 - position))

    one_side = jax.random.permutation(own_key, blocks)[block_of(target)]
    other_side = (block_of(target) + blocks // 2) % blocks
    return jnp.where((block_of(source) == one_side) | (block_of(source) == other_side), factor * drawn, drawn)


def shard_levels(stream_key, dims, pieces, least, top_value):
    level = 1.0
    for dim, parts in pieces:
        heights = jax.random.uniform(jax.random.fold_in(jax.random.fold_in(stream_key, 6), dim), (parts,), jnp.float32, least / len(pieces), top_value / len(pieces))
        level = level * jnp.repeat(jnp.exp(heights), dims[dim] // parts).reshape((-1,) + (1,) * (len(dims) - 1 - dim))
    return level


def profile(count, total, limit, lean):
    weights = [(1 << 20) // math.isqrt(grade ** lean) + 1 for grade in range(2, count + 1)]
    spare, holding = total - limit - (count - 1), [1] * (count - 1)
    while spare > 0:
        candidates = [i for i in range(count - 1) if holding[i] < limit]
        mass, left = sum([weights[i] for i in candidates]), spare
        for i in candidates:
            extra = min(limit - holding[i], max(1, left * weights[i] // mass), spare)
            holding[i] = holding[i] + extra
            spare = spare - extra
    return np.array([limit] + holding)


def uneven_parts(own_key, count, total, reach, slope):
    if count == 2:
        one = jax.random.randint(own_key, (), max(1, total - reach), min(reach, total - 1) + 1)
        return jnp.stack([one, total - one])
    sizes = jnp.asarray(profile(count, total, reach, slope), jnp.int32)
    pairs = (count - 1) // 2
    giver, taker = sizes[1:1 + 2 * pairs:2], sizes[2:2 + 2 * pairs:2]
    slack = jnp.minimum(giver - 1, reach - taker)
    moved = jax.random.randint(jax.random.fold_in(own_key, 1), (pairs,), 0, 1 << 20) % (slack + 1)
    sizes = sizes.at[1:1 + 2 * pairs:2].set(giver - moved).at[2:2 + 2 * pairs:2].set(taker + moved)
    return sizes[jax.random.permutation(jax.random.fold_in(own_key, 2), count)]


def bell_draw(rng, extent, spread, reach, cuts=(), kind=jnp.bfloat16):
    loudness = shard_levels(rng, extent, cuts, -0.22, 0.18) if cuts else 1.0
    array = jax.random.normal(rng, extent, jnp.float32) * spread * loudness
    return jnp.minimum(jnp.maximum(array, -reach), reach).astype(kind)


def bell_draw_with(own_key, extent, spread, reach, shards, heavy, kind=jnp.bfloat16):
    entries = spread * jax.random.normal(own_key, extent, jnp.float32)
    if shards:
        entries = entries * shard_levels(own_key, extent, shards, -0.22, 0.18)
    return jnp.clip(raised(entries, jax.random.fold_in(own_key, 3), *heavy), -reach, reach).astype(kind)


def setup_inputs(seed: int = 0) -> dict:
    key_of = jax.random.split(jax.random.key(seed), 13)
    return {
        "hidden_in": bell_draw_with(key_of[0], (TOKENS, D), 1.0, 6.0, ((0, 16),), (0, 1, 16, 2.0), jnp.float32),
        "segment_ids": jax.vmap(lambda own: jnp.searchsorted(jnp.cumsum(uneven_parts(own, SEGMENTS, SEQ, SEG_MOST, 1)), jnp.arange(SEQ), side="right"))(jax.random.split(key_of[1], ROWS)).reshape((ROWS, SEQ)).astype(jnp.int32),
        "gain_attn": jnp.clip(1.0 + 0.1 * jax.random.normal(key_of[2], (LAYERS, D), jnp.float32), 0.5, 1.5).astype(jnp.bfloat16),
        "w_query": bell_draw(key_of[3], (LAYERS, D, HQ * HD), D ** -0.5, 0.125, ((1, 16), (2, 2))),
        "w_key": bell_draw(key_of[4], (LAYERS, D, KV * HD), D ** -0.5, 0.125, ((1, 16), (2, 2))),
        "w_value": bell_draw(key_of[5], (LAYERS, D, KV * HD), D ** -0.5, 0.125, ((1, 16), (2, 2))),
        "w_out": bell_draw(key_of[6], (LAYERS, HQ * HD, D), (HQ * HD // 12) ** -0.5, 0.4375, ((1, 2), (2, 16))),
        "gain_ffn": jnp.clip(1.0 + 0.1 * jax.random.normal(key_of[7], (LAYERS, D), jnp.float32), 0.5, 1.5).astype(jnp.bfloat16),
        "w_gate": bell_draw(key_of[8], (LAYERS, D, FF), D ** -0.5, 0.125, ((1, 16), (2, 2))),
        "w_up": bell_draw(key_of[9], (LAYERS, D, FF), D ** -0.5, 0.125, ((1, 16), (2, 2))),
        "w_down": bell_draw(key_of[10], (LAYERS, FF, D), FF ** -0.5, 0.078125, ((1, 2), (2, 16))),
        "cotangent": bell_draw_with(key_of[11], (TOKENS, D), 1.0, 6.0, ((0, 16),), (0, 1, 16, 2.0), jnp.float32),
    }


epsilon = 1e-05
rope_base = 10000.0
masked_score = -1e+30

def segment_positions(segment_ids):
    row_count, seq_len = segment_ids.shape
    index_grid = lax.broadcasted_iota(jnp.int32, (row_count, seq_len), 1)
    previous = jnp.concatenate([segment_ids[:, :1] - 1, segment_ids[:, :-1]], axis=1)
    starts = jnp.where(segment_ids != previous, index_grid, 0)
    return index_grid - lax.cummax(starts, axis=1)

def rope_tables(positions):
    half_dim = HD // 2
    inv_freq = rope_base ** (-(jnp.arange(half_dim, dtype=jnp.float32) * 2.0 / HD))
    angles = positions.astype(jnp.float32)[:, :, None] * inv_freq
    return (jnp.cos(angles), jnp.sin(angles))

def expand_table(table, values):
    extra_dims = values.ndim - 3
    return table.reshape(table.shape[:2] + (1,) * extra_dims + table.shape[2:])

def rotate_pairs(values, cos_t, sin_t):
    half_dim = values.shape[-1] // 2
    cos_e = expand_table(cos_t, values)
    sin_e = expand_table(sin_t, values)
    first, second = (values[..., :half_dim], values[..., half_dim:])
    return jnp.concatenate([first * cos_e - second * sin_e, second * cos_e + first * sin_e], axis=-1)

def unrotate_pairs(values, cos_t, sin_t):
    half_dim = values.shape[-1] // 2
    cos_e = expand_table(cos_t, values)
    sin_e = expand_table(sin_t, values)
    first, second = (values[..., :half_dim], values[..., half_dim:])
    return jnp.concatenate([first * cos_e + second * sin_e, second * cos_e - first * sin_e], axis=-1)

def attention_mask(segment_ids):
    seq_len = segment_ids.shape[1]
    same_seg = segment_ids[:, :, None] == segment_ids[:, None, :]
    query_pos = lax.broadcasted_iota(jnp.int32, (seq_len, seq_len), 0)
    key_pos = lax.broadcasted_iota(jnp.int32, (seq_len, seq_len), 1)
    return (same_seg & (key_pos <= query_pos))[:, None, None, :, :]

def as_wide(values):
    return values.astype(jnp.float32)

def score_block(query_heads, key_heads, allowed):
    scores = jnp.einsum('rikgd,rjkd->rkgij', as_wide(query_heads), as_wide(key_heads)) * HD ** (-0.5)
    return jnp.where(allowed, scores, masked_score)

def attend(query_heads, key_heads, value_heads, allowed):
    scores = score_block(query_heads, key_heads, allowed)
    row_max = lax.optimization_barrier(jnp.max(scores, axis=-1, keepdims=True))
    log_norm = row_max + jnp.log(lax.optimization_barrier(jnp.sum(jnp.exp(scores - row_max), axis=-1, keepdims=True)))
    attn_probs = jnp.exp(scores - log_norm).astype(jnp.bfloat16)
    context = jnp.einsum('rkgij,rjkd->rikgd', as_wide(attn_probs), as_wide(value_heads)).astype(jnp.bfloat16)
    return (context, log_norm)

def attend_back(query_heads, key_heads, value_heads, context, log_norm, grad_context, allowed):
    scores = score_block(query_heads, key_heads, allowed)
    probs_full = jnp.exp(scores - log_norm)
    probs_b = probs_full.astype(jnp.bfloat16)
    grad_v = jnp.einsum('rkgij,rikgd->rjkd', as_wide(probs_b), as_wide(grad_context))
    grad_probs = jnp.einsum('rikgd,rjkd->rkgij', as_wide(grad_context), as_wide(value_heads))
    delta = lax.optimization_barrier(jnp.sum(as_wide(grad_context) * as_wide(context), axis=-1))
    delta = jnp.transpose(delta, (0, 2, 3, 1))[..., None]
    grad_scores = (probs_full * (grad_probs - delta)).astype(jnp.bfloat16)
    grad_q = jnp.einsum('rkgij,rjkd->rikgd', as_wide(grad_scores), as_wide(key_heads)) * HD ** (-0.5)
    grad_k = jnp.einsum('rkgij,rikgd->rjkd', as_wide(grad_scores), as_wide(query_heads)) * HD ** (-0.5)
    return (grad_q, grad_k, grad_v)

def contract_rows(left, right):
    return lax.dot_general(left, right, (((0,), (0,)), ((), ())), preferred_element_type=jnp.float32)

def contract_cols(left, right):
    return lax.dot_general(left, right, (((1,), (1,)), ((), ())), preferred_element_type=jnp.float32)

def norm_backward(resid, recip, gain, grad_normed):
    scaled = grad_normed * gain.astype(jnp.float32)
    grad_gain = lax.optimization_barrier(jnp.sum(grad_normed * resid * recip, axis=0))
    grad_resid = recip * scaled - resid * (recip * recip * recip) * lax.optimization_barrier(jnp.mean(scaled * resid, axis=-1, keepdims=True))
    return (grad_gain, grad_resid)

def layer_forward(resid, weights, cos_t, sin_t, allowed):
    gain_one, w_query, w_key, w_value, w_out, gain_two, w_gate, w_up, w_down = weights
    row_count, seq_len = (cos_t.shape[0], cos_t.shape[1])
    heads_here = w_query.shape[1] // HD
    kv_here = w_key.shape[1] // HD
    group_size = heads_here // kv_here
    recip_one = lax.rsqrt(lax.optimization_barrier(jnp.mean(resid * resid, axis=-1, keepdims=True)) + epsilon)
    normed_one = (resid * recip_one * gain_one.astype(jnp.float32)).astype(jnp.bfloat16)
    query_raw = jnp.dot(normed_one, w_query, preferred_element_type=jnp.float32)
    query_heads = rotate_pairs(query_raw.reshape(row_count, seq_len, kv_here, group_size, HD), cos_t, sin_t).astype(jnp.bfloat16)
    key_raw = jnp.dot(normed_one, w_key, preferred_element_type=jnp.float32)
    key_heads = rotate_pairs(key_raw.reshape(row_count, seq_len, kv_here, HD), cos_t, sin_t).astype(jnp.bfloat16)
    value_raw = jnp.dot(normed_one, w_value, preferred_element_type=jnp.float32)
    value_heads = value_raw.reshape(row_count, seq_len, kv_here, HD).astype(jnp.bfloat16)
    context, log_norm = attend(query_heads, key_heads, value_heads, allowed)
    context_flat = context.reshape(row_count * seq_len, heads_here * HD)
    attn_sum = jnp.dot(context_flat, w_out, preferred_element_type=jnp.float32)
    middle = resid + attn_sum
    recip_two = lax.rsqrt(lax.optimization_barrier(jnp.mean(middle * middle, axis=-1, keepdims=True)) + epsilon)
    normed_two = (middle * recip_two * gain_two.astype(jnp.float32)).astype(jnp.bfloat16)
    gate = jnp.dot(normed_two, w_gate, preferred_element_type=jnp.float32)
    up_proj = jnp.dot(normed_two, w_up, preferred_element_type=jnp.float32)
    hidden_act = (jax.nn.silu(gate) * up_proj).astype(jnp.bfloat16)
    feed_out = jnp.dot(hidden_act, w_down, preferred_element_type=jnp.float32)
    kept_state = (resid, recip_one, normed_one, query_heads, key_heads, value_heads, context, log_norm, middle, recip_two, normed_two, gate, up_proj, hidden_act)
    return (middle + feed_out, kept_state)

def backward_layer(grad_resid, kept_state, weights, cos_t, sin_t, allowed):
    resid, recip_one, normed_one, query_heads, key_heads, value_heads, context, log_norm, middle, recip_two, normed_two, gate, up_proj, hidden_act = kept_state
    gain_one, w_query, w_key, w_value, w_out, gain_two, w_gate, w_up, w_down = weights
    token_count = resid.shape[0]
    grad_b = grad_resid.astype(jnp.bfloat16)
    grad_down = contract_rows(hidden_act, grad_b)
    grad_hidden = contract_cols(grad_b, w_down)
    sigma = jax.nn.sigmoid(gate)
    grad_gate_b = (grad_hidden * up_proj * sigma * (1.0 + gate * (1.0 - sigma))).astype(jnp.bfloat16)
    grad_up_b = (grad_hidden * (gate * sigma)).astype(jnp.bfloat16)
    grad_gate_w = contract_rows(normed_two, grad_gate_b)
    grad_up_w = contract_rows(normed_two, grad_up_b)
    grad_normed_two = contract_cols(grad_gate_b, w_gate) + contract_cols(grad_up_b, w_up)
    grad_gain_two, grad_mid_norm = norm_backward(middle, recip_two, gain_two, grad_normed_two)
    grad_middle = grad_resid + grad_mid_norm
    middle_b = grad_middle.astype(jnp.bfloat16)
    context_flat = context.reshape(token_count, -1)
    grad_out_w = contract_rows(context_flat, middle_b)
    grad_context = contract_cols(middle_b, w_out).astype(jnp.bfloat16).reshape(context.shape)
    grad_q, grad_k, grad_v = attend_back(query_heads, key_heads, value_heads, context, log_norm, grad_context, allowed)
    grad_q = unrotate_pairs(grad_q, cos_t, sin_t).astype(jnp.bfloat16).reshape(token_count, -1)
    grad_k = unrotate_pairs(grad_k, cos_t, sin_t).astype(jnp.bfloat16).reshape(token_count, -1)
    grad_v = grad_v.astype(jnp.bfloat16).reshape(token_count, -1)
    grad_query_w = contract_rows(normed_one, grad_q)
    grad_key_w = contract_rows(normed_one, grad_k)
    grad_value_w = contract_rows(normed_one, grad_v)
    grad_normed_one = contract_cols(grad_q, w_query) + contract_cols(grad_k, w_key) + contract_cols(grad_v, w_value)
    grad_gain_one, grad_res_norm = norm_backward(resid, recip_one, gain_one, grad_normed_one)
    grad_input = grad_middle + grad_res_norm
    layer_grads = (grad_gain_one, grad_query_w, grad_key_w, grad_value_w, grad_out_w, grad_gain_two, grad_gate_w, grad_up_w, grad_down)
    return (grad_input, layer_grads)

def reference(hidden_in, segment_ids, gain_attn, w_query, w_key, w_value, w_out, gain_ffn, w_gate, w_up, w_down, cotangent):
    group_rows = ROWS_DEV * math.gcd(N_DP, 8)
    group_count = ROWS // group_rows
    group_tokens = group_rows * SEQ
    params = (gain_attn, w_query, w_key, w_value, w_out, gain_ffn, w_gate, w_up, w_down)

    def process(totals, inputs):
        resid, segments, grad_resid = inputs
        cos_t, sin_t = rope_tables(segment_positions(segments))
        allowed = attention_mask(segments)
        states = []
        for layer_no in range(LAYERS):
            weights = tuple((weight_arr[layer_no] for weight_arr in params))
            resid, kept_state = layer_forward(resid, weights, cos_t, sin_t, allowed)
            states.append(kept_state)
        collected = [None] * LAYERS
        for layer_no in reversed(range(LAYERS)):
            weights = tuple((weight_arr[layer_no] for weight_arr in params))
            grad_resid, collected[layer_no] = backward_layer(grad_resid, states[layer_no], weights, cos_t, sin_t, allowed)
        new_totals = tuple((totals[member] + jnp.stack([collected[layer_no][member] for layer_no in range(LAYERS)]) for member in range(9)))
        return (new_totals, (resid, grad_resid))
    initial = tuple((jnp.zeros(weight_arr.shape, jnp.float32) for weight_arr in params))
    inputs = (hidden_in.reshape(group_count, group_tokens, D), segment_ids.reshape(group_count, group_rows, SEQ), cotangent.reshape(group_count, group_tokens, D))
    totals, (outputs, grads) = lax.scan(process, initial, inputs)
    return (outputs.reshape(TOKENS, D), grads.reshape(TOKENS, D), totals[0], totals[1], totals[2], totals[3], totals[4], totals[5], totals[6], totals[7], totals[8])
```

```python
import jax
import jax.numpy as jnp
from jax import lax
from jax.experimental import pallas as pl
from jax.experimental.pallas import tpu as pltpu
from jax.sharding import PartitionSpec as P

HD = 64


epsilon = 1e-05
rope_base = 10000.0
masked_score = -1e30


def segment_positions(segment_ids):
    row_count, seq_len = segment_ids.shape
    index_grid = lax.broadcasted_iota(jnp.int32, (row_count, seq_len), 1)
    previous = jnp.concatenate([segment_ids[:, :1] - 1, segment_ids[:, :-1]], axis=1)
    starts = jnp.where(segment_ids != previous, index_grid, 0)
    return index_grid - lax.cummax(starts, axis=1)


def rope_tables(positions):
    half_dim = HD // 2
    inv_freq = rope_base ** (-(jnp.arange(half_dim, dtype=jnp.float32) * 2.0 / HD))
    angles = positions.astype(jnp.float32)[:, :, None] * inv_freq
    return (jnp.cos(angles), jnp.sin(angles))


def expand_table(table, values):
    extra_dims = values.ndim - 3
    return table.reshape(table.shape[:2] + (1,) * extra_dims + table.shape[2:])


def rotate_pairs(values, cos_t, sin_t):
    half_dim = values.shape[-1] // 2
    cos_e = expand_table(cos_t, values)
    sin_e = expand_table(sin_t, values)
    first, second = (values[..., :half_dim], values[..., half_dim:])
    return jnp.concatenate(
        [first * cos_e - second * sin_e, second * cos_e + first * sin_e], axis=-1
    )


def unrotate_pairs(values, cos_t, sin_t):
    half_dim = values.shape[-1] // 2
    cos_e = expand_table(cos_t, values)
    sin_e = expand_table(sin_t, values)
    first, second = (values[..., :half_dim], values[..., half_dim:])
    return jnp.concatenate(
        [first * cos_e + second * sin_e, second * cos_e - first * sin_e], axis=-1
    )


def attention_mask(segment_ids):
    seq_len = segment_ids.shape[1]
    same_seg = segment_ids[:, :, None] == segment_ids[:, None, :]
    query_pos = lax.broadcasted_iota(jnp.int32, (seq_len, seq_len), 0)
    key_pos = lax.broadcasted_iota(jnp.int32, (seq_len, seq_len), 1)
    return (same_seg & (key_pos <= query_pos))[:, None, None, :, :]


def score_block(query_heads, key_heads, allowed):
    scores = jnp.einsum(
        "rikgd,rjkd->rkgij", query_heads, key_heads, preferred_element_type=jnp.float32
    ) * HD ** (-0.5)
    return jnp.where(allowed, scores, masked_score)


def attend(query_heads, key_heads, value_heads, allowed):
    scores = score_block(query_heads, key_heads, allowed)
    row_max = jnp.max(scores, axis=-1, keepdims=True)
    log_norm = row_max + jnp.log(jnp.sum(jnp.exp(scores - row_max), axis=-1, keepdims=True))
    attn_probs = jnp.exp(scores - log_norm).astype(jnp.bfloat16)
    context = jnp.einsum(
        "rkgij,rjkd->rikgd", attn_probs, value_heads, preferred_element_type=jnp.float32
    )
    return (context.astype(jnp.bfloat16), log_norm)


def attend_back(query_heads, key_heads, value_heads, context, log_norm, grad_context, allowed):
    scores = score_block(query_heads, key_heads, allowed)
    probs_full = jnp.exp(scores - log_norm)
    probs_b = probs_full.astype(jnp.bfloat16)
    grad_v = jnp.einsum(
        "rkgij,rikgd->rjkd", probs_b, grad_context, preferred_element_type=jnp.float32
    )
    grad_probs = jnp.einsum(
        "rikgd,rjkd->rkgij", grad_context, value_heads, preferred_element_type=jnp.float32
    )
    delta = jnp.sum(grad_context.astype(jnp.float32) * context.astype(jnp.float32), axis=-1)
    delta = jnp.transpose(delta, (0, 2, 3, 1))[..., None]
    grad_scores = (probs_full * (grad_probs - delta)).astype(jnp.bfloat16)
    grad_q = jnp.einsum(
        "rkgij,rjkd->rikgd", grad_scores, key_heads, preferred_element_type=jnp.float32
    ) * HD ** (-0.5)
    grad_k = jnp.einsum(
        "rkgij,rikgd->rjkd", grad_scores, query_heads, preferred_element_type=jnp.float32
    ) * HD ** (-0.5)
    return (grad_q, grad_k, grad_v)


def contract_rows(left, right):
    return lax.dot_general(
        left, right, (((0,), (0,)), ((), ())), preferred_element_type=jnp.float32
    )


def contract_cols(left, right):
    return lax.dot_general(
        left, right, (((1,), (1,)), ((), ())), preferred_element_type=jnp.float32
    )


def norm_backward(resid, recip, gain, grad_normed):
    scaled = grad_normed * gain.astype(jnp.float32)
    grad_gain = jnp.sum(grad_normed * resid * recip, axis=0)
    grad_resid = recip * scaled - resid * (recip * recip * recip) * jnp.mean(
        scaled * resid, axis=-1, keepdims=True
    )
    return (grad_gain, grad_resid)


def layer_forward(resid, weights, cos_t, sin_t, allowed):
    gain_one, w_query, w_key, w_value, w_out, gain_two, w_gate, w_up, w_down = weights
    row_count, seq_len = (cos_t.shape[0], cos_t.shape[1])
    heads_here = w_query.shape[1] // HD
    kv_here = w_key.shape[1] // HD
    group_size = heads_here // kv_here
    recip_one = lax.rsqrt(jnp.mean(resid * resid, axis=-1, keepdims=True) + epsilon)
    normed_one = (resid * recip_one * gain_one.astype(jnp.float32)).astype(jnp.bfloat16)
    query_raw = jnp.dot(normed_one, w_query, preferred_element_type=jnp.float32)
    query_heads = rotate_pairs(
        query_raw.reshape(row_count, seq_len, kv_here, group_size, HD), cos_t, sin_t
    ).astype(jnp.bfloat16)
    key_raw = jnp.dot(normed_one, w_key, preferred_element_type=jnp.float32)
    key_heads = rotate_pairs(key_raw.reshape(row_count, seq_len, kv_here, HD), cos_t, sin_t).astype(
        jnp.bfloat16
    )
    value_raw = jnp.dot(normed_one, w_value, preferred_element_type=jnp.float32)
    value_heads = value_raw.reshape(row_count, seq_len, kv_here, HD).astype(jnp.bfloat16)
    context, log_norm = attend(query_heads, key_heads, value_heads, allowed)
    context_flat = context.reshape(row_count * seq_len, heads_here * HD)
    attn_sum = lax.psum(jnp.dot(context_flat, w_out, preferred_element_type=jnp.float32), "tensor")
    middle = resid + attn_sum
    recip_two = lax.rsqrt(jnp.mean(middle * middle, axis=-1, keepdims=True) + epsilon)
    normed_two = (middle * recip_two * gain_two.astype(jnp.float32)).astype(jnp.bfloat16)
    gate = jnp.dot(normed_two, w_gate, preferred_element_type=jnp.float32)
    up_proj = jnp.dot(normed_two, w_up, preferred_element_type=jnp.float32)
    hidden_act = (jax.nn.silu(gate) * up_proj).astype(jnp.bfloat16)
    feed_out = lax.psum(jnp.dot(hidden_act, w_down, preferred_element_type=jnp.float32), "tensor")
    kept_state = (
        resid,
        recip_one,
        normed_one,
        query_heads,
        key_heads,
        value_heads,
        context,
        log_norm,
        middle,
        recip_two,
        normed_two,
        gate,
        up_proj,
        hidden_act,
    )
    return (middle + feed_out, kept_state)


def backward_layer(grad_resid, kept_state, weights, cos_t, sin_t, allowed):
    (
        resid,
        recip_one,
        normed_one,
        query_heads,
        key_heads,
        value_heads,
        context,
        log_norm,
        middle,
        recip_two,
        normed_two,
        gate,
        up_proj,
        hidden_act,
    ) = kept_state
    gain_one, w_query, w_key, w_value, w_out, gain_two, w_gate, w_up, w_down = weights
    token_count = resid.shape[0]
    grad_b = grad_resid.astype(jnp.bfloat16)
    grad_down = contract_rows(hidden_act, grad_b)
    grad_hidden = contract_cols(grad_b, w_down)
    sigma = jax.nn.sigmoid(gate)
    grad_gate_b = (grad_hidden * up_proj * sigma * (1.0 + gate * (1.0 - sigma))).astype(
        jnp.bfloat16
    )
    grad_up_b = (grad_hidden * (gate * sigma)).astype(jnp.bfloat16)
    grad_gate_w = contract_rows(normed_two, grad_gate_b)
    grad_up_w = contract_rows(normed_two, grad_up_b)
    grad_normed_two = lax.psum(
        contract_cols(grad_gate_b, w_gate) + contract_cols(grad_up_b, w_up), "tensor"
    )
    grad_gain_two, grad_mid_norm = norm_backward(middle, recip_two, gain_two, grad_normed_two)
    grad_middle = grad_resid + grad_mid_norm
    middle_b = grad_middle.astype(jnp.bfloat16)
    context_flat = context.reshape(token_count, -1)
    grad_out_w = contract_rows(context_flat, middle_b)
    grad_context = contract_cols(middle_b, w_out).astype(jnp.bfloat16).reshape(context.shape)
    grad_q, grad_k, grad_v = attend_back(
        query_heads, key_heads, value_heads, context, log_norm, grad_context, allowed
    )
    grad_q = unrotate_pairs(grad_q, cos_t, sin_t).astype(jnp.bfloat16).reshape(token_count, -1)
    grad_k = unrotate_pairs(grad_k, cos_t, sin_t).astype(jnp.bfloat16).reshape(token_count, -1)
    grad_v = grad_v.astype(jnp.bfloat16).reshape(token_count, -1)
    grad_query_w = contract_rows(normed_one, grad_q)
    grad_key_w = contract_rows(normed_one, grad_k)
    grad_value_w = contract_rows(normed_one, grad_v)
    grad_normed_one = lax.psum(
        contract_cols(grad_q, w_query)
        + contract_cols(grad_k, w_key)
        + contract_cols(grad_v, w_value),
        "tensor",
    )
    grad_gain_one, grad_res_norm = norm_backward(resid, recip_one, gain_one, grad_normed_one)
    grad_input = grad_middle + grad_res_norm
    layer_grads = (
        lax.psum_scatter(grad_gain_one, "dp", scatter_dimension=0, tiled=True),
        lax.psum_scatter(grad_query_w, "dp", scatter_dimension=0, tiled=True),
        lax.psum_scatter(grad_key_w, "dp", scatter_dimension=0, tiled=True),
        lax.psum_scatter(grad_value_w, "dp", scatter_dimension=0, tiled=True),
        lax.psum_scatter(grad_out_w, "dp", scatter_dimension=1, tiled=True),
        lax.psum_scatter(grad_gain_two, "dp", scatter_dimension=0, tiled=True),
        lax.psum_scatter(grad_gate_w, "dp", scatter_dimension=0, tiled=True),
        lax.psum_scatter(grad_up_w, "dp", scatter_dimension=0, tiled=True),
        lax.psum_scatter(grad_down, "dp", scatter_dimension=1, tiled=True),
    )
    return (grad_input, tuple(layer_grads))


def body(
    hidden_in,
    segment_ids,
    gain_attn,
    w_query,
    w_key,
    w_value,
    w_out,
    gain_ffn,
    w_gate,
    w_up,
    w_down,
    cotangent,
):
    cos_t, sin_t = rope_tables(segment_positions(segment_ids))
    allowed = attention_mask(segment_ids)
    layer_count = w_query.shape[0]
    resid = hidden_in
    retained = []
    layer_no = 0
    gathered = (
        lax.all_gather(gain_attn[layer_no], "dp", axis=0, tiled=True),
        lax.all_gather(w_query[layer_no], "dp", axis=0, tiled=True),
        lax.all_gather(w_key[layer_no], "dp", axis=0, tiled=True),
        lax.all_gather(w_value[layer_no], "dp", axis=0, tiled=True),
        lax.all_gather(w_out[layer_no], "dp", axis=1, tiled=True),
        lax.all_gather(gain_ffn[layer_no], "dp", axis=0, tiled=True),
        lax.all_gather(w_gate[layer_no], "dp", axis=0, tiled=True),
        lax.all_gather(w_up[layer_no], "dp", axis=0, tiled=True),
        lax.all_gather(w_down[layer_no], "dp", axis=1, tiled=True),
    )
    retained.append(gathered)
    resid, kept_state = layer_forward(resid, gathered, cos_t, sin_t, allowed)
    states = [kept_state]
    grad_resid = cotangent
    collected = [None] * layer_count
    for layer_no in reversed(range(layer_count)):
        gathered = (
            lax.all_gather(gain_attn[layer_no], "dp", axis=0, tiled=True),
            lax.all_gather(w_query[layer_no], "dp", axis=0, tiled=True),
            lax.all_gather(w_key[layer_no], "dp", axis=0, tiled=True),
            lax.all_gather(w_value[layer_no], "dp", axis=0, tiled=True),
            lax.all_gather(w_out[layer_no], "dp", axis=1, tiled=True),
            lax.all_gather(gain_ffn[layer_no], "dp", axis=0, tiled=True),
            lax.all_gather(w_gate[layer_no], "dp", axis=0, tiled=True),
            lax.all_gather(w_up[layer_no], "dp", axis=0, tiled=True),
            lax.all_gather(w_down[layer_no], "dp", axis=1, tiled=True),
        )
        grad_resid, collected[layer_no] = backward_layer(
            grad_resid, states[layer_no], gathered, cos_t, sin_t, allowed
        )
    stacked = tuple((jnp.stack([collected[0][member]]) for member in range(9)))
    return (
        resid,
        grad_resid,
        stacked[0],
        stacked[1],
        stacked[2],
        stacked[3],
        stacked[4],
        stacked[5],
        stacked[6],
        stacked[7],
        stacked[8],
    )


ZN = 4
MESH = pl.DeviceIdType.MESH
BF = jnp.bfloat16
F32 = jnp.float32
LANE = 128


def place():
    dp = lax.axis_index("dp")
    return dp // 4, (dp // 2) % 2, dp % 2, lax.axis_index("tensor")


def dev(z, x, c, y):
    return (z * 4 + x * 2 + c, y)


def rid(z, x, c):
    return (z * 2 + x) * 2 + c


def lanes(r, width=LANE):
    return pl.ds(pl.multiple_of(r * width, LANE), width)


def rows(r, height):
    return pl.ds(pl.multiple_of(r * height, 16), height)


def greet(peers):
    barrier = pltpu.get_barrier_semaphore()
    for peer in peers:
        pl.semaphore_signal(barrier, inc=1, device_id=peer, device_id_type=MESH)
    pl.semaphore_wait(barrier, len(peers))


class Wire:
    def __init__(self, send_sem, recv_sem):
        self.send_sem = send_sem
        self.recv_sem = recv_sem
        self.started = []

    def make(self, src, dst, si, ri, to):
        return pltpu.make_async_remote_copy(
            src_ref=src,
            dst_ref=dst,
            send_sem=self.send_sem.at[si],
            recv_sem=self.recv_sem.at[ri],
            device_id=to,
            device_id_type=MESH,
        )

    def send(self, src, dst, si, ri, to, cond=None):
        def go():
            self.make(src, dst, si, ri, to).start()

        def done():
            self.make(src, dst, si, ri, to).wait_send()

        if cond is None:
            go()
            self.started.append(done)
        else:
            pl.when(cond)(go)
            self.started.append(lambda: pl.when(cond)(done))

    def arrived(self, dst, ri, to, cond=None):
        def wait():
            self.make(dst, dst, 0, ri, to).wait_recv()

        if cond is None:
            wait()
        else:
            pl.when(cond)(wait)

    def drain(self):
        for done in self.started:
            done()


def all_peers(z, x, c, y):
    near = [dev(z, x, 1 - c, y), dev(z, 1 - x, c, y), dev(z, x, c, 1 - y)]
    return near + [dev((z + d) % ZN, x, c, y) for d in (1, 2, 3)]


def params(cid):
    return pltpu.CompilerParams(
        collective_id=cid, has_side_effects=True, vmem_limit_bytes=60 * 1024 * 1024
    )


def any_spec():
    return pl.BlockSpec(memory_space=pl.ANY)


def vm_spec():
    return pl.BlockSpec(memory_space=pltpu.VMEM)


def sems(n):
    return pltpu.SemaphoreType.DMA((n,))


def dot_nn(a, b):
    return lax.dot_general(a, b, (((1,), (0,)), ((), ())), preferred_element_type=F32)


def dot_nt(a, b):
    return lax.dot_general(a, b, (((1,), (1,)), ((), ())), preferred_element_type=F32)


def dot_tn(a, b):
    return lax.dot_general(a, b, (((0,), (0,)), ((), ())), preferred_element_type=F32)


def by_rows(height, step, one):
    def wrapped(i, carry):
        one(pl.ds(pl.multiple_of(i * step, step), step))
        return carry

    lax.fori_loop(0, height // step, wrapped, 0)


def swap_halves(v):
    lane = lax.broadcasted_iota(jnp.int32, v.shape, 1)
    first = (lane % HD) < (HD // 2)
    return jnp.where(first, pltpu.roll(v, LANE - HD // 2, 1), pltpu.roll(v, HD // 2, 1))


def spread_pair(dst, pair):
    lane = lax.broadcasted_iota(jnp.int32, pair.shape, 1)
    low = lane < HD
    turned = pltpu.roll(pair, HD, 1)
    zero = jnp.zeros_like(pair)
    dst[0] = jnp.where(low, pair, zero).astype(BF)
    dst[1] = jnp.where(low, zero, turned).astype(BF)
    dst[2] = jnp.where(low, turned, zero).astype(BF)
    dst[3] = jnp.where(low, zero, pair).astype(BF)


class Line:
    def __init__(self, wire, own, buf, send_base, recv_base):
        self.wire, self.own, self.buf = wire, own, buf
        self.s, self.r = send_base, recv_base
        z, x, c, y = place()
        self.z, self.y = z, y
        self.up, self.down = dev(z + 1, x, c, y), dev(z - 1, x, c, y)
        self.other = dev(z, x, c, 1 - y)
        self.seq, self.half = own.shape[0], own.shape[1] // 2

    def blk(self, o, h):
        return self.buf.at[rows(o, self.seq), lanes(h, self.half)]

    def start(self):
        z, wire = self.z, self.wire
        src = self.own.at[:, lanes(self.y, self.half)]
        dst = self.blk(z, self.y)
        wire.send(src, dst, self.s + z, self.r + z, self.up, z < ZN - 1)
        wire.send(src, dst, self.s + 4 + z, self.r + z, self.down, z > 0)

    def relay(self, s):
        z, wire = self.z, self.wire
        for o, cond, fwd, to, frm, base in (
            (z - s, z >= s, z < ZN - 1, self.up, self.down, 0),
            (z + s, z + s < ZN, z > 0, self.down, self.up, 4),
        ):
            b = self.blk(o, self.y)
            wire.arrived(b, self.r + o, frm, cond)
            wire.send(b, b, self.s + base + o, self.r + o, to, cond & fwd)
            wire.send(b, b, self.s + 8 + o, self.r + 4 + o, self.other, cond)

    def finish(self):
        for o in range(ZN):
            self.wire.arrived(self.blk(o, 1 - self.y), self.r + 4 + o, self.other, self.z != o)


class Tree:
    def __init__(self, wire, own, blk, send_base, recv_base):
        self.wire, self.own, self.blk = wire, own, blk
        self.s, self.r = send_base, recv_base
        self.z, self.x, self.c, y = place()
        z, x, c = self.z, self.x, self.c
        self.up, self.down = dev(z + 1, x, c, y), dev(z - 1, x, c, y)
        self.side, self.twin = dev(z, 1 - x, c, y), dev(z, x, 1 - c, y)

    def start(self):
        z, wire = self.z, self.wire
        d = self.blk(rid(z, self.x, self.c))
        wire.send(self.own, d, self.s + z, self.r + z, self.up, z < ZN - 1)
        wire.send(self.own, d, self.s + 4 + z, self.r + z, self.down, z > 0)
        wire.send(self.own, d, self.s + 8 + z, self.r + 4 + z, self.side)
        k = z * 2 + self.x
        wire.send(self.own, d, self.s + 12 + k, self.r + 8 + k, self.twin)

    def relay(self, s):
        z, wire = self.z, self.wire
        for o, cond, fwd, to, frm, base in (
            (z - s, z >= s, z < ZN - 1, self.up, self.down, 0),
            (z + s, z + s < ZN, z > 0, self.down, self.up, 4),
        ):
            b = self.blk(rid(o, self.x, self.c))
            wire.arrived(b, self.r + o, frm, cond)
            wire.send(b, b, self.s + base + o, self.r + o, to, cond & fwd)
            wire.send(b, b, self.s + 8 + o, self.r + 4 + o, self.side, cond)
            k = o * 2 + self.x
            wire.send(b, b, self.s + 12 + k, self.r + 8 + k, self.twin, cond)

    def across(self, s):
        z = self.z
        todo = ((z, None),) if s == 0 else ((z - s, z >= s), (z + s, z + s < ZN))
        for o, cond in todo:
            b = self.blk(rid(o, 1 - self.x, self.c))
            self.wire.arrived(b, self.r + 4 + o, self.side, cond)
            k = o * 2 + 1 - self.x
            self.wire.send(b, b, self.s + 12 + k, self.r + 8 + k, self.twin, cond)

    def finish(self):
        for o in range(ZN):
            for xx in (0, 1):
                b = self.blk(rid(o, xx, 1 - self.c))
                self.wire.arrived(b, self.r + 8 + o * 2 + xx, self.twin)


def front_kernel(
    resid, wq_l, wk_l, wv_l, wo_l, ga_l, wg_l, wu_l, wd_l, cot, cos_t, sin_t, mask,
    wqkv, wo, ga, w3, dres, n1, q, kv, ctx, mid, normed,
    qkv_l, w3_l, dres_l, kx, vx, attn, part, nrm, ss, rs, ls,
):
    z, x, c, y = place()
    units = w3.shape[1]
    seq, width = resid.shape
    q_width = q.shape[1]
    pairs = q_width // LANE
    wire = Wire(ss, rs)
    side, twin, other = dev(z, 1 - x, c, y), dev(z, x, 1 - c, y), dev(z, x, c, 1 - y)
    qkv_l[:, pl.ds(0, q_width)] = wq_l[0]
    qkv_l[:, pl.ds(q_width, LANE)] = wk_l[0]
    qkv_l[:, pl.ds(q_width + LANE, LANE)] = wv_l[0]
    greet(all_peers(z, x, c, y))

    def qkv_blk(r):
        return wqkv.at[pl.ds(pl.multiple_of(r * LANE, LANE), LANE), :]

    def wo_blk(r):
        return wo.at[:, lanes(r)]

    def ga_blk(r):
        return ga.at[:, lanes(r)]

    def ffn(r):
        return w3.at[:, :, lanes(r)]

    t_qkv = Tree(wire, qkv_l, qkv_blk, 0, 0)
    t_wo = Tree(wire, wo_l.at[0], wo_blk, 20, 16)
    t_ga = Tree(wire, ga_l, ga_blk, 40, 32)
    l_dres = Line(wire, dres_l, dres, 76, 64)
    l_norm = Line(wire, nrm, normed, 88, 72)
    mine = rid(z, x, c)
    t_ga.start()
    t_qkv.start()
    own = [
        pltpu.make_async_copy(qkv_l, qkv_blk(mine), ls.at[0]),
        pltpu.make_async_copy(wo_l.at[0], wo_blk(mine), ls.at[1]),
        pltpu.make_async_copy(ga_l, ga_blk(mine), ls.at[2]),
    ]
    for cp in own:
        cp.start()

    def round_cot(r):
        dres_l[r, :] = cot[r, :].astype(BF)

    by_rows(seq, 16, round_cot)
    for s in (1, 2, 3):
        t_ga.relay(s)
    for s in (0, 1, 2, 3):
        t_ga.across(s)
    t_qkv.relay(1)
    t_qkv.across(0)
    t_ga.finish()
    own[2].wait()
    gain_one = ga[pl.ds(0, 8), :].astype(F32)[0:1]
    gain_two = ga[pl.ds(0, 8), :].astype(F32)[1:2]

    def norm_one(r):
        v = resid[r, :]
        recip = lax.rsqrt(jnp.mean(v * v, axis=-1, keepdims=True) + epsilon)
        n1[r, :] = (v * recip * gain_one).astype(BF)

    by_rows(seq, 16, norm_one)
    t_qkv.relay(2)
    t_qkv.across(1)
    t_qkv.relay(3)
    t_wo.start()

    def turn(i, carry):
        cut = lanes(i)
        w3_l[0, pl.ds(pl.multiple_of(i * LANE, LANE), LANE), :] = (
            wg_l[0, :, cut].astype(F32).T.astype(BF)
        )
        w3_l[1, pl.ds(pl.multiple_of(i * LANE, LANE), LANE), :] = (
            wu_l[0, :, cut].astype(F32).T.astype(BF)
        )
        return carry

    lax.fori_loop(0, w3_l.shape[1] // LANE, turn, 0)
    by_rows(w3_l.shape[1], 64, lambda r: w3_l.at[2].__setitem__((r, slice(None)), wd_l[0, r, :]))
    t_qkv.across(2)
    t_qkv.across(3)
    t_wo.relay(1)
    t_qkv.finish()
    own[0].wait()

    def turned(v):
        return v * cos_t[...] + swap_halves(v) * sin_t[...]

    def q_tile(j, carry):
        acc = dot_nn(n1[...], wqkv[:, lanes(j, 2 * LANE)])
        for h in (0, 1):
            q[:, lanes(2 * j + h)] = turned(acc[:, h * LANE : (h + 1) * LANE]).astype(BF)
        return carry

    lax.fori_loop(0, pairs // 2, q_tile, 0)
    acc = dot_nn(n1[...], wqkv[:, pl.ds(q_width, 2 * LANE)])
    key = turned(acc[:, :LANE]).astype(BF)
    val = acc[:, LANE:].astype(BF)
    kv[:, pl.ds(0, LANE)] = key
    kv[:, pl.ds(LANE, LANE)] = val
    spread_pair(kx, key.astype(F32))
    spread_pair(vx, val.astype(F32))
    t_wo.relay(2)
    t_wo.across(0)

    def pair(p, carry):
        qp = q[:, lanes(p)]
        g = p // (pairs // 2)
        out = jnp.zeros((seq, LANE), F32)
        for h in (0, 1):
            s = dot_nt(qp, kx[2 * g + h]) * HD ** (-0.5)
            s = jnp.where(mask[...] > 0.0, s, masked_score)
            top = jnp.max(s, axis=-1, keepdims=True)
            lse = top + jnp.log(jnp.sum(jnp.exp(s - top), axis=-1, keepdims=True))
            out = out + dot_nn(jnp.exp(s - lse).astype(BF), vx[2 * g + h])
        ctx[:, lanes(p)] = out.astype(BF)
        return carry

    lax.fori_loop(0, pairs // 2, pair, 0)
    t_wo.relay(3)
    for d in (2, 1, 3):
        zt = (z + d) % ZN
        wire.send(w3_l.at[:, rows(zt, units), :], ffn(mine), 60 + d - 1, 48 + z, dev(zt, x, c, y))
    mine3 = w3_l.at[:, rows(z, units), :]
    wire.send(mine3, ffn(mine), 64 + z, 52 + z, side)
    wire.send(mine3, ffn(mine), 68 + z * 2 + x, 56 + z * 2 + x, twin)
    l_dres.start()
    own += [
        pltpu.make_async_copy(mine3, ffn(mine), ls.at[3]),
        pltpu.make_async_copy(dres_l, dres.at[rows(z, seq), :], ls.at[4]),
    ]
    own[3].start()
    own[4].start()
    lax.fori_loop(pairs // 2, pairs, pair, 0)
    for s in (1, 2, 3):
        t_wo.across(s)
    t_wo.finish()
    own[1].wait()

    def out_tile(j, carry):
        cut = lanes(j, 2 * LANE)
        attn[:, cut] = dot_nn(ctx[...], wo[:, cut]).astype(BF)
        return carry

    lax.fori_loop(0, width // (2 * LANE), out_tile, 0)
    wire.send(attn, part, 100, 80, other)
    l_dres.relay(1)

    def ffn_in(d):
        o = (z + ZN - d) % ZN
        b = ffn(rid(o, x, c))
        wire.arrived(b, 48 + o, dev(o, x, c, y))
        wire.send(b, b, 64 + o, 52 + o, side)
        wire.send(b, b, 68 + o * 2 + x, 56 + o * 2 + x, twin)

    def ffn_across(d):
        o = (z + ZN - d) % ZN
        b = ffn(rid(o, 1 - x, c))
        wire.arrived(b, 52 + o, side)
        k = o * 2 + 1 - x
        wire.send(b, b, 68 + k, 56 + k, twin)

    ffn_in(2)
    wire.arrived(part, 80, other)

    def second(r):
        m = resid[r, :] + (attn[r, :].astype(F32) + part[r, :].astype(F32))
        mid[r, :] = m
        recip = lax.rsqrt(jnp.mean(m * m, axis=-1, keepdims=True) + epsilon)
        nrm[r, :] = (m * recip * gain_two).astype(BF)

    by_rows(seq, 16, second)
    l_norm.start()
    own.append(pltpu.make_async_copy(nrm, normed.at[rows(z, seq), :], ls.at[5]))
    own[5].start()
    ffn_in(1)
    l_dres.relay(2)
    l_norm.relay(1)
    ffn_across(0)
    ffn_in(3)
    l_dres.relay(3)
    l_norm.relay(2)
    l_norm.relay(3)
    for d in (2, 1, 3):
        ffn_across(d)
    for o in range(ZN):
        for xx in (0, 1):
            wire.arrived(ffn(rid(o, xx, 1 - c)), 56 + o * 2 + xx, twin)
    l_dres.finish()
    l_norm.finish()
    wire.drain()
    for cp in own[3:]:
        cp.wait()


def front(resid, w_query, w_key, w_value, w_out, gains, w_gate, w_up, w_down, cot, cos_t, sin_t, mask):
    seq, width = resid.shape
    q_width, out_rows = w_query.shape[2], w_out.shape[1]
    total = q_width + 2 * LANE
    units = w_gate.shape[2] // ZN
    pair_shape = (4, seq, LANE)
    return pl.pallas_call(
        front_kernel,
        name="front",
        out_shape=(
            jax.ShapeDtypeStruct((width, total), BF),
            jax.ShapeDtypeStruct((out_rows, width), BF),
            jax.ShapeDtypeStruct((16, width), BF),
            jax.ShapeDtypeStruct((3, units, width), BF),
            jax.ShapeDtypeStruct((seq * ZN, width), BF),
            jax.ShapeDtypeStruct((seq, width), BF),
            jax.ShapeDtypeStruct((seq, q_width), BF),
            jax.ShapeDtypeStruct((seq, 2 * LANE), BF),
            jax.ShapeDtypeStruct((seq, q_width), BF),
            jax.ShapeDtypeStruct((seq, width), F32),
            jax.ShapeDtypeStruct((seq * ZN, width), BF),
        ),
        in_specs=[vm_spec()] * 13,
        out_specs=[vm_spec()] * 3 + [any_spec()] * 2 + [vm_spec()] * 5 + [any_spec()],
        scratch_shapes=[
            pltpu.VMEM((LANE, total), BF),
            pltpu.VMEM((3, units * ZN, LANE), BF),
            pltpu.VMEM((seq, width), BF),
            pltpu.VMEM(pair_shape, BF),
            pltpu.VMEM(pair_shape, BF),
            pltpu.VMEM((seq, width), BF),
            pltpu.VMEM((seq, width), BF),
            pltpu.VMEM((seq, width), BF),
            sems(101),
            sems(81),
            sems(6),
        ],
        compiler_params=params(0),
    )(resid, w_query, w_key, w_value, w_out, gains, w_gate, w_up, w_down, cot, cos_t, sin_t, mask)


def add_into(dst, src, height, step):
    def one(r):
        dst[r, :] = (dst[r, :].astype(F32) + src[r, :].astype(F32)).astype(dst.dtype)

    by_rows(height, step, one)


class Chain:
    def __init__(self, wire, held, zin, height, step, send_base, recv_base):
        self.wire, self.held, self.zin = wire, held, zin
        self.height, self.step = height, step
        self.s, self.r = send_base, recv_base
        self.z, x, c, y = place()
        self.up, self.down = dev(self.z + 1, x, c, y), dev(self.z - 1, x, c, y)

    def inbound(self, o, slot, frm, cond):
        self.wire.arrived(self.zin(slot), self.r + slot, frm, cond)

        @pl.when(cond)
        def _():
            add_into(self.held(o), self.zin(slot), self.height, self.step)

    def outward(self, t, ready):
        z = self.z
        for o, cond, more, to, frm, base, slot in (
            (z + t, z + t < ZN, z > 0, self.up, self.down, 0, z + t),
            (z - t, z >= t, z < ZN - 1, self.down, self.up, 4, 4 if t == 1 else z - t),
        ):
            ready(o, cond)
            self.inbound(o, o, frm, cond & more)
            self.wire.send(
                self.held(o), self.zin(slot), self.s + base + o, self.r + slot, to, cond
            )

    def home(self):
        z = self.z
        self.inbound(z, z, self.down, z > 0)
        self.inbound(z, 4, self.up, z < ZN - 1)


class Fold:
    def __init__(self, wire, part, cin, xin, zin, height, step, send_base, recv_base):
        self.wire, self.part, self.cin, self.xin = wire, part, cin, xin
        self.height, self.step = height, step
        self.s, self.r = send_base, recv_base
        self.z, self.x, self.c, y = place()
        z, x, c = self.z, self.x, self.c
        self.side, self.twin = dev(z, 1 - x, c, y), dev(z, x, 1 - c, y)
        self.chain = Chain(
            wire, lambda o: xin.at[o], lambda s: zin.at[s], height, step, self.s + 12, self.r + 12
        )

    def order(self):
        return [(self.z + d) % ZN for d in (2, 1, 3, 0)]

    def to_twin(self):
        for xx in (1 - self.x, self.x):
            for o in self.order():
                k = o * 2 + xx
                self.wire.send(
                    self.part(k * 2 + 1 - self.c), self.cin.at[k], self.s + k, self.r + k, self.twin
                )

    def from_twin(self, k):
        self.wire.arrived(self.cin.at[k], self.r + k, self.twin)
        add_into(self.cin.at[k], self.part(k * 2 + self.c), self.height, self.step)

    def across(self):
        for o in self.order():
            k = o * 2 + 1 - self.x
            self.from_twin(k)
            self.wire.send(self.cin.at[k], self.xin.at[o], self.s + 8 + o, self.r + 8 + o, self.side)

    def stay(self):
        for o in self.order():
            self.from_twin(o * 2 + self.x)

    def ready(self, o, cond):
        self.wire.arrived(self.xin.at[o], self.r + 8 + o, self.side, cond)

        @pl.when(cond)
        def _():
            add_into(self.xin.at[o], self.cin.at[o * 2 + self.x], self.height, self.step)

    def outward(self, t):
        self.chain.outward(t, self.ready)

    def home(self):
        self.ready(self.z, self.z >= 0)
        self.chain.home()
        return self.xin.at[self.z]


def back_kernel(
    dn_p, feed_p, g3_p, mid, cot, resid, ga, n1, q, kv, ctx, wqkv, wo, cos_t, sin_t, mask,
    hidden, grad_in, g3, gq_out, gk_out, gv_out, go_out, gains_out,
    fown, yin, zin, gbuf, cin, xin, gq_p, go_p, gp, qc, qx, qz, oc, ox, oz, gc, gx, gz,
    dn, feed, mid_b, dctx, dqkv, dn1, dn1_o, kx, vx, kacc, vacc, wbuf, gs, gr, ss, rs, ls,
):
    z, x, c, y = place()
    units = g3_p.shape[1]
    seq, width = mid.shape
    half = width // 2
    q_width = q.shape[1]
    pairs = q_width // LANE
    out_rows = wo.shape[0]
    wire = Wire(ss, rs)
    side, twin, other = dev(z, 1 - x, c, y), dev(z, x, 1 - c, y), dev(z, x, c, 1 - y)
    ring = [(z + d) % ZN for d in (2, 1, 3, 0)]
    greet(all_peers(z, x, c, y))

    def y_out(src, k):
        for t in (3, 2, 1):
            for o, cond in ((z + t, z + t < ZN), (z - t, z >= t)):
                s = src.at[rows(o, seq), lanes(1 - y, half)]
                wire.send(s, yin.at[k, o], k * 4 + o, k * 4 + o, other, cond)
        s = src.at[rows(z, seq), lanes(1 - y, half)]
        wire.send(s, yin.at[k, z], k * 4 + z, k * 4 + z, other)

    y_out(dn_p, 0)
    for k in range(8):
        wire.send(g3_p.at[:, :, lanes(k * 2 + 1 - c)], cin.at[k], 26 + k, 20 + k, twin)
    ks = [o * 2 + 1 - x for o in ring] + [o * 2 + x for o in ring]

    def load(i):
        return pltpu.make_async_copy(
            g3_p.at[:, :, lanes(ks[i] * 2 + c)], gbuf.at[i % 2], ls.at[i % 2]
        )

    def own_half(o):
        return pltpu.make_async_copy(
            feed_p.at[rows(o, seq), lanes(y, half)], fown.at[o], ls.at[2 + o]
        )

    def add3(dst, src):
        for m in range(3):
            add_into(dst.at[m], src.at[m], units, 64)

    load(0).start()
    for i in range(8):
        if i < 7:
            load(i + 1).start()
        load(i).wait()
        wire.arrived(cin.at[ks[i]], 20 + ks[i], twin)
        add3(cin.at[ks[i]], gbuf.at[i % 2])
        if i < 4:
            o = ring[i]
            wire.send(cin.at[ks[i]], xin.at[o], 34 + o, 28 + o, side)
    for o in range(ZN):
        own_half(o).start()

    def chain_of(k):
        return Chain(
            wire, lambda o: yin.at[k, o], lambda s: zin.at[k, s], seq, 16, 8 + k * 8, 8 + k * 5
        )

    def dn_ready(o, cond):
        wire.arrived(yin.at[0, o], o, other, cond)

        @pl.when(cond)
        def _():
            def one(r):
                mine = dn_p[pl.ds(pl.multiple_of(o * seq, 16) + r.start, 16), lanes(y, half)]
                yin[0, o, r, :] = (yin[0, o, r, :].astype(F32) + mine.astype(F32)).astype(BF)

            by_rows(seq, 16, one)

    line = chain_of(0)
    for t in (3, 2, 1):
        line.outward(t, dn_ready)
    dn_ready(z, z >= 0)
    line.home()
    blk = dn.at[:, lanes(y, half)]

    def keep_dn(r):
        dn[r, lanes(y, half)] = yin[0, z, r, :]

    by_rows(seq, 16, keep_dn)
    wire.send(blk, blk, 24, 18, other)
    y_out(feed_p, 1)

    def ffn_z(i):
        o = ring[i]
        wire.arrived(xin.at[o], 28 + o, side)
        add3(xin.at[o], cin.at[o * 2 + x])
        d = (2, 1, 3, 0)[i]
        if d:
            wire.send(xin.at[o], g3.at[:, rows(z, units), :], 38 + d - 1, 32 + z, dev(o, x, c, y))
        else:
            pltpu.make_async_copy(xin.at[o], g3.at[:, rows(z, units), :], ls.at[6]).start()

    ffn_z(0)
    ffn_z(1)
    spread_pair(kx, kv[:, pl.ds(0, LANE)].astype(F32))
    spread_pair(vx, kv[:, pl.ds(LANE, LANE)].astype(F32))
    kacc[...] = jnp.zeros_like(kacc)
    vacc[...] = jnp.zeros_like(vacc)
    gp[...] = jnp.zeros_like(gp)
    gain_one = ga[pl.ds(0, 8), :].astype(F32)[0:1]
    gain_two = ga[pl.ds(0, 8), :].astype(F32)[1:2]
    wire.arrived(dn.at[:, lanes(1 - y, half)], 18, other)

    def norm_two(r):
        v, g = mid[r, :], dn[r, :].astype(F32)
        recip = lax.rsqrt(jnp.mean(v * v, axis=-1, keepdims=True) + epsilon)
        e = g * gain_two
        d = recip * e - v * (recip * recip * recip) * jnp.mean(e * v, axis=-1, keepdims=True)
        out = cot[r, :] + d
        grad_in[r, :] = out
        mid_b[r, :] = out.astype(BF)
        t = g * v * recip
        gp[pl.ds(8, 8), :] += t[:8] + t[8:]

    by_rows(seq, 16, norm_two)

    def out_grad(i, carry):
        cut = lanes(i, 2 * LANE)
        for h in range(2):
            hh = pl.ds(h * (out_rows // 2), out_rows // 2)
            go_p[hh, cut] = dot_tn(ctx[:, hh], mid_b[:, cut]).astype(BF)
        return carry

    lax.fori_loop(0, width // (2 * LANE), out_grad, 0)
    f_o = Fold(wire, lambda r: go_p.at[:, lanes(r)], oc, ox, oz, out_rows, 64, 61, 53)
    f_q = Fold(
        wire,
        lambda r: gq_p.at[pl.ds(pl.multiple_of(r * LANE, LANE), LANE), :],
        qc, qx, qz, LANE, 16, 41, 36,
    )
    f_g = Fold(wire, lambda r: gp.at[:, lanes(r)], gc, gx, gz, 16, 16, 81, 70)
    f_o.to_twin()

    def ctx_grad(j, carry):
        cut = lanes(j, 2 * LANE)
        dctx[:, cut] = dot_nt(mid_b[...], wo[cut, :]).astype(BF)
        return carry

    lax.fori_loop(0, q_width // (2 * LANE), ctx_grad, 0)
    ffn_z(2)
    ffn_z(3)
    f_o.across()

    def back_turned(v):
        return v * cos_t[...] - swap_halves(v) * sin_t[...]

    def pair(p, carry):
        qp, dc = q[:, lanes(p)], dctx[:, lanes(p)]
        g = p // (pairs // 2)
        prod = dc.astype(F32) * ctx[:, lanes(p)].astype(F32)
        low = lax.broadcasted_iota(jnp.int32, prod.shape, 1) < HD
        dq = jnp.zeros((seq, LANE), F32)
        for h in (0, 1):
            i = 2 * g + h
            s = dot_nt(qp, kx[i]) * HD ** (-0.5)
            s = jnp.where(mask[...] > 0.0, s, masked_score)
            top = jnp.max(s, axis=-1, keepdims=True)
            lse = top + jnp.log(jnp.sum(jnp.exp(s - top), axis=-1, keepdims=True))
            full = jnp.exp(s - lse)
            delta = jnp.sum(jnp.where(low if h == 0 else ~low, prod, 0.0), axis=-1, keepdims=True)
            ds = (full * (dot_nt(dc, vx[i]) - delta)).astype(BF)
            dq = dq + dot_nn(ds, kx[i])
            kacc[i] += dot_tn(ds, qp)
            vacc[i] += dot_tn(full.astype(BF), dc)
        dqkv[:, lanes(p)] = back_turned(dq * HD ** (-0.5)).astype(BF)
        return carry

    lax.fori_loop(0, pairs, pair, 0)

    def joined(acc):
        low = lax.broadcasted_iota(jnp.int32, (seq, LANE), 1) < HD
        return jnp.where(
            low, acc[0] + pltpu.roll(acc[1], HD, 1), acc[3] + pltpu.roll(acc[2], HD, 1)
        )

    dqkv[:, pl.ds(q_width, LANE)] = back_turned(joined(kacc) * HD ** (-0.5)).astype(BF)
    dqkv[:, pl.ds(q_width + LANE, LANE)] = joined(vacc).astype(BF)

    def w_tile(j, slot):
        r = pl.ds(pl.multiple_of(j * 2 * LANE, 2 * LANE), 2 * LANE)
        return pltpu.make_async_copy(wqkv.at[r, :], wbuf.at[slot], ls.at[7 + slot])

    w_tile(0, 0).start()

    def in_grad(r, carry):
        gq_p[pl.ds(pl.multiple_of(r * LANE, LANE), LANE), :] = dot_tn(
            n1[:, lanes(r)], dqkv[...]
        ).astype(BF)
        return carry

    lax.fori_loop(0, width // LANE, in_grad, 0)
    f_q.to_twin()
    tiles = width // (2 * LANE)
    for j in range(tiles):
        if j + 1 < tiles:
            w_tile(j + 1, (j + 1) % 2).start()
        w_tile(j, j % 2).wait()
        dn1[:, pl.ds(j * 2 * LANE, 2 * LANE)] = dot_nt(dqkv[...], wbuf[j % 2]).astype(BF)
    wire.send(dn1, dn1_o, 101, 87, other)
    f_q.across()

    def gain_part(r):
        v = resid[r, :]
        recip = lax.rsqrt(jnp.mean(v * v, axis=-1, keepdims=True) + epsilon)
        t = dn1[r, :].astype(F32) * v * recip
        gp[pl.ds(0, 8), :] += t[:8] + t[8:]

    by_rows(seq, 16, gain_part)
    f_g.to_twin()
    f_g.across()
    f_o.stay()
    for t in (3, 2, 1):
        f_o.outward(t)

    for o in range(ZN):
        own_half(o).wait()

    def feed_ready(o, cond):
        wire.arrived(yin.at[1, o], 4 + o, other, cond)

        @pl.when(cond)
        def _():
            add_into(yin.at[1, o], fown.at[o], seq, 16)

    line = chain_of(1)
    for t in (3, 2, 1):
        line.outward(t, feed_ready)
    f_q.stay()
    f_g.stay()
    for t in (3, 2, 1):
        f_q.outward(t)
        f_g.outward(t)
    feed_ready(z, z >= 0)
    line.home()
    fb = feed.at[:, lanes(y, half)]

    def keep_feed(r):
        feed[r, lanes(y, half)] = yin[1, z, r, :]

    by_rows(seq, 16, keep_feed)
    wire.send(fb, fb, 25, 19, other)
    wire.arrived(dn1_o, 87, other)

    def norm_one(r):
        v = resid[r, :]
        g = dn1[r, :].astype(F32) + dn1_o[r, :].astype(F32)
        recip = lax.rsqrt(jnp.mean(v * v, axis=-1, keepdims=True) + epsilon)
        e = g * gain_one
        d = recip * e - v * (recip * recip * recip) * jnp.mean(e * v, axis=-1, keepdims=True)
        grad_in[r, :] += d

    by_rows(seq, 16, norm_one)
    done = f_o.home()
    by_rows(out_rows, 64, lambda r: go_out.at[0].__setitem__((r, slice(None)), done[r, :].astype(F32)))
    mine = f_g.home()
    gs[...] = mine[...]
    wire.send(gs, gr, 102, 88, other)
    got = f_q.home()
    cut_k, cut_v = pl.ds(q_width, LANE), pl.ds(q_width + LANE, LANE)
    gq_out[0] = got[:, pl.ds(0, q_width)].astype(F32)
    gk_out[0] = got[:, cut_k].astype(F32)
    gv_out[0] = got[:, cut_v].astype(F32)
    wire.arrived(feed.at[:, lanes(1 - y, half)], 19, other)

    def last(r):
        hidden[r, :] = mid[r, :] + feed[r, :].astype(F32)

    by_rows(seq, 16, last)
    wire.arrived(gr, 88, other)
    first = jnp.sum(gs[pl.ds(0, 8), :] + gr[pl.ds(0, 8), :], axis=0, keepdims=True)
    second = jnp.sum(gs[pl.ds(8, 8), :], axis=0, keepdims=True)
    row = lax.broadcasted_iota(jnp.int32, (8, LANE), 0)
    gains_out[...] = jnp.where(row == 0, first, second)
    for d in (1, 2, 3):
        o = (z + ZN - d) % ZN
        wire.arrived(g3.at[:, rows(o, units), :], 32 + o, dev(o, x, c, y))
    wire.drain()
    pltpu.make_async_copy(xin.at[z], g3.at[:, rows(z, units), :], ls.at[6]).wait()


def back(dn_p, feed_p, g3_p, mid, cot, resid, ga, n1, q, kv, ctx, wqkv, wo, cos_t, sin_t, mask):
    seq, width = mid.shape
    units = g3_p.shape[1]
    q_width, total = q.shape[1], wqkv.shape[1]
    out_rows = wo.shape[0]
    half = width // 2

    def vm(*shape, dtype=BF):
        return pltpu.VMEM(shape, dtype)

    return pl.pallas_call(
        back_kernel,
        name="back",
        out_shape=(
            jax.ShapeDtypeStruct((seq, width), F32),
            jax.ShapeDtypeStruct((seq, width), F32),
            jax.ShapeDtypeStruct((3, units * ZN, LANE), BF),
            jax.ShapeDtypeStruct((1, LANE, q_width), F32),
            jax.ShapeDtypeStruct((1, LANE, LANE), F32),
            jax.ShapeDtypeStruct((1, LANE, LANE), F32),
            jax.ShapeDtypeStruct((1, out_rows, LANE), F32),
            jax.ShapeDtypeStruct((8, LANE), F32),
        ),
        in_specs=[vm_spec()] + [any_spec()] * 2 + [vm_spec()] * 8 + [any_spec()] + [vm_spec()] * 4,
        out_specs=[vm_spec()] * 2 + [any_spec()] + [vm_spec()] * 5,
        scratch_shapes=[
            vm(ZN, seq, half),
            vm(2, ZN, seq, half),
            vm(2, 5, seq, half),
            vm(2, 3, units, LANE),
            vm(8, 3, units, LANE),
            vm(4, 3, units, LANE),
            vm(width, total),
            vm(out_rows, width),
            vm(16, width, dtype=F32),
            vm(8, LANE, total),
            vm(4, LANE, total),
            vm(5, LANE, total),
            vm(8, out_rows, LANE),
            vm(4, out_rows, LANE),
            vm(5, out_rows, LANE),
            vm(8, 16, LANE, dtype=F32),
            vm(4, 16, LANE, dtype=F32),
            vm(5, 16, LANE, dtype=F32),
            vm(seq, width),
            vm(seq, width),
            vm(seq, width),
            vm(seq, q_width),
            vm(seq, total),
            vm(seq, width),
            vm(seq, width),
            vm(4, seq, LANE),
            vm(4, seq, LANE),
            vm(4, seq, LANE, dtype=F32),
            vm(4, seq, LANE, dtype=F32),
            vm(2, 2 * LANE, total),
            vm(16, LANE, dtype=F32),
            vm(16, LANE, dtype=F32),
            sems(103),
            sems(89),
            sems(9),
        ],
        compiler_params=pltpu.CompilerParams(
            collective_id=1, has_side_effects=True, vmem_limit_bytes=67043328
        ),
    )(dn_p, feed_p, g3_p, mid, cot, resid, ga, n1, q, kv, ctx, wqkv, wo, cos_t, sin_t, mask)


def fast_body(
    hidden_in,
    segment_ids,
    gain_attn,
    w_query,
    w_key,
    w_value,
    w_out,
    gain_ffn,
    w_gate,
    w_up,
    w_down,
    cotangent,
):
    cos_t, sin_t = rope_tables(segment_positions(segment_ids))
    cos_w = jnp.tile(cos_t[0], (1, 4))
    sin_w = jnp.tile(jnp.concatenate([-sin_t[0], sin_t[0]], axis=1), (1, 2))
    mask = attention_mask(segment_ids)[0, 0, 0].astype(F32)
    gains = jnp.concatenate([gain_attn, gain_ffn, jnp.zeros((14, LANE), BF)], axis=0)
    resid = hidden_in
    wqkv, wo, ga, w3, dres_all, n1, q, kv, ctx, middle, normed_all = front(
        resid, w_query, w_key, w_value, w_out, gains, w_gate, w_up, w_down, cotangent,
        cos_w, sin_w, mask,
    )
    gate = contract_cols(normed_all, w3[0])
    up_proj = contract_cols(normed_all, w3[1])
    sigma = jax.nn.sigmoid(gate)
    hidden_act = (gate * sigma * up_proj).astype(BF)
    grad_hidden = contract_cols(dres_all, w3[2])
    grad_gate_b = (grad_hidden * up_proj * sigma * (1.0 + gate * (1.0 - sigma))).astype(BF)
    grad_up_b = (grad_hidden * (gate * sigma)).astype(BF)
    feed_p = jnp.dot(hidden_act, w3[2], preferred_element_type=F32).astype(BF)
    dn_p = (
        jnp.dot(grad_gate_b, w3[0], preferred_element_type=F32)
        + jnp.dot(grad_up_b, w3[1], preferred_element_type=F32)
    ).astype(BF)
    g3_p = jnp.stack(
        [
            contract_rows(grad_gate_b, normed_all).astype(BF),
            contract_rows(grad_up_b, normed_all).astype(BF),
            contract_rows(hidden_act, dres_all).astype(BF),
        ]
    )
    hidden_out, grad_input, g3, gq, gk, gv, go, gains_g = back(
        dn_p, feed_p, g3_p, middle, cotangent, resid, ga, n1, q, kv, ctx, wqkv, wo,
        cos_w, sin_w, mask,
    )
    return (
        hidden_out,
        grad_input,
        gains_g[0:1],
        gq,
        gk,
        gv,
        go,
        gains_g[1:2],
        g3[0].T.astype(F32)[None],
        g3[1].T.astype(F32)[None],
        g3[2].astype(F32)[None],
    )


def solution(mesh):
    small = mesh.shape["dp"] == 16 and mesh.shape["tensor"] == 2
    chosen = fast_body if small else body
    return jax.shard_map(
        chosen,
        mesh=mesh,
        in_specs=(
            P("dp", None),
            P("dp", None),
            P(None, "dp"),
            P(None, "dp", "tensor"),
            P(None, "dp", "tensor"),
            P(None, "dp", "tensor"),
            P(None, "tensor", "dp"),
            P(None, "dp"),
            P(None, "dp", "tensor"),
            P(None, "dp", "tensor"),
            P(None, "tensor", "dp"),
            P("dp", None),
        ),
        out_specs=(
            P("dp", None),
            P("dp", None),
            P(None, "dp"),
            P(None, "dp", "tensor"),
            P(None, "dp", "tensor"),
            P(None, "dp", "tensor"),
            P(None, "tensor", "dp"),
            P(None, "dp"),
            P(None, "dp", "tensor"),
            P(None, "dp", "tensor"),
            P(None, "tensor", "dp"),
        ),
        check_vma=False,
    )
```

```python
import jax
import jax.numpy as jnp
import numpy as np
from jax import lax
from jax.experimental import pallas as pl
from jax.experimental.pallas import tpu as pltpu
from jax.sharding import PartitionSpec as P

HD = 64


epsilon = 1e-05
rope_base = 10000.0
masked_score = -1e30


def segment_positions(segment_ids):
    row_count, seq_len = segment_ids.shape
    index_grid = lax.broadcasted_iota(jnp.int32, (row_count, seq_len), 1)
    previous = jnp.concatenate([segment_ids[:, :1] - 1, segment_ids[:, :-1]], axis=1)
    starts = jnp.where(segment_ids != previous, index_grid, 0)
    return index_grid - lax.cummax(starts, axis=1)


def rope_tables(positions):
    half_dim = HD // 2
    inv_freq = rope_base ** (-(jnp.arange(half_dim, dtype=jnp.float32) * 2.0 / HD))
    angles = positions.astype(jnp.float32)[:, :, None] * inv_freq
    return (jnp.cos(angles), jnp.sin(angles))


def expand_table(table, values):
    extra_dims = values.ndim - 3
    return table.reshape(table.shape[:2] + (1,) * extra_dims + table.shape[2:])


def rotate_pairs(values, cos_t, sin_t):
    half_dim = values.shape[-1] // 2
    cos_e = expand_table(cos_t, values)
    sin_e = expand_table(sin_t, values)
    first, second = (values[..., :half_dim], values[..., half_dim:])
    return jnp.concatenate(
        [first * cos_e - second * sin_e, second * cos_e + first * sin_e], axis=-1
    )


def unrotate_pairs(values, cos_t, sin_t):
    half_dim = values.shape[-1] // 2
    cos_e = expand_table(cos_t, values)
    sin_e = expand_table(sin_t, values)
    first, second = (values[..., :half_dim], values[..., half_dim:])
    return jnp.concatenate(
        [first * cos_e + second * sin_e, second * cos_e - first * sin_e], axis=-1
    )


def attention_mask(segment_ids):
    seq_len = segment_ids.shape[1]
    same_seg = segment_ids[:, :, None] == segment_ids[:, None, :]
    query_pos = lax.broadcasted_iota(jnp.int32, (seq_len, seq_len), 0)
    key_pos = lax.broadcasted_iota(jnp.int32, (seq_len, seq_len), 1)
    return (same_seg & (key_pos <= query_pos))[:, None, None, :, :]


def score_block(query_heads, key_heads, allowed):
    scores = jnp.einsum(
        "rikgd,rjkd->rkgij", query_heads, key_heads, preferred_element_type=jnp.float32
    ) * HD ** (-0.5)
    return jnp.where(allowed, scores, masked_score)


def attend(query_heads, key_heads, value_heads, allowed):
    scores = score_block(query_heads, key_heads, allowed)
    row_max = jnp.max(scores, axis=-1, keepdims=True)
    log_norm = row_max + jnp.log(jnp.sum(jnp.exp(scores - row_max), axis=-1, keepdims=True))
    attn_probs = jnp.exp(scores - log_norm).astype(jnp.bfloat16)
    context = jnp.einsum(
        "rkgij,rjkd->rikgd", attn_probs, value_heads, preferred_element_type=jnp.float32
    )
    return (context.astype(jnp.bfloat16), log_norm)


def attend_back(query_heads, key_heads, value_heads, context, log_norm, grad_context, allowed):
    scores = score_block(query_heads, key_heads, allowed)
    probs_full = jnp.exp(scores - log_norm)
    probs_b = probs_full.astype(jnp.bfloat16)
    grad_v = jnp.einsum(
        "rkgij,rikgd->rjkd", probs_b, grad_context, preferred_element_type=jnp.float32
    )
    grad_probs = jnp.einsum(
        "rikgd,rjkd->rkgij", grad_context, value_heads, preferred_element_type=jnp.float32
    )
    delta = jnp.sum(grad_context.astype(jnp.float32) * context.astype(jnp.float32), axis=-1)
    delta = jnp.transpose(delta, (0, 2, 3, 1))[..., None]
    grad_scores = (probs_full * (grad_probs - delta)).astype(jnp.bfloat16)
    grad_q = jnp.einsum(
        "rkgij,rjkd->rikgd", grad_scores, key_heads, preferred_element_type=jnp.float32
    ) * HD ** (-0.5)
    grad_k = jnp.einsum(
        "rkgij,rikgd->rjkd", grad_scores, query_heads, preferred_element_type=jnp.float32
    ) * HD ** (-0.5)
    return (grad_q, grad_k, grad_v)


def contract_rows(left, right):
    return lax.dot_general(
        left, right, (((0,), (0,)), ((), ())), preferred_element_type=jnp.float32
    )


def contract_cols(left, right):
    return lax.dot_general(
        left, right, (((1,), (1,)), ((), ())), preferred_element_type=jnp.float32
    )


def norm_backward(resid, recip, gain, grad_normed):
    scaled = grad_normed * gain.astype(jnp.float32)
    grad_gain = jnp.sum(grad_normed * resid * recip, axis=0)
    grad_resid = recip * scaled - resid * (recip * recip * recip) * jnp.mean(
        scaled * resid, axis=-1, keepdims=True
    )
    return (grad_gain, grad_resid)


def layer_forward(resid, weights, cos_t, sin_t, allowed):
    gain_one, w_query, w_key, w_value, w_out, gain_two, w_gate, w_up, w_down = weights
    row_count, seq_len = (cos_t.shape[0], cos_t.shape[1])
    heads_here = w_query.shape[1] // HD
    kv_here = w_key.shape[1] // HD
    group_size = heads_here // kv_here
    recip_one = lax.rsqrt(jnp.mean(resid * resid, axis=-1, keepdims=True) + epsilon)
    normed_one = (resid * recip_one * gain_one.astype(jnp.float32)).astype(jnp.bfloat16)
    query_raw = jnp.dot(normed_one, w_query, preferred_element_type=jnp.float32)
    query_heads = rotate_pairs(
        query_raw.reshape(row_count, seq_len, kv_here, group_size, HD), cos_t, sin_t
    ).astype(jnp.bfloat16)
    key_raw = jnp.dot(normed_one, w_key, preferred_element_type=jnp.float32)
    key_heads = rotate_pairs(key_raw.reshape(row_count, seq_len, kv_here, HD), cos_t, sin_t).astype(
        jnp.bfloat16
    )
    value_raw = jnp.dot(normed_one, w_value, preferred_element_type=jnp.float32)
    value_heads = value_raw.reshape(row_count, seq_len, kv_here, HD).astype(jnp.bfloat16)
    context, log_norm = attend(query_heads, key_heads, value_heads, allowed)
    context_flat = context.reshape(row_count * seq_len, heads_here * HD)
    attn_sum = lax.psum(jnp.dot(context_flat, w_out, preferred_element_type=jnp.float32), "tensor")
    middle = resid + attn_sum
    recip_two = lax.rsqrt(jnp.mean(middle * middle, axis=-1, keepdims=True) + epsilon)
    normed_two = (middle * recip_two * gain_two.astype(jnp.float32)).astype(jnp.bfloat16)
    gate = jnp.dot(normed_two, w_gate, preferred_element_type=jnp.float32)
    up_proj = jnp.dot(normed_two, w_up, preferred_element_type=jnp.float32)
    hidden_act = (jax.nn.silu(gate) * up_proj).astype(jnp.bfloat16)
    feed_out = lax.psum(jnp.dot(hidden_act, w_down, preferred_element_type=jnp.float32), "tensor")
    kept_state = (
        resid,
        recip_one,
        normed_one,
        query_heads,
        key_heads,
        value_heads,
        context,
        log_norm,
        middle,
        recip_two,
        normed_two,
        gate,
        up_proj,
        hidden_act,
    )
    return (middle + feed_out, kept_state)


def backward_layer(grad_resid, kept_state, weights, cos_t, sin_t, allowed):
    (
        resid,
        recip_one,
        normed_one,
        query_heads,
        key_heads,
        value_heads,
        context,
        log_norm,
        middle,
        recip_two,
        normed_two,
        gate,
        up_proj,
        hidden_act,
    ) = kept_state
    gain_one, w_query, w_key, w_value, w_out, gain_two, w_gate, w_up, w_down = weights
    token_count = resid.shape[0]
    grad_b = grad_resid.astype(jnp.bfloat16)
    grad_down = contract_rows(hidden_act, grad_b)
    grad_hidden = contract_cols(grad_b, w_down)
    sigma = jax.nn.sigmoid(gate)
    grad_gate_b = (grad_hidden * up_proj * sigma * (1.0 + gate * (1.0 - sigma))).astype(
        jnp.bfloat16
    )
    grad_up_b = (grad_hidden * (gate * sigma)).astype(jnp.bfloat16)
    grad_gate_w = contract_rows(normed_two, grad_gate_b)
    grad_up_w = contract_rows(normed_two, grad_up_b)
    grad_normed_two = lax.psum(
        contract_cols(grad_gate_b, w_gate) + contract_cols(grad_up_b, w_up), "tensor"
    )
    grad_gain_two, grad_mid_norm = norm_backward(middle, recip_two, gain_two, grad_normed_two)
    grad_middle = grad_resid + grad_mid_norm
    middle_b = grad_middle.astype(jnp.bfloat16)
    context_flat = context.reshape(token_count, -1)
    grad_out_w = contract_rows(context_flat, middle_b)
    grad_context = contract_cols(middle_b, w_out).astype(jnp.bfloat16).reshape(context.shape)
    grad_q, grad_k, grad_v = attend_back(
        query_heads, key_heads, value_heads, context, log_norm, grad_context, allowed
    )
    grad_q = unrotate_pairs(grad_q, cos_t, sin_t).astype(jnp.bfloat16).reshape(token_count, -1)
    grad_k = unrotate_pairs(grad_k, cos_t, sin_t).astype(jnp.bfloat16).reshape(token_count, -1)
    grad_v = grad_v.astype(jnp.bfloat16).reshape(token_count, -1)
    grad_query_w = contract_rows(normed_one, grad_q)
    grad_key_w = contract_rows(normed_one, grad_k)
    grad_value_w = contract_rows(normed_one, grad_v)
    grad_normed_one = lax.psum(
        contract_cols(grad_q, w_query)
        + contract_cols(grad_k, w_key)
        + contract_cols(grad_v, w_value),
        "tensor",
    )
    grad_gain_one, grad_res_norm = norm_backward(resid, recip_one, gain_one, grad_normed_one)
    grad_input = grad_middle + grad_res_norm
    layer_grads = (
        lax.psum_scatter(grad_gain_one, "dp", scatter_dimension=0, tiled=True),
        lax.psum_scatter(grad_query_w, "dp", scatter_dimension=0, tiled=True),
        lax.psum_scatter(grad_key_w, "dp", scatter_dimension=0, tiled=True),
        lax.psum_scatter(grad_value_w, "dp", scatter_dimension=0, tiled=True),
        lax.psum_scatter(grad_out_w, "dp", scatter_dimension=1, tiled=True),
        lax.psum_scatter(grad_gain_two, "dp", scatter_dimension=0, tiled=True),
        lax.psum_scatter(grad_gate_w, "dp", scatter_dimension=0, tiled=True),
        lax.psum_scatter(grad_up_w, "dp", scatter_dimension=0, tiled=True),
        lax.psum_scatter(grad_down, "dp", scatter_dimension=1, tiled=True),
    )
    return (grad_input, tuple(layer_grads))


def body(
    hidden_in,
    segment_ids,
    gain_attn,
    w_query,
    w_key,
    w_value,
    w_out,
    gain_ffn,
    w_gate,
    w_up,
    w_down,
    cotangent,
):
    cos_t, sin_t = rope_tables(segment_positions(segment_ids))
    allowed = attention_mask(segment_ids)
    layer_count = w_query.shape[0]
    resid = hidden_in
    retained = []
    layer_no = 0
    gathered = (
        lax.all_gather(gain_attn[layer_no], "dp", axis=0, tiled=True),
        lax.all_gather(w_query[layer_no], "dp", axis=0, tiled=True),
        lax.all_gather(w_key[layer_no], "dp", axis=0, tiled=True),
        lax.all_gather(w_value[layer_no], "dp", axis=0, tiled=True),
        lax.all_gather(w_out[layer_no], "dp", axis=1, tiled=True),
        lax.all_gather(gain_ffn[layer_no], "dp", axis=0, tiled=True),
        lax.all_gather(w_gate[layer_no], "dp", axis=0, tiled=True),
        lax.all_gather(w_up[layer_no], "dp", axis=0, tiled=True),
        lax.all_gather(w_down[layer_no], "dp", axis=1, tiled=True),
    )
    retained.append(gathered)
    resid, kept_state = layer_forward(resid, gathered, cos_t, sin_t, allowed)
    states = [kept_state]
    grad_resid = cotangent
    collected = [None] * layer_count
    for layer_no in reversed(range(layer_count)):
        gathered = (
            lax.all_gather(gain_attn[layer_no], "dp", axis=0, tiled=True),
            lax.all_gather(w_query[layer_no], "dp", axis=0, tiled=True),
            lax.all_gather(w_key[layer_no], "dp", axis=0, tiled=True),
            lax.all_gather(w_value[layer_no], "dp", axis=0, tiled=True),
            lax.all_gather(w_out[layer_no], "dp", axis=1, tiled=True),
            lax.all_gather(gain_ffn[layer_no], "dp", axis=0, tiled=True),
            lax.all_gather(w_gate[layer_no], "dp", axis=0, tiled=True),
            lax.all_gather(w_up[layer_no], "dp", axis=0, tiled=True),
            lax.all_gather(w_down[layer_no], "dp", axis=1, tiled=True),
        )
        grad_resid, collected[layer_no] = backward_layer(
            grad_resid, states[layer_no], gathered, cos_t, sin_t, allowed
        )
    stacked = tuple((jnp.stack([collected[0][member]]) for member in range(9)))
    return (
        resid,
        grad_resid,
        stacked[0],
        stacked[1],
        stacked[2],
        stacked[3],
        stacked[4],
        stacked[5],
        stacked[6],
        stacked[7],
        stacked[8],
    )


ZN = 4
MESH = pl.DeviceIdType.MESH
BF = jnp.bfloat16
F32 = jnp.float32
LANE = 128


def place():
    dp = lax.axis_index("dp")
    return dp // 4, (dp // 2) % 2, dp % 2, lax.axis_index("tensor")


def dev(z, x, c, y):
    return (z * 4 + x * 2 + c, y)


def rid(z, x, c):
    return (z * 2 + x) * 2 + c


def lanes(r, width=LANE):
    return pl.ds(pl.multiple_of(r * width, LANE), width)


def rows(r, height):
    return pl.ds(pl.multiple_of(r * height, 16), height)


def greet(peers):
    barrier = pltpu.get_barrier_semaphore()
    for peer in peers:
        pl.semaphore_signal(barrier, inc=1, device_id=peer, device_id_type=MESH)
    pl.semaphore_wait(barrier, len(peers))


class Wire:
    def __init__(self, send_sem, recv_sem):
        self.send_sem = send_sem
        self.recv_sem = recv_sem
        self.started = []

    def make(self, src, dst, si, ri, to):
        return pltpu.make_async_remote_copy(
            src_ref=src,
            dst_ref=dst,
            send_sem=self.send_sem.at[si],
            recv_sem=self.recv_sem.at[ri],
            device_id=to,
            device_id_type=MESH,
        )

    def send(self, src, dst, si, ri, to, cond=None):
        def go():
            self.make(src, dst, si, ri, to).start()

        def done():
            self.make(src, dst, si, ri, to).wait_send()

        if cond is None:
            go()
            self.started.append(done)
        else:
            pl.when(cond)(go)
            self.started.append(lambda: pl.when(cond)(done))

    def arrived(self, dst, ri, to, cond=None):
        def wait():
            self.make(dst, dst, 0, ri, to).wait_recv()

        if cond is None:
            wait()
        else:
            pl.when(cond)(wait)

    def drain(self):
        for done in self.started:
            done()


def all_peers(z, x, c, y):
    near = [dev(z, x, 1 - c, y), dev(z, 1 - x, c, y), dev(z, x, c, 1 - y)]
    return near + [dev((z + d) % ZN, x, c, y) for d in (1, 2, 3)]


def params(cid):
    return pltpu.CompilerParams(
        collective_id=cid, has_side_effects=True, vmem_limit_bytes=60 * 1024 * 1024
    )


def any_spec():
    return pl.BlockSpec(memory_space=pl.ANY)


def vm_spec():
    return pl.BlockSpec(memory_space=pltpu.VMEM)


def sems(n):
    return pltpu.SemaphoreType.DMA((n,))


def dot_nn(a, b):
    return lax.dot_general(a, b, (((1,), (0,)), ((), ())), preferred_element_type=F32)


def dot_nt(a, b):
    return lax.dot_general(a, b, (((1,), (1,)), ((), ())), preferred_element_type=F32)


def dot_tn(a, b):
    return lax.dot_general(a, b, (((0,), (0,)), ((), ())), preferred_element_type=F32)


def by_rows(height, step, one):
    def wrapped(i, carry):
        one(pl.ds(pl.multiple_of(i * step, step), step))
        return carry

    lax.fori_loop(0, height // step, wrapped, 0)


def swap_halves(v):
    lane = lax.broadcasted_iota(jnp.int32, v.shape, 1)
    first = (lane % HD) < (HD // 2)
    return jnp.where(first, pltpu.roll(v, LANE - HD // 2, 1), pltpu.roll(v, HD // 2, 1))


def spread_pair(dst, pair):
    lane = lax.broadcasted_iota(jnp.int32, pair.shape, 1)
    low = lane < HD
    turned = pltpu.roll(pair, HD, 1)
    zero = jnp.zeros_like(pair)
    dst[0] = jnp.where(low, pair, zero).astype(BF)
    dst[1] = jnp.where(low, zero, turned).astype(BF)
    dst[2] = jnp.where(low, turned, zero).astype(BF)
    dst[3] = jnp.where(low, zero, pair).astype(BF)


class Line:
    def __init__(self, wire, own, buf, send_base, recv_base):
        self.wire, self.own, self.buf = wire, own, buf
        self.s, self.r = send_base, recv_base
        z, x, c, y = place()
        self.z, self.y = z, y
        self.up, self.down = dev(z + 1, x, c, y), dev(z - 1, x, c, y)
        self.other = dev(z, x, c, 1 - y)
        self.seq, self.half = own.shape[0], own.shape[1] // 2

    def blk(self, o, h):
        return self.buf.at[rows(o, self.seq), lanes(h, self.half)]

    def start(self):
        z, wire = self.z, self.wire
        src = self.own.at[:, lanes(self.y, self.half)]
        dst = self.blk(z, self.y)
        wire.send(src, dst, self.s + z, self.r + z, self.up, z < ZN - 1)
        wire.send(src, dst, self.s + 4 + z, self.r + z, self.down, z > 0)

    def relay(self, s):
        z, wire = self.z, self.wire
        for o, cond, fwd, to, frm, base in (
            (z - s, z >= s, z < ZN - 1, self.up, self.down, 0),
            (z + s, z + s < ZN, z > 0, self.down, self.up, 4),
        ):
            b = self.blk(o, self.y)
            wire.arrived(b, self.r + o, frm, cond)
            wire.send(b, b, self.s + base + o, self.r + o, to, cond & fwd)
            wire.send(b, b, self.s + 8 + o, self.r + 4 + o, self.other, cond)

    def finish(self):
        for o in range(ZN):
            self.wire.arrived(self.blk(o, 1 - self.y), self.r + 4 + o, self.other, self.z != o)


class Tree:
    def __init__(self, wire, own, blk, send_base, recv_base):
        self.wire, self.own, self.blk = wire, own, blk
        self.s, self.r = send_base, recv_base
        self.z, self.x, self.c, y = place()
        z, x, c = self.z, self.x, self.c
        self.up, self.down = dev(z + 1, x, c, y), dev(z - 1, x, c, y)
        self.side, self.twin = dev(z, 1 - x, c, y), dev(z, x, 1 - c, y)

    def start_z(self):
        z, wire = self.z, self.wire
        d = self.blk(rid(z, self.x, self.c))
        wire.send(self.own, d, self.s + z, self.r + z, self.up, z < ZN - 1)
        wire.send(self.own, d, self.s + 4 + z, self.r + z, self.down, z > 0)

    def start_near(self):
        z, wire = self.z, self.wire
        d = self.blk(rid(z, self.x, self.c))
        wire.send(self.own, d, self.s + 8 + z, self.r + 4 + z, self.side)
        k = z * 2 + self.x
        wire.send(self.own, d, self.s + 12 + k, self.r + 8 + k, self.twin)

    def start(self):
        self.start_z()
        self.start_near()

    def relay(self, s):
        z, wire = self.z, self.wire
        for o, cond, fwd, to, frm, base in (
            (z - s, z >= s, z < ZN - 1, self.up, self.down, 0),
            (z + s, z + s < ZN, z > 0, self.down, self.up, 4),
        ):
            b = self.blk(rid(o, self.x, self.c))
            wire.arrived(b, self.r + o, frm, cond)
            wire.send(b, b, self.s + base + o, self.r + o, to, cond & fwd)
            wire.send(b, b, self.s + 8 + o, self.r + 4 + o, self.side, cond)
            k = o * 2 + self.x
            wire.send(b, b, self.s + 12 + k, self.r + 8 + k, self.twin, cond)

    def across(self, s):
        z = self.z
        todo = ((z, None),) if s == 0 else ((z - s, z >= s), (z + s, z + s < ZN))
        for o, cond in todo:
            b = self.blk(rid(o, 1 - self.x, self.c))
            self.wire.arrived(b, self.r + 4 + o, self.side, cond)
            k = o * 2 + 1 - self.x
            self.wire.send(b, b, self.s + 12 + k, self.r + 8 + k, self.twin, cond)

    def finish(self):
        for o in range(ZN):
            for xx in (0, 1):
                b = self.blk(rid(o, xx, 1 - self.c))
                self.wire.arrived(b, self.r + 8 + o * 2 + xx, self.twin)


def front_kernel(
    resid_h, wq_l, wk_l, wv_l, wo_l, g1_l, g2_l, wg_h, wu_h, wd_h, cot_h, seg, freq,
    wqkv, wo, ga, w3, dres, n1, q, kv, ctx, mid, normed, cos_t, sin_t, mask,
    resid, wg_l, wu_l, cot, ga_l, qkv_l, w3_l, dres_l, kx, vx, attn, part, nrm, ss, rs, ls,
):
    z, x, c, y = place()
    units = w3.shape[1]
    seq, width = resid.shape
    q_width = q.shape[1]
    pairs = q_width // LANE
    loads = [
        pltpu.make_async_copy(cot_h, cot, ls.at[6]),
        pltpu.make_async_copy(wg_h.at[0], wg_l, ls.at[7]),
        pltpu.make_async_copy(wu_h.at[0], wu_l, ls.at[8]),
        pltpu.make_async_copy(wd_h.at[0], w3_l.at[2], ls.at[9]),
        pltpu.make_async_copy(resid_h, resid, ls.at[10]),
    ]
    for cp in loads:
        cp.start()
    wire = Wire(ss, rs)
    side, twin, other = dev(z, 1 - x, c, y), dev(z, x, 1 - c, y), dev(z, x, c, 1 - y)
    qkv_l[:, pl.ds(0, q_width)] = wq_l[0]
    qkv_l[:, pl.ds(q_width, LANE)] = wk_l[0]
    qkv_l[:, pl.ds(q_width + LANE, LANE)] = wv_l[0]
    row = lax.broadcasted_iota(jnp.int32, (16, LANE), 0)
    two = jnp.where(row == 0, g1_l[...].astype(F32), g2_l[...].astype(F32))
    ga_l[...] = jnp.where(row < 2, two, 0.0).astype(BF)
    greet(all_peers(z, x, c, y))

    def qkv_blk(r):
        return wqkv.at[pl.ds(pl.multiple_of(r * LANE, LANE), LANE), :]

    def wo_blk(r):
        return wo.at[:, lanes(r)]

    def ga_blk(r):
        return ga.at[:, lanes(r)]

    def ffn(r):
        return w3.at[:, :, lanes(r)]

    t_qkv = Tree(wire, qkv_l, qkv_blk, 0, 0)
    t_wo = Tree(wire, wo_l.at[0], wo_blk, 20, 16)
    t_ga = Tree(wire, ga_l, ga_blk, 40, 32)
    l_dres = Line(wire, dres_l, dres, 76, 64)
    l_norm = Line(wire, nrm, normed, 88, 72)
    mine = rid(z, x, c)
    t_ga.start()
    t_qkv.start()
    own = [
        pltpu.make_async_copy(qkv_l, qkv_blk(mine), ls.at[0]),
        pltpu.make_async_copy(wo_l.at[0], wo_blk(mine), ls.at[1]),
        pltpu.make_async_copy(ga_l, ga_blk(mine), ls.at[2]),
    ]
    for cp in own:
        cp.start()

    def round_cot(r):
        dres_l[r, :] = cot[r, :].astype(BF)

    def turn(i, carry):
        cut = lanes(i)
        w3_l[0, pl.ds(pl.multiple_of(i * LANE, LANE), LANE), :] = (
            wg_l[:, cut].astype(F32).T.astype(BF)
        )
        w3_l[1, pl.ds(pl.multiple_of(i * LANE, LANE), LANE), :] = (
            wu_l[:, cut].astype(F32).T.astype(BF)
        )
        return carry

    def turned(v):
        return v * cos_t[...] + swap_halves(v) * sin_t[...]

    def q_tile(j, carry):
        acc = dot_nn(n1[...], wqkv[:, lanes(j, 2 * LANE)])
        for h in (0, 1):
            q[:, lanes(2 * j + h)] = turned(acc[:, h * LANE : (h + 1) * LANE]).astype(BF)
        return carry

    def pair(p, carry):
        qp = q[:, lanes(p)]
        g = p // (pairs // 2)
        out = jnp.zeros((seq, LANE), F32)
        for h in (0, 1):
            s = dot_nt(qp, kx[2 * g + h]) * HD ** (-0.5)
            s = jnp.where(mask[...] > 0.0, s, masked_score)
            top = jnp.max(s, axis=-1, keepdims=True)
            lse = top + jnp.log(jnp.sum(jnp.exp(s - top), axis=-1, keepdims=True))
            out = out + dot_nn(jnp.exp(s - lse).astype(BF), vx[2 * g + h])
        ctx[:, lanes(p)] = out.astype(BF)
        return carry

    ids = jnp.broadcast_to(seg[...].astype(F32), (seq, seq))
    own_id = lax.broadcasted_iota(jnp.int32, (seq, seq), 0)
    key_id = lax.broadcasted_iota(jnp.int32, (seq, seq), 1)
    mine_id = jnp.sum(jnp.where(own_id == key_id, ids, 0.0), axis=1, keepdims=True)
    seen = jnp.where((ids == mine_id) & (key_id <= own_id), 1.0, 0.0)
    mask[...] = seen
    angles = (jnp.sum(seen, axis=1, keepdims=True) - 1.0) * freq[...]
    lane = lax.broadcasted_iota(jnp.int32, (seq, LANE), 1)
    cos_t[...] = jnp.cos(angles)
    sin_t[...] = jnp.where(lane % HD < HD // 2, -1.0, 1.0) * jnp.sin(angles)
    loads[0].wait()
    by_rows(seq, 16, round_cot)
    t_ga.relay(1)
    t_qkv.relay(1)
    t_ga.across(0)
    t_qkv.across(0)
    t_ga.relay(2)
    t_qkv.relay(2)
    t_wo.start_z()
    for cp in loads[1:]:
        cp.wait()
    lax.fori_loop(0, w3_l.shape[1] // LANE, turn, 0)
    t_ga.across(1)
    t_qkv.across(1)
    t_ga.relay(3)
    t_qkv.relay(3)
    t_wo.start_near()
    t_ga.across(2)
    t_ga.across(3)
    t_ga.finish()
    own[2].wait()
    gain_one = ga[pl.ds(0, 8), :].astype(F32)[0:1]
    gain_two = ga[pl.ds(0, 8), :].astype(F32)[1:2]

    def norm_one(r):
        v = resid[r, :]
        recip = lax.rsqrt(jnp.mean(v * v, axis=-1, keepdims=True) + epsilon)
        n1[r, :] = (v * recip * gain_one).astype(BF)

    by_rows(seq, 16, norm_one)
    t_wo.relay(1)
    t_qkv.across(2)
    t_wo.relay(2)
    l_dres.start()
    for d in (2, 1, 3):
        zt = (z + d) % ZN
        wire.send(w3_l.at[:, rows(zt, units), :], ffn(mine), 60 + d - 1, 48 + z, dev(zt, x, c, y))
    t_qkv.across(3)
    t_qkv.finish()
    own[0].wait()
    lax.fori_loop(0, pairs // 2, q_tile, 0)
    acc = dot_nn(n1[...], wqkv[:, pl.ds(q_width, 2 * LANE)])
    key = turned(acc[:, :LANE]).astype(BF)
    val = acc[:, LANE:].astype(BF)
    kv[:, pl.ds(0, LANE)] = key
    kv[:, pl.ds(LANE, LANE)] = val
    spread_pair(kx, key.astype(F32))
    spread_pair(vx, val.astype(F32))
    t_wo.across(0)
    t_wo.relay(3)
    mine3 = w3_l.at[:, rows(z, units), :]
    wire.send(mine3, ffn(mine), 64 + z, 52 + z, side)
    wire.send(mine3, ffn(mine), 68 + z * 2 + x, 56 + z * 2 + x, twin)
    own += [
        pltpu.make_async_copy(mine3, ffn(mine), ls.at[3]),
        pltpu.make_async_copy(dres_l, dres.at[rows(z, seq), :], ls.at[4]),
    ]
    own[3].start()
    own[4].start()
    lax.fori_loop(0, pairs, pair, 0)
    for s in (1, 2, 3):
        t_wo.across(s)
    t_wo.finish()
    own[1].wait()

    def out_tile(j, carry):
        cut = lanes(j, 2 * LANE)
        attn[:, cut] = dot_nn(ctx[...], wo[:, cut]).astype(BF)
        return carry

    lax.fori_loop(0, width // (2 * LANE), out_tile, 0)
    wire.send(attn, part, 100, 80, other)

    def ffn_in(d):
        o = (z + ZN - d) % ZN
        b = ffn(rid(o, x, c))
        wire.arrived(b, 48 + o, dev(o, x, c, y))
        wire.send(b, b, 64 + o, 52 + o, side)
        wire.send(b, b, 68 + o * 2 + x, 56 + o * 2 + x, twin)

    def ffn_across(d):
        o = (z + ZN - d) % ZN
        b = ffn(rid(o, 1 - x, c))
        wire.arrived(b, 52 + o, side)
        k = o * 2 + 1 - x
        wire.send(b, b, 68 + k, 56 + k, twin)

    def second(r):
        m = resid[r, :] + (attn[r, :].astype(F32) + part[r, :].astype(F32))
        mid[r, :] = m
        recip = lax.rsqrt(jnp.mean(m * m, axis=-1, keepdims=True) + epsilon)
        nrm[r, :] = (m * recip * gain_two).astype(BF)

    l_dres.relay(1)
    ffn_in(2)
    wire.arrived(part, 80, other)
    by_rows(seq, 16, second)
    l_norm.start()
    own.append(pltpu.make_async_copy(nrm, normed.at[rows(z, seq), :], ls.at[5]))
    own[5].start()
    l_dres.relay(2)
    ffn_in(1)
    ffn_across(0)
    l_norm.relay(1)
    ffn_in(3)
    l_dres.relay(3)
    l_norm.relay(2)
    l_norm.relay(3)
    for d in (2, 1, 3):
        ffn_across(d)
    for o in range(ZN):
        for xx in (0, 1):
            wire.arrived(ffn(rid(o, xx, 1 - c)), 56 + o * 2 + xx, twin)
    l_dres.finish()
    l_norm.finish()
    wire.drain()
    for cp in own[3:]:
        cp.wait()


def front(resid, w_query, w_key, w_value, w_out, g1, g2, w_gate, w_up, w_down, cot, seg):
    seq, width = resid.shape
    q_width, out_rows = w_query.shape[2], w_out.shape[1]
    total = q_width + 2 * LANE
    units = w_gate.shape[2] // ZN
    pair_shape = (4, seq, LANE)
    freq = rope_base ** (-(np.arange(LANE) % (HD // 2)) * 2.0 / HD)
    freq = jnp.asarray(freq[None].astype(np.float32))
    vm, hb = vm_spec(), any_spec()
    return pl.pallas_call(
        front_kernel,
        name="front",
        out_shape=(
            jax.ShapeDtypeStruct((width, total), BF),
            jax.ShapeDtypeStruct((out_rows, width), BF),
            jax.ShapeDtypeStruct((16, width), BF),
            jax.ShapeDtypeStruct((3, units, width), BF),
            jax.ShapeDtypeStruct((seq * ZN, width), BF),
            jax.ShapeDtypeStruct((seq, width), BF),
            jax.ShapeDtypeStruct((seq, q_width), BF),
            jax.ShapeDtypeStruct((seq, 2 * LANE), BF),
            jax.ShapeDtypeStruct((seq, q_width), BF),
            jax.ShapeDtypeStruct((seq, width), F32),
            jax.ShapeDtypeStruct((seq * ZN, width), BF),
            jax.ShapeDtypeStruct((seq, LANE), F32),
            jax.ShapeDtypeStruct((seq, LANE), F32),
            jax.ShapeDtypeStruct((seq, seq), F32),
        ),
        in_specs=[hb] + [vm] * 6 + [hb] * 4 + [vm] * 2,
        out_specs=[vm] * 3 + [hb] * 2 + [vm] * 5 + [hb] + [vm] * 3,
        scratch_shapes=[
            pltpu.VMEM((seq, width), F32),
            pltpu.VMEM((LANE, units * ZN), BF),
            pltpu.VMEM((LANE, units * ZN), BF),
            pltpu.VMEM((seq, width), F32),
            pltpu.VMEM((16, LANE), BF),
            pltpu.VMEM((LANE, total), BF),
            pltpu.VMEM((3, units * ZN, LANE), BF),
            pltpu.VMEM((seq, width), BF),
            pltpu.VMEM(pair_shape, BF),
            pltpu.VMEM(pair_shape, BF),
            pltpu.VMEM((seq, width), BF),
            pltpu.VMEM((seq, width), BF),
            pltpu.VMEM((seq, width), BF),
            sems(101),
            sems(81),
            sems(11),
        ],
        compiler_params=params(0),
    )(resid, w_query, w_key, w_value, w_out, g1, g2, w_gate, w_up, w_down, cot, seg, freq)


def add_into(dst, src, height, step):
    def one(r):
        dst[r, :] = (dst[r, :].astype(F32) + src[r, :].astype(F32)).astype(dst.dtype)

    by_rows(height, step, one)


class Chain:
    def __init__(self, wire, held, zin, height, step, send_base, recv_base):
        self.wire, self.held, self.zin = wire, held, zin
        self.height, self.step = height, step
        self.s, self.r = send_base, recv_base
        self.z, x, c, y = place()
        self.up, self.down = dev(self.z + 1, x, c, y), dev(self.z - 1, x, c, y)

    def inbound(self, o, slot, frm, cond):
        self.wire.arrived(self.zin(slot), self.r + slot, frm, cond)

        @pl.when(cond)
        def _():
            add_into(self.held(o), self.zin(slot), self.height, self.step)

    def outward(self, t, ready):
        z = self.z
        for o, cond, more, to, frm, base, slot in (
            (z + t, z + t < ZN, z > 0, self.up, self.down, 0, z + t),
            (z - t, z >= t, z < ZN - 1, self.down, self.up, 4, 4 if t == 1 else z - t),
        ):
            ready(o, cond)
            self.inbound(o, o, frm, cond & more)
            self.wire.send(
                self.held(o), self.zin(slot), self.s + base + o, self.r + slot, to, cond
            )

    def home(self):
        z = self.z
        self.inbound(z, z, self.down, z > 0)
        self.inbound(z, 4, self.up, z < ZN - 1)


class Fold:
    def __init__(self, wire, part, cin, xin, zin, height, step, send_base, recv_base):
        self.wire, self.part, self.cin, self.xin = wire, part, cin, xin
        self.height, self.step = height, step
        self.s, self.r = send_base, recv_base
        self.z, self.x, self.c, y = place()
        z, x, c = self.z, self.x, self.c
        self.side, self.twin = dev(z, 1 - x, c, y), dev(z, x, 1 - c, y)
        self.chain = Chain(
            wire, lambda o: xin.at[o], lambda s: zin.at[s], height, step, self.s + 12, self.r + 12
        )

    def order(self):
        return [(self.z + d) % ZN for d in (2, 1, 3, 0)]

    def to_twin(self):
        for xx in (1 - self.x, self.x):
            for o in self.order():
                k = o * 2 + xx
                self.wire.send(
                    self.part(k * 2 + 1 - self.c), self.cin.at[k], self.s + k, self.r + k, self.twin
                )

    def from_twin(self, k):
        self.wire.arrived(self.cin.at[k], self.r + k, self.twin)
        add_into(self.cin.at[k], self.part(k * 2 + self.c), self.height, self.step)

    def from_twin_if(self, k, cond):
        self.wire.arrived(self.cin.at[k], self.r + k, self.twin, cond)

        @pl.when(cond)
        def _():
            add_into(self.cin.at[k], self.part(k * 2 + self.c), self.height, self.step)

    def across_one(self, o, cond=None):
        k = o * 2 + 1 - self.x
        if cond is None:
            self.from_twin(k)
        else:
            self.from_twin_if(k, cond)
        self.wire.send(
            self.cin.at[k], self.xin.at[o], self.s + 8 + o, self.r + 8 + o, self.side, cond
        )

    def across(self):
        z = self.z
        for t in (3, 2, 1):
            self.across_one(z + t, z + t < ZN)
            self.across_one(z - t, z >= t)
        self.across_one(z)

    def stay(self):
        for o in self.order():
            self.from_twin(o * 2 + self.x)

    def ready(self, o, cond):
        self.wire.arrived(self.xin.at[o], self.r + 8 + o, self.side, cond)

        @pl.when(cond)
        def _():
            add_into(self.xin.at[o], self.cin.at[o * 2 + self.x], self.height, self.step)

    def outward(self, t):
        self.chain.outward(t, self.ready)

    def home(self):
        self.ready(self.z, self.z >= 0)
        self.chain.home()
        return self.xin.at[self.z]


def back_kernel(
    dn_p, feed_p, g3_p, wqkv, mid_h, cot_h, resid_h, ga_h, n1_h, q_h, kv_h, ctx_h, wo_h, cos_h,
    sin_h, mask_h,
    feed_out, grad_out, g3, gq_out, go_out, gains_out,
    mid, cot, resid, ga, n1, q, kv, ctx, wo, cos_t, sin_t, mask, grad_in, fown, yin, zin, gbuf, cin, xin, gq_p, go_p, gp, qc, qx, qz, oc, ox, oz, gc, gx, gz,
    dn, feed, mid_b, dctx, dqkv, dn1, dn1_o, kx, vx, kacc, vacc, wbuf, gs, gr, ss, rs, ls,
):
    z, x, c, y = place()
    units = g3_p.shape[1]
    seq, width = mid.shape
    half = width // 2
    q_width = q.shape[1]
    pairs = q_width // LANE
    out_rows = wo.shape[0]
    wire = Wire(ss, rs)
    side, twin, other = dev(z, 1 - x, c, y), dev(z, x, 1 - c, y), dev(z, x, c, 1 - y)
    ring = [(z + d) % ZN for d in (2, 1, 3, 0)]
    greet(all_peers(z, x, c, y))

    def y_out(src, k):
        for t in (3, 2, 1):
            for o, cond in ((z + t, z + t < ZN), (z - t, z >= t)):
                s = src.at[rows(o, seq), lanes(1 - y, half)]
                wire.send(s, yin.at[k, o], k * 4 + o, k * 4 + o, other, cond)
        s = src.at[rows(z, seq), lanes(1 - y, half)]
        wire.send(s, yin.at[k, z], k * 4 + z, k * 4 + z, other)

    y_out(dn_p, 0)

    def own_half(k, o):
        src = (dn_p, feed_p)[k]
        return pltpu.make_async_copy(
            src.at[rows(o, seq), lanes(y, half)], fown.at[k, o], ls.at[2 + k * 4 + o]
        )

    for o in range(ZN):
        own_half(0, o).start()
    for k in range(8):
        wire.send(g3_p.at[:, :, lanes(k * 2 + 1 - c)], cin.at[k], 26 + k, 20 + k, twin)
    ks = [o * 2 + 1 - x for o in ring] + [o * 2 + x for o in ring]

    def load(i):
        return pltpu.make_async_copy(
            g3_p.at[:, :, lanes(ks[i] * 2 + c)], gbuf.at[i % 2], ls.at[i % 2]
        )

    def add3(dst, src):
        for m in range(3):
            add_into(dst.at[m], src.at[m], units, 64)

    load(0).start()
    for i in range(8):
        if i < 7:
            load(i + 1).start()
        load(i).wait()
        wire.arrived(cin.at[ks[i]], 20 + ks[i], twin)
        add3(cin.at[ks[i]], gbuf.at[i % 2])
        if i < 4:
            o = ring[i]
            wire.send(cin.at[ks[i]], xin.at[o], 34 + o, 28 + o, side)
    pairs_in = (
        (wo_h, wo), (ga_h, ga), (kv_h, kv), (mask_h, mask), (mid_h, mid), (cot_h, cot), (n1_h, n1),
        (q_h, q), (ctx_h, ctx), (cos_h, cos_t), (sin_h, sin_t), (resid_h, resid),
    )
    inward = [
        pltpu.make_async_copy(a, b, ls.at[13 + i]) for i, (a, b) in enumerate(pairs_in)
    ]
    for cp in inward:
        cp.start()
    for o in range(ZN):
        own_half(1, o).start()
        own_half(0, o).wait()
    def chain_of(k):
        return Chain(
            wire, lambda o: yin.at[k, o], lambda s: zin.at[k, s], seq, 16, 8 + k * 8, 8 + k * 5
        )

    def dn_ready(o, cond):
        wire.arrived(yin.at[0, o], o, other, cond)

        @pl.when(cond)
        def _():
            add_into(yin.at[0, o], fown.at[0, o], seq, 16)

    line = chain_of(0)
    for t in (3, 2, 1):
        line.outward(t, dn_ready)
    dn_ready(z, z >= 0)
    line.home()
    blk = dn.at[:, lanes(y, half)]

    def keep_dn(r):
        dn[r, lanes(y, half)] = yin[0, z, r, :]

    by_rows(seq, 16, keep_dn)
    wire.send(blk, blk, 24, 18, other)
    y_out(feed_p, 1)

    def ffn_z(i):
        o = ring[i]
        wire.arrived(xin.at[o], 28 + o, side)
        add3(xin.at[o], cin.at[o * 2 + x])
        d = (2, 1, 3, 0)[i]
        if d:
            wire.send(xin.at[o], g3.at[:, rows(z, units), :], 38 + d - 1, 32 + z, dev(o, x, c, y))
        else:
            pltpu.make_async_copy(xin.at[o], g3.at[:, rows(z, units), :], ls.at[10]).start()

    ffn_z(0)
    ffn_z(1)
    for cp in inward:
        cp.wait()
    spread_pair(kx, kv[:, pl.ds(0, LANE)].astype(F32))
    spread_pair(vx, kv[:, pl.ds(LANE, LANE)].astype(F32))
    kacc[...] = jnp.zeros_like(kacc)
    vacc[...] = jnp.zeros_like(vacc)
    gp[...] = jnp.zeros_like(gp)
    gain_one = ga[pl.ds(0, 8), :].astype(F32)[0:1]
    gain_two = ga[pl.ds(0, 8), :].astype(F32)[1:2]
    wire.arrived(dn.at[:, lanes(1 - y, half)], 18, other)

    def norm_two(r):
        v, g = mid[r, :], dn[r, :].astype(F32)
        recip = lax.rsqrt(jnp.mean(v * v, axis=-1, keepdims=True) + epsilon)
        e = g * gain_two
        d = recip * e - v * (recip * recip * recip) * jnp.mean(e * v, axis=-1, keepdims=True)
        out = cot[r, :] + d
        grad_in[r, :] = out
        mid_b[r, :] = out.astype(BF)
        t = g * v * recip
        gp[pl.ds(8, 8), :] += t[:8] + t[8:]

    by_rows(seq, 16, norm_two)

    def out_grad(i, carry):
        cut = lanes(i, 2 * LANE)
        for h in range(2):
            hh = pl.ds(h * (out_rows // 2), out_rows // 2)
            go_p[hh, cut] = dot_tn(ctx[:, hh], mid_b[:, cut]).astype(BF)
        return carry

    lax.fori_loop(0, width // (2 * LANE), out_grad, 0)
    f_o = Fold(wire, lambda r: go_p.at[:, lanes(r)], oc, ox, oz, out_rows, 64, 61, 53)
    f_q = Fold(
        wire,
        lambda r: gq_p.at[pl.ds(pl.multiple_of(r * LANE, LANE), LANE), :],
        qc, qx, qz, LANE, 16, 41, 36,
    )
    f_g = Fold(wire, lambda r: gp.at[:, lanes(r)], gc, gx, gz, 16, 16, 81, 70)
    f_o.to_twin()

    def ctx_grad(j, carry):
        cut = lanes(j, 2 * LANE)
        dctx[:, cut] = dot_nt(mid_b[...], wo[cut, :]).astype(BF)
        return carry

    lax.fori_loop(0, q_width // (2 * LANE), ctx_grad, 0)
    ffn_z(2)
    ffn_z(3)
    f_o.across()

    def back_turned(v):
        return v * cos_t[...] - swap_halves(v) * sin_t[...]

    def pair(p, carry):
        qp, dc = q[:, lanes(p)], dctx[:, lanes(p)]
        g = p // (pairs // 2)
        prod = dc.astype(F32) * ctx[:, lanes(p)].astype(F32)
        low = lax.broadcasted_iota(jnp.int32, prod.shape, 1) < HD
        dq = jnp.zeros((seq, LANE), F32)
        for h in (0, 1):
            i = 2 * g + h
            s = dot_nt(qp, kx[i]) * HD ** (-0.5)
            s = jnp.where(mask[...] > 0.0, s, masked_score)
            top = jnp.max(s, axis=-1, keepdims=True)
            lse = top + jnp.log(jnp.sum(jnp.exp(s - top), axis=-1, keepdims=True))
            full = jnp.exp(s - lse)
            delta = jnp.sum(jnp.where(low if h == 0 else ~low, prod, 0.0), axis=-1, keepdims=True)
            ds = (full * (dot_nt(dc, vx[i]) - delta)).astype(BF)
            dq = dq + dot_nn(ds, kx[i])
            kacc[i] += dot_tn(ds, qp)
            vacc[i] += dot_tn(full.astype(BF), dc)
        dqkv[:, lanes(p)] = back_turned(dq * HD ** (-0.5)).astype(BF)
        return carry

    lax.fori_loop(0, pairs, pair, 0)

    def joined(acc):
        low = lax.broadcasted_iota(jnp.int32, (seq, LANE), 1) < HD
        return jnp.where(
            low, acc[0] + pltpu.roll(acc[1], HD, 1), acc[3] + pltpu.roll(acc[2], HD, 1)
        )

    dqkv[:, pl.ds(q_width, LANE)] = back_turned(joined(kacc) * HD ** (-0.5)).astype(BF)
    dqkv[:, pl.ds(q_width + LANE, LANE)] = joined(vacc).astype(BF)

    def w_tile(j, slot):
        r = pl.ds(pl.multiple_of(j * 2 * LANE, 2 * LANE), 2 * LANE)
        return pltpu.make_async_copy(wqkv.at[r, :], wbuf.at[slot], ls.at[11 + slot])

    w_tile(0, 0).start()

    def in_grad(r, carry):
        gq_p[pl.ds(pl.multiple_of(r * LANE, LANE), LANE), :] = dot_tn(
            n1[:, lanes(r)], dqkv[...]
        ).astype(BF)
        return carry

    lax.fori_loop(0, width // LANE, in_grad, 0)
    f_q.to_twin()
    f_q.across()
    tiles = width // (2 * LANE)
    for j in range(tiles):
        if j + 1 < tiles:
            w_tile(j + 1, (j + 1) % 2).start()
        w_tile(j, j % 2).wait()
        dn1[:, pl.ds(j * 2 * LANE, 2 * LANE)] = dot_nt(dqkv[...], wbuf[j % 2]).astype(BF)
    wire.send(dn1, dn1_o, 101, 87, other)

    def gain_part(r):
        v = resid[r, :]
        recip = lax.rsqrt(jnp.mean(v * v, axis=-1, keepdims=True) + epsilon)
        t = dn1[r, :].astype(F32) * v * recip
        gp[pl.ds(0, 8), :] += t[:8] + t[8:]

    by_rows(seq, 16, gain_part)
    f_g.to_twin()
    f_g.across()
    f_o.stay()
    for t in (3, 2, 1):
        f_o.outward(t)

    for o in range(ZN):
        own_half(1, o).wait()

    def feed_ready(o, cond):
        wire.arrived(yin.at[1, o], 4 + o, other, cond)

        @pl.when(cond)
        def _():
            add_into(yin.at[1, o], fown.at[1, o], seq, 16)

    line = chain_of(1)
    for t in (3, 2, 1):
        line.outward(t, feed_ready)
    f_q.stay()
    f_g.stay()
    for t in (3, 2, 1):
        f_q.outward(t)
        f_g.outward(t)
    feed_ready(z, z >= 0)
    line.home()
    fb = feed.at[:, lanes(y, half)]

    def keep_feed(r):
        feed[r, lanes(y, half)] = yin[1, z, r, :]

    by_rows(seq, 16, keep_feed)
    wire.send(fb, fb, 25, 19, other)
    wire.arrived(dn1_o, 87, other)

    def norm_one(r):
        v = resid[r, :]
        g = dn1[r, :].astype(F32) + dn1_o[r, :].astype(F32)
        recip = lax.rsqrt(jnp.mean(v * v, axis=-1, keepdims=True) + epsilon)
        e = g * gain_one
        d = recip * e - v * (recip * recip * recip) * jnp.mean(e * v, axis=-1, keepdims=True)
        grad_in[r, :] += d

    by_rows(seq, 16, norm_one)
    outward = [pltpu.make_async_copy(grad_in, grad_out, ls.at[25])]
    outward[0].start()
    done = f_o.home()
    outward.append(pltpu.make_async_copy(done, go_out, ls.at[26]))
    outward[1].start()
    mine = f_g.home()
    gs[...] = mine[...]
    wire.send(gs, gr, 102, 88, other)
    got = f_q.home()
    outward.append(pltpu.make_async_copy(got, gq_out, ls.at[27]))
    outward[2].start()
    wire.arrived(feed.at[:, lanes(1 - y, half)], 19, other)
    outward.append(pltpu.make_async_copy(feed, feed_out, ls.at[28]))
    outward[3].start()
    wire.arrived(gr, 88, other)
    first = jnp.sum(gs[pl.ds(0, 8), :] + gr[pl.ds(0, 8), :], axis=0, keepdims=True)
    second = jnp.sum(gs[pl.ds(8, 8), :], axis=0, keepdims=True)
    row = lax.broadcasted_iota(jnp.int32, (8, LANE), 0)
    gains_out[...] = jnp.where(row == 0, first, second)
    for d in (1, 2, 3):
        o = (z + ZN - d) % ZN
        wire.arrived(g3.at[:, rows(o, units), :], 32 + o, dev(o, x, c, y))
    wire.drain()
    pltpu.make_async_copy(xin.at[z], g3.at[:, rows(z, units), :], ls.at[10]).wait()
    for cp in outward:
        cp.wait()


def back(dn_p, feed_p, g3_p, wqkv, mid, cot, resid, ga, n1, q, kv, ctx, wo, cos_t, sin_t, mask):
    seq, width = mid.shape
    units = g3_p.shape[1]
    q_width, total = q.shape[1], wqkv.shape[1]
    out_rows = wo.shape[0]
    half = width // 2

    def vm(*shape, dtype=BF):
        return pltpu.VMEM(shape, dtype)

    held = (mid, cot, resid, ga, n1, q, kv, ctx, wo, cos_t, sin_t, mask)
    return pl.pallas_call(
        back_kernel,
        name="back",
        out_shape=(
            jax.ShapeDtypeStruct((seq, width), BF),
            jax.ShapeDtypeStruct((seq, width), F32),
            jax.ShapeDtypeStruct((3, units * ZN, LANE), BF),
            jax.ShapeDtypeStruct((LANE, total), BF),
            jax.ShapeDtypeStruct((out_rows, LANE), BF),
            jax.ShapeDtypeStruct((8, LANE), F32),
        ),
        in_specs=[any_spec()] * 16,
        out_specs=[any_spec()] * 5 + [vm_spec()],
        scratch_shapes=[vm(*a.shape, dtype=a.dtype) for a in held]
        + [
            vm(seq, width, dtype=F32),
            vm(2, ZN, seq, half),
            vm(2, ZN, seq, half),
            vm(2, 5, seq, half),
            vm(2, 3, units, LANE),
            vm(8, 3, units, LANE),
            vm(4, 3, units, LANE),
            vm(width, total),
            vm(out_rows, width),
            vm(16, width, dtype=F32),
            vm(8, LANE, total),
            vm(4, LANE, total),
            vm(5, LANE, total),
            vm(8, out_rows, LANE),
            vm(4, out_rows, LANE),
            vm(5, out_rows, LANE),
            vm(8, 16, LANE, dtype=F32),
            vm(4, 16, LANE, dtype=F32),
            vm(5, 16, LANE, dtype=F32),
            vm(seq, width),
            vm(seq, width),
            vm(seq, width),
            vm(seq, q_width),
            vm(seq, total),
            vm(seq, width),
            vm(seq, width),
            vm(4, seq, LANE),
            vm(4, seq, LANE),
            vm(4, seq, LANE, dtype=F32),
            vm(4, seq, LANE, dtype=F32),
            vm(2, 2 * LANE, total),
            vm(16, LANE, dtype=F32),
            vm(16, LANE, dtype=F32),
            sems(103),
            sems(89),
            sems(29),
        ],
        compiler_params=pltpu.CompilerParams(
            collective_id=1, has_side_effects=True, vmem_limit_bytes=67043328
        ),
    )(dn_p, feed_p, g3_p, wqkv, *held)


def finish_kernel(
    mid_h, feed_h, grad_h, g3_h, gq_h, go_h, gains,
    hidden, grad_in, wg, wu, wd, wq, wk, wv, wo, first, second,
    mid, feed, grad, g3, gq, go, tg, td, tq, to, ls,
):
    q_width = wq.shape[2]
    units = td.shape[0]
    into = [
        pltpu.make_async_copy(a, b, ls.at[i])
        for i, (a, b) in enumerate(
            ((g3_h, g3), (mid_h, mid), (feed_h, feed), (gq_h, gq), (go_h, go), (grad_h, grad))
        )
    ]
    for cp in into:
        cp.start()
    first[...] = gains[pl.ds(0, 1), :]
    second[...] = gains[pl.ds(1, 1), :]
    out = []

    def put(src, dst):
        cp = pltpu.make_async_copy(src, dst, ls.at[6 + len(out)])
        cp.start()
        out.append(cp)

    into[0].wait()
    for m, dst in ((0, wg), (1, wu)):

        def turn(i, carry):
            r = pl.ds(pl.multiple_of(i * LANE, LANE), LANE)
            tg[m, :, lanes(i)] = g3[m, r, :].astype(F32).T
            return carry

        lax.fori_loop(0, units // LANE, turn, 0)
        put(tg.at[m], dst.at[0])

    def wide(r):
        td[r, :] = g3[2, r, :].astype(F32)

    by_rows(units, 64, wide)
    put(td, wd.at[0])
    into[1].wait()
    into[2].wait()

    def total(r):
        mid[r, :] += feed[r, :].astype(F32)

    by_rows(mid.shape[0], 16, total)
    put(mid, hidden)
    into[3].wait()

    def wide_q(r):
        tq[r, :] = gq[r, :].astype(F32)

    by_rows(LANE, 16, wide_q)
    put(tq.at[:, pl.ds(0, q_width)], wq.at[0])
    put(tq.at[:, pl.ds(q_width, LANE)], wk.at[0])
    put(tq.at[:, pl.ds(q_width + LANE, LANE)], wv.at[0])
    into[4].wait()

    def wide_o(r):
        to[r, :] = go[r, :].astype(F32)

    by_rows(to.shape[0], 64, wide_o)
    put(to, wo.at[0])
    into[5].wait()
    put(grad, grad_in)
    for cp in out:
        cp.wait()


def finish(mid, feed, grad, g3, gq, go, gains):
    seq, width = mid.shape
    units = g3.shape[1]
    q_width = gq.shape[1] - 2 * LANE
    f32 = lambda *shape: jax.ShapeDtypeStruct(shape, F32)
    ins = (mid, feed, grad, g3, gq, go)
    return pl.pallas_call(
        finish_kernel,
        name="finish",
        out_shape=(
            f32(seq, width),
            f32(seq, width),
            f32(1, LANE, units),
            f32(1, LANE, units),
            f32(1, units, LANE),
            f32(1, LANE, q_width),
            f32(1, LANE, LANE),
            f32(1, LANE, LANE),
            f32(1, go.shape[0], LANE),
            f32(1, LANE),
            f32(1, LANE),
        ),
        in_specs=[any_spec()] * 6 + [vm_spec()],
        out_specs=[any_spec()] * 9 + [vm_spec()] * 2,
        scratch_shapes=[pltpu.VMEM(a.shape, a.dtype) for a in ins]
        + [
            pltpu.VMEM((2, LANE, units), F32),
            pltpu.VMEM((units, LANE), F32),
            pltpu.VMEM(gq.shape, F32),
            pltpu.VMEM(go.shape, F32),
            sems(15),
        ],
        compiler_params=pltpu.CompilerParams(vmem_limit_bytes=67043328),
    )(*ins, gains)


def fast_body(
    hidden_in,
    segment_ids,
    gain_attn,
    w_query,
    w_key,
    w_value,
    w_out,
    gain_ffn,
    w_gate,
    w_up,
    w_down,
    cotangent,
):
    resid = hidden_in
    wqkv, wo, ga, w3, dres_all, n1, q, kv, ctx, middle, normed_all, cos_w, sin_w, mask = front(
        resid, w_query, w_key, w_value, w_out, gain_attn, gain_ffn, w_gate, w_up, w_down,
        cotangent, segment_ids,
    )
    gate = contract_cols(normed_all, w3[0])
    up_proj = contract_cols(normed_all, w3[1])
    sigma = jax.nn.sigmoid(gate)
    hidden_act = (gate * sigma * up_proj).astype(BF)
    grad_hidden = contract_cols(dres_all, w3[2])
    grad_gate_b = (grad_hidden * up_proj * sigma * (1.0 + gate * (1.0 - sigma))).astype(BF)
    grad_up_b = (grad_hidden * (gate * sigma)).astype(BF)
    feed_p = jnp.dot(hidden_act, w3[2], preferred_element_type=F32).astype(BF)
    dn_p = (
        jnp.dot(grad_gate_b, w3[0], preferred_element_type=F32)
        + jnp.dot(grad_up_b, w3[1], preferred_element_type=F32)
    ).astype(BF)
    g3_p = jnp.stack(
        [
            contract_rows(grad_gate_b, normed_all).astype(BF),
            contract_rows(grad_up_b, normed_all).astype(BF),
            contract_rows(hidden_act, dres_all).astype(BF),
        ]
    )
    feed, grad_b, g3, gq, go, gains_g = back(
        dn_p, feed_p, g3_p, wqkv, middle, cotangent, resid, ga, n1, q, kv, ctx, wo,
        cos_w, sin_w, mask,
    )
    hidden_out, grad_input, wg, wu, wd, wq, wk, wv, wo_g, first, second = finish(
        middle, feed, grad_b, g3, gq, go, gains_g
    )
    return (
        hidden_out,
        grad_input,
        first,
        wq,
        wk,
        wv,
        wo_g,
        second,
        wg,
        wu,
        wd,
    )


def solution(mesh):
    small = mesh.shape["dp"] == 16 and mesh.shape["tensor"] == 2
    chosen = fast_body if small else body
    return jax.shard_map(
        chosen,
        mesh=mesh,
        in_specs=(
            P("dp", None),
            P("dp", None),
            P(None, "dp"),
            P(None, "dp", "tensor"),
            P(None, "dp", "tensor"),
            P(None, "dp", "tensor"),
            P(None, "tensor", "dp"),
            P(None, "dp"),
            P(None, "dp", "tensor"),
            P(None, "dp", "tensor"),
            P(None, "tensor", "dp"),
            P("dp", None),
        ),
        out_specs=(
            P("dp", None),
            P("dp", None),
            P(None, "dp"),
            P(None, "dp", "tensor"),
            P(None, "dp", "tensor"),
            P(None, "dp", "tensor"),
            P(None, "tensor", "dp"),
            P(None, "dp"),
            P(None, "dp", "tensor"),
            P(None, "dp", "tensor"),
            P(None, "tensor", "dp"),
        ),
        check_vma=False,
    )
```

```python
import jax
import jax.numpy as jnp
import numpy as np
from jax import lax
from jax.experimental import pallas as pl
from jax.experimental.pallas import tpu as pltpu
from jax.sharding import PartitionSpec as P

HD = 64


epsilon = 1e-05
rope_base = 10000.0
masked_score = -1e30


def segment_positions(segment_ids):
    row_count, seq_len = segment_ids.shape
    index_grid = lax.broadcasted_iota(jnp.int32, (row_count, seq_len), 1)
    previous = jnp.concatenate([segment_ids[:, :1] - 1, segment_ids[:, :-1]], axis=1)
    starts = jnp.where(segment_ids != previous, index_grid, 0)
    return index_grid - lax.cummax(starts, axis=1)


def rope_tables(positions):
    half_dim = HD // 2
    inv_freq = rope_base ** (-(jnp.arange(half_dim, dtype=jnp.float32) * 2.0 / HD))
    angles = positions.astype(jnp.float32)[:, :, None] * inv_freq
    return (jnp.cos(angles), jnp.sin(angles))


def expand_table(table, values):
    extra_dims = values.ndim - 3
    return table.reshape(table.shape[:2] + (1,) * extra_dims + table.shape[2:])


def rotate_pairs(values, cos_t, sin_t):
    half_dim = values.shape[-1] // 2
    cos_e = expand_table(cos_t, values)
    sin_e = expand_table(sin_t, values)
    first, second = (values[..., :half_dim], values[..., half_dim:])
    return jnp.concatenate(
        [first * cos_e - second * sin_e, second * cos_e + first * sin_e], axis=-1
    )


def unrotate_pairs(values, cos_t, sin_t):
    half_dim = values.shape[-1] // 2
    cos_e = expand_table(cos_t, values)
    sin_e = expand_table(sin_t, values)
    first, second = (values[..., :half_dim], values[..., half_dim:])
    return jnp.concatenate(
        [first * cos_e + second * sin_e, second * cos_e - first * sin_e], axis=-1
    )


def attention_mask(segment_ids):
    seq_len = segment_ids.shape[1]
    same_seg = segment_ids[:, :, None] == segment_ids[:, None, :]
    query_pos = lax.broadcasted_iota(jnp.int32, (seq_len, seq_len), 0)
    key_pos = lax.broadcasted_iota(jnp.int32, (seq_len, seq_len), 1)
    return (same_seg & (key_pos <= query_pos))[:, None, None, :, :]


def score_block(query_heads, key_heads, allowed):
    scores = jnp.einsum(
        "rikgd,rjkd->rkgij", query_heads, key_heads, preferred_element_type=jnp.float32
    ) * HD ** (-0.5)
    return jnp.where(allowed, scores, masked_score)


def attend(query_heads, key_heads, value_heads, allowed):
    scores = score_block(query_heads, key_heads, allowed)
    row_max = jnp.max(scores, axis=-1, keepdims=True)
    log_norm = row_max + jnp.log(jnp.sum(jnp.exp(scores - row_max), axis=-1, keepdims=True))
    attn_probs = jnp.exp(scores - log_norm).astype(jnp.bfloat16)
    context = jnp.einsum(
        "rkgij,rjkd->rikgd", attn_probs, value_heads, preferred_element_type=jnp.float32
    )
    return (context.astype(jnp.bfloat16), log_norm)


def attend_back(query_heads, key_heads, value_heads, context, log_norm, grad_context, allowed):
    scores = score_block(query_heads, key_heads, allowed)
    probs_full = jnp.exp(scores - log_norm)
    probs_b = probs_full.astype(jnp.bfloat16)
    grad_v = jnp.einsum(
        "rkgij,rikgd->rjkd", probs_b, grad_context, preferred_element_type=jnp.float32
    )
    grad_probs = jnp.einsum(
        "rikgd,rjkd->rkgij", grad_context, value_heads, preferred_element_type=jnp.float32
    )
    delta = jnp.sum(grad_context.astype(jnp.float32) * context.astype(jnp.float32), axis=-1)
    delta = jnp.transpose(delta, (0, 2, 3, 1))[..., None]
    grad_scores = (probs_full * (grad_probs - delta)).astype(jnp.bfloat16)
    grad_q = jnp.einsum(
        "rkgij,rjkd->rikgd", grad_scores, key_heads, preferred_element_type=jnp.float32
    ) * HD ** (-0.5)
    grad_k = jnp.einsum(
        "rkgij,rikgd->rjkd", grad_scores, query_heads, preferred_element_type=jnp.float32
    ) * HD ** (-0.5)
    return (grad_q, grad_k, grad_v)


def contract_rows(left, right):
    return lax.dot_general(
        left, right, (((0,), (0,)), ((), ())), preferred_element_type=jnp.float32
    )


def contract_cols(left, right):
    return lax.dot_general(
        left, right, (((1,), (1,)), ((), ())), preferred_element_type=jnp.float32
    )


def norm_backward(resid, recip, gain, grad_normed):
    scaled = grad_normed * gain.astype(jnp.float32)
    grad_gain = jnp.sum(grad_normed * resid * recip, axis=0)
    grad_resid = recip * scaled - resid * (recip * recip * recip) * jnp.mean(
        scaled * resid, axis=-1, keepdims=True
    )
    return (grad_gain, grad_resid)


def layer_forward(resid, weights, cos_t, sin_t, allowed):
    gain_one, w_query, w_key, w_value, w_out, gain_two, w_gate, w_up, w_down = weights
    row_count, seq_len = (cos_t.shape[0], cos_t.shape[1])
    heads_here = w_query.shape[1] // HD
    kv_here = w_key.shape[1] // HD
    group_size = heads_here // kv_here
    recip_one = lax.rsqrt(jnp.mean(resid * resid, axis=-1, keepdims=True) + epsilon)
    normed_one = (resid * recip_one * gain_one.astype(jnp.float32)).astype(jnp.bfloat16)
    query_raw = jnp.dot(normed_one, w_query, preferred_element_type=jnp.float32)
    query_heads = rotate_pairs(
        query_raw.reshape(row_count, seq_len, kv_here, group_size, HD), cos_t, sin_t
    ).astype(jnp.bfloat16)
    key_raw = jnp.dot(normed_one, w_key, preferred_element_type=jnp.float32)
    key_heads = rotate_pairs(key_raw.reshape(row_count, seq_len, kv_here, HD), cos_t, sin_t).astype(
        jnp.bfloat16
    )
    value_raw = jnp.dot(normed_one, w_value, preferred_element_type=jnp.float32)
    value_heads = value_raw.reshape(row_count, seq_len, kv_here, HD).astype(jnp.bfloat16)
    context, log_norm = attend(query_heads, key_heads, value_heads, allowed)
    context_flat = context.reshape(row_count * seq_len, heads_here * HD)
    attn_sum = lax.psum(jnp.dot(context_flat, w_out, preferred_element_type=jnp.float32), "tensor")
    middle = resid + attn_sum
    recip_two = lax.rsqrt(jnp.mean(middle * middle, axis=-1, keepdims=True) + epsilon)
    normed_two = (middle * recip_two * gain_two.astype(jnp.float32)).astype(jnp.bfloat16)
    gate = jnp.dot(normed_two, w_gate, preferred_element_type=jnp.float32)
    up_proj = jnp.dot(normed_two, w_up, preferred_element_type=jnp.float32)
    hidden_act = (jax.nn.silu(gate) * up_proj).astype(jnp.bfloat16)
    feed_out = lax.psum(jnp.dot(hidden_act, w_down, preferred_element_type=jnp.float32), "tensor")
    kept_state = (
        resid,
        recip_one,
        normed_one,
        query_heads,
        key_heads,
        value_heads,
        context,
        log_norm,
        middle,
        recip_two,
        normed_two,
        gate,
        up_proj,
        hidden_act,
    )
    return (middle + feed_out, kept_state)


def backward_layer(grad_resid, kept_state, weights, cos_t, sin_t, allowed):
    (
        resid,
        recip_one,
        normed_one,
        query_heads,
        key_heads,
        value_heads,
        context,
        log_norm,
        middle,
        recip_two,
        normed_two,
        gate,
        up_proj,
        hidden_act,
    ) = kept_state
    gain_one, w_query, w_key, w_value, w_out, gain_two, w_gate, w_up, w_down = weights
    token_count = resid.shape[0]
    grad_b = grad_resid.astype(jnp.bfloat16)
    grad_down = contract_rows(hidden_act, grad_b)
    grad_hidden = contract_cols(grad_b, w_down)
    sigma = jax.nn.sigmoid(gate)
    grad_gate_b = (grad_hidden * up_proj * sigma * (1.0 + gate * (1.0 - sigma))).astype(
        jnp.bfloat16
    )
    grad_up_b = (grad_hidden * (gate * sigma)).astype(jnp.bfloat16)
    grad_gate_w = contract_rows(normed_two, grad_gate_b)
    grad_up_w = contract_rows(normed_two, grad_up_b)
    grad_normed_two = lax.psum(
        contract_cols(grad_gate_b, w_gate) + contract_cols(grad_up_b, w_up), "tensor"
    )
    grad_gain_two, grad_mid_norm = norm_backward(middle, recip_two, gain_two, grad_normed_two)
    grad_middle = grad_resid + grad_mid_norm
    middle_b = grad_middle.astype(jnp.bfloat16)
    context_flat = context.reshape(token_count, -1)
    grad_out_w = contract_rows(context_flat, middle_b)
    grad_context = contract_cols(middle_b, w_out).astype(jnp.bfloat16).reshape(context.shape)
    grad_q, grad_k, grad_v = attend_back(
        query_heads, key_heads, value_heads, context, log_norm, grad_context, allowed
    )
    grad_q = unrotate_pairs(grad_q, cos_t, sin_t).astype(jnp.bfloat16).reshape(token_count, -1)
    grad_k = unrotate_pairs(grad_k, cos_t, sin_t).astype(jnp.bfloat16).reshape(token_count, -1)
    grad_v = grad_v.astype(jnp.bfloat16).reshape(token_count, -1)
    grad_query_w = contract_rows(normed_one, grad_q)
    grad_key_w = contract_rows(normed_one, grad_k)
    grad_value_w = contract_rows(normed_one, grad_v)
    grad_normed_one = lax.psum(
        contract_cols(grad_q, w_query)
        + contract_cols(grad_k, w_key)
        + contract_cols(grad_v, w_value),
        "tensor",
    )
    grad_gain_one, grad_res_norm = norm_backward(resid, recip_one, gain_one, grad_normed_one)
    grad_input = grad_middle + grad_res_norm
    layer_grads = (
        lax.psum_scatter(grad_gain_one, "dp", scatter_dimension=0, tiled=True),
        lax.psum_scatter(grad_query_w, "dp", scatter_dimension=0, tiled=True),
        lax.psum_scatter(grad_key_w, "dp", scatter_dimension=0, tiled=True),
        lax.psum_scatter(grad_value_w, "dp", scatter_dimension=0, tiled=True),
        lax.psum_scatter(grad_out_w, "dp", scatter_dimension=1, tiled=True),
        lax.psum_scatter(grad_gain_two, "dp", scatter_dimension=0, tiled=True),
        lax.psum_scatter(grad_gate_w, "dp", scatter_dimension=0, tiled=True),
        lax.psum_scatter(grad_up_w, "dp", scatter_dimension=0, tiled=True),
        lax.psum_scatter(grad_down, "dp", scatter_dimension=1, tiled=True),
    )
    return (grad_input, tuple(layer_grads))


def body(
    hidden_in,
    segment_ids,
    gain_attn,
    w_query,
    w_key,
    w_value,
    w_out,
    gain_ffn,
    w_gate,
    w_up,
    w_down,
    cotangent,
):
    cos_t, sin_t = rope_tables(segment_positions(segment_ids))
    allowed = attention_mask(segment_ids)
    layer_count = w_query.shape[0]
    resid = hidden_in
    retained = []
    layer_no = 0
    gathered = (
        lax.all_gather(gain_attn[layer_no], "dp", axis=0, tiled=True),
        lax.all_gather(w_query[layer_no], "dp", axis=0, tiled=True),
        lax.all_gather(w_key[layer_no], "dp", axis=0, tiled=True),
        lax.all_gather(w_value[layer_no], "dp", axis=0, tiled=True),
        lax.all_gather(w_out[layer_no], "dp", axis=1, tiled=True),
        lax.all_gather(gain_ffn[layer_no], "dp", axis=0, tiled=True),
        lax.all_gather(w_gate[layer_no], "dp", axis=0, tiled=True),
        lax.all_gather(w_up[layer_no], "dp", axis=0, tiled=True),
        lax.all_gather(w_down[layer_no], "dp", axis=1, tiled=True),
    )
    retained.append(gathered)
    resid, kept_state = layer_forward(resid, gathered, cos_t, sin_t, allowed)
    states = [kept_state]
    grad_resid = cotangent
    collected = [None] * layer_count
    for layer_no in reversed(range(layer_count)):
        gathered = (
            lax.all_gather(gain_attn[layer_no], "dp", axis=0, tiled=True),
            lax.all_gather(w_query[layer_no], "dp", axis=0, tiled=True),
            lax.all_gather(w_key[layer_no], "dp", axis=0, tiled=True),
            lax.all_gather(w_value[layer_no], "dp", axis=0, tiled=True),
            lax.all_gather(w_out[layer_no], "dp", axis=1, tiled=True),
            lax.all_gather(gain_ffn[layer_no], "dp", axis=0, tiled=True),
            lax.all_gather(w_gate[layer_no], "dp", axis=0, tiled=True),
            lax.all_gather(w_up[layer_no], "dp", axis=0, tiled=True),
            lax.all_gather(w_down[layer_no], "dp", axis=1, tiled=True),
        )
        grad_resid, collected[layer_no] = backward_layer(
            grad_resid, states[layer_no], gathered, cos_t, sin_t, allowed
        )
    stacked = tuple((jnp.stack([collected[0][member]]) for member in range(9)))
    return (
        resid,
        grad_resid,
        stacked[0],
        stacked[1],
        stacked[2],
        stacked[3],
        stacked[4],
        stacked[5],
        stacked[6],
        stacked[7],
        stacked[8],
    )


ZN = 4
MESH = pl.DeviceIdType.MESH
BF = jnp.bfloat16
F32 = jnp.float32
LANE = 128


def place():
    dp = lax.axis_index("dp")
    return dp // 4, (dp // 2) % 2, dp % 2, lax.axis_index("tensor")


def dev(z, x, c, y):
    return (z * 4 + x * 2 + c, y)


def rid(z, x, c):
    return (z * 2 + x) * 2 + c


def lanes(r, width=LANE):
    return pl.ds(pl.multiple_of(r * width, LANE), width)


def rows(r, height):
    return pl.ds(pl.multiple_of(r * height, 16), height)


def tokens(o, pitch, count):
    return pl.ds(pl.multiple_of(o * pitch, 16), count)


def greet(peers):
    barrier = pltpu.get_barrier_semaphore()
    for peer in peers:
        pl.semaphore_signal(barrier, inc=1, device_id=peer, device_id_type=MESH)
    pl.semaphore_wait(barrier, len(peers))


class Wire:
    def __init__(self, send_sem, recv_sem):
        self.send_sem = send_sem
        self.recv_sem = recv_sem
        self.started = []

    def make(self, src, dst, si, ri, to):
        return pltpu.make_async_remote_copy(
            src_ref=src,
            dst_ref=dst,
            send_sem=self.send_sem.at[si],
            recv_sem=self.recv_sem.at[ri],
            device_id=to,
            device_id_type=MESH,
        )

    def send(self, src, dst, si, ri, to, cond=None):
        def go():
            self.make(src, dst, si, ri, to).start()

        def done():
            self.make(src, dst, si, ri, to).wait_send()

        if cond is None:
            go()
            self.started.append(done)
        else:
            pl.when(cond)(go)
            self.started.append(lambda: pl.when(cond)(done))

    def arrived(self, dst, ri, to, cond=None):
        def wait():
            self.make(dst, dst, 0, ri, to).wait_recv()

        if cond is None:
            wait()
        else:
            pl.when(cond)(wait)

    def drain(self):
        for done in self.started:
            done()


def all_peers(z, x, c, y):
    near = [dev(z, x, 1 - c, y), dev(z, 1 - x, c, y), dev(z, x, c, 1 - y)]
    return near + [dev((z + d) % ZN, x, c, y) for d in (1, 2, 3)]


def params(cid):
    return pltpu.CompilerParams(
        collective_id=cid, has_side_effects=True, vmem_limit_bytes=67043328
    )


def any_spec():
    return pl.BlockSpec(memory_space=pl.ANY)


def vm_spec():
    return pl.BlockSpec(memory_space=pltpu.VMEM)


def sems(n):
    return pltpu.SemaphoreType.DMA((n,))


def dot_nn(a, b):
    return lax.dot_general(a, b, (((1,), (0,)), ((), ())), preferred_element_type=F32)


def dot_nt(a, b):
    return lax.dot_general(a, b, (((1,), (1,)), ((), ())), preferred_element_type=F32)


def dot_tn(a, b):
    return lax.dot_general(a, b, (((0,), (0,)), ((), ())), preferred_element_type=F32)


def by_rows(height, step, one):
    def wrapped(i, carry):
        one(pl.ds(pl.multiple_of(i * step, step), step))
        return carry

    lax.fori_loop(0, height // step, wrapped, 0)


def add_into(dst, src, height, step):
    def one(r):
        dst[r, :] = (dst[r, :].astype(F32) + src[r, :].astype(F32)).astype(dst.dtype)

    by_rows(height, step, one)


def swap_halves(v):
    lane = lax.broadcasted_iota(jnp.int32, v.shape, 1)
    first = (lane % HD) < (HD // 2)
    return jnp.where(first, pltpu.roll(v, LANE - HD // 2, 1), pltpu.roll(v, HD // 2, 1))


def spread_pair(dst, pair):
    lane = lax.broadcasted_iota(jnp.int32, pair.shape, 1)
    low = lane < HD
    turned = pltpu.roll(pair, HD, 1)
    zero = jnp.zeros_like(pair)
    dst[0] = jnp.where(low, pair, zero).astype(BF)
    dst[1] = jnp.where(low, zero, turned).astype(BF)
    dst[2] = jnp.where(low, turned, zero).astype(BF)
    dst[3] = jnp.where(low, zero, pair).astype(BF)


class Line:
    def __init__(self, wire, own, buf, send_base, recv_base):
        self.wire, self.own, self.buf = wire, own, buf
        self.s, self.r = send_base, recv_base
        self.pitch = buf.shape[0] // ZN
        z, x, c, y = place()
        self.z, self.y = z, y
        self.up, self.down = dev(z + 1, x, c, y), dev(z - 1, x, c, y)
        self.other = dev(z, x, c, 1 - y)
        self.seq, self.half = own.shape[0], own.shape[1] // 2

    def blk(self, o, h):
        return self.buf.at[tokens(o, self.pitch, self.seq), lanes(h, self.half)]

    def start(self):
        z, wire = self.z, self.wire
        src = self.own.at[:, lanes(self.y, self.half)]
        dst = self.blk(z, self.y)
        wire.send(src, dst, self.s + z, self.r + z, self.up, z < ZN - 1)
        wire.send(src, dst, self.s + 4 + z, self.r + z, self.down, z > 0)

    def relay(self, s):
        z, wire = self.z, self.wire
        for o, cond, fwd, to, frm, base in (
            (z - s, z >= s, z < ZN - 1, self.up, self.down, 0),
            (z + s, z + s < ZN, z > 0, self.down, self.up, 4),
        ):
            b = self.blk(o, self.y)
            wire.arrived(b, self.r + o, frm, cond)
            wire.send(b, b, self.s + base + o, self.r + o, to, cond & fwd)
            wire.send(b, b, self.s + 8 + o, self.r + 4 + o, self.other, cond)

    def half_of(self, o):
        self.wire.arrived(self.blk(o, 1 - self.y), self.r + 4 + o, self.other)


class Chain:
    def __init__(self, wire, held, zin, height, step, send_base, recv_base):
        self.wire, self.held, self.zin = wire, held, zin
        self.height, self.step = height, step
        self.s, self.r = send_base, recv_base
        self.z, x, c, y = place()
        self.up, self.down = dev(self.z + 1, x, c, y), dev(self.z - 1, x, c, y)

    def inbound(self, o, slot, frm, cond):
        self.wire.arrived(self.zin(slot), self.r + slot, frm, cond)

        @pl.when(cond)
        def _():
            add_into(self.held(o), self.zin(slot), self.height, self.step)

    def outward(self, t, ready):
        z = self.z
        for o, cond, more, to, frm, base, slot in (
            (z + t, z + t < ZN, z > 0, self.up, self.down, 0, z + t),
            (z - t, z >= t, z < ZN - 1, self.down, self.up, 4, 4 if t == 1 else z - t),
        ):
            ready(o, cond)
            self.inbound(o, o, frm, cond & more)
            self.wire.send(
                self.held(o), self.zin(slot), self.s + base + o, self.r + slot, to, cond
            )

    def home(self):
        z = self.z
        self.inbound(z, z, self.down, z > 0)
        self.inbound(z, 4, self.up, z < ZN - 1)


class Tree:
    def __init__(self, wire, own, blk, send_base, recv_base):
        self.wire, self.own, self.blk = wire, own, blk
        self.s, self.r = send_base, recv_base
        self.z, self.x, self.c, y = place()
        z, x, c = self.z, self.x, self.c
        self.up, self.down = dev(z + 1, x, c, y), dev(z - 1, x, c, y)
        self.side, self.twin = dev(z, 1 - x, c, y), dev(z, x, 1 - c, y)

    def start_z(self):
        z, wire = self.z, self.wire
        d = self.blk(rid(z, self.x, self.c))
        wire.send(self.own, d, self.s + z, self.r + z, self.up, z < ZN - 1)
        wire.send(self.own, d, self.s + 4 + z, self.r + z, self.down, z > 0)

    def start_near(self):
        z, wire = self.z, self.wire
        d = self.blk(rid(z, self.x, self.c))
        wire.send(self.own, d, self.s + 8 + z, self.r + 4 + z, self.side)
        k = z * 2 + self.x
        wire.send(self.own, d, self.s + 12 + k, self.r + 8 + k, self.twin)

    def start(self):
        self.start_z()
        self.start_near()

    def relay(self, s):
        z, wire = self.z, self.wire
        for o, cond, fwd, to, frm, base in (
            (z - s, z >= s, z < ZN - 1, self.up, self.down, 0),
            (z + s, z + s < ZN, z > 0, self.down, self.up, 4),
        ):
            b = self.blk(rid(o, self.x, self.c))
            wire.arrived(b, self.r + o, frm, cond)
            wire.send(b, b, self.s + base + o, self.r + o, to, cond & fwd)
            wire.send(b, b, self.s + 8 + o, self.r + 4 + o, self.side, cond)
            k = o * 2 + self.x
            wire.send(b, b, self.s + 12 + k, self.r + 8 + k, self.twin, cond)

    def across(self, s):
        z = self.z
        todo = ((z, None),) if s == 0 else ((z - s, z >= s), (z + s, z + s < ZN))
        for o, cond in todo:
            b = self.blk(rid(o, 1 - self.x, self.c))
            self.wire.arrived(b, self.r + 4 + o, self.side, cond)
            k = o * 2 + 1 - self.x
            self.wire.send(b, b, self.s + 12 + k, self.r + 8 + k, self.twin, cond)

    def finish(self):
        for o in range(ZN):
            for xx in (0, 1):
                b = self.blk(rid(o, xx, 1 - self.c))
                self.wire.arrived(b, self.r + 8 + o * 2 + xx, self.twin)


def front_kernel(
    resid_h, wq_l, wk_l, wv_l, wo_l, g1_l, g2_l, wg_h, wu_h, wd_h, cot_h, seg, freq,
    wqkv_o, wo_o, ga, n1_o, q_o, kv, ctx_o, mid_o, cos_t, sin_t, mask, dn, feed_out, g3_out,
    wqkv, wo, n1, q, ctx, mid, zin, w3, dres, normed, hid_t, dg_t, du_t, hid, dg, du, dnp, yin, stage,
    resid, wg_l, wu_l, cot, ga_l, qkv_l, w3_l, dres_l, kx, vx, attn, part, nrm, ss, rs, ls,
):
    z, x, c, y = place()
    units = w3.shape[1]
    seq, width = resid.shape
    half = width // 2
    pitch = normed.shape[0] // ZN
    q_width = q.shape[1]
    pairs = q_width // LANE
    loads = [
        pltpu.make_async_copy(cot_h, cot, ls.at[6]),
        pltpu.make_async_copy(wg_h.at[0], wg_l, ls.at[7]),
        pltpu.make_async_copy(wu_h.at[0], wu_l, ls.at[8]),
        pltpu.make_async_copy(wd_h.at[0], w3_l.at[2], ls.at[9]),
        pltpu.make_async_copy(resid_h, resid, ls.at[10]),
    ]
    for cp in loads:
        cp.start()
    wire = Wire(ss, rs)
    side, twin, other = dev(z, 1 - x, c, y), dev(z, x, 1 - c, y), dev(z, x, c, 1 - y)
    qkv_l[:, pl.ds(0, q_width)] = wq_l[0]
    qkv_l[:, pl.ds(q_width, LANE)] = wk_l[0]
    qkv_l[:, pl.ds(q_width + LANE, LANE)] = wv_l[0]
    row = lax.broadcasted_iota(jnp.int32, (16, LANE), 0)
    two = jnp.where(row == 0, g1_l[...].astype(F32), g2_l[...].astype(F32))
    ga_l[...] = jnp.where(row < 2, two, 0.0).astype(BF)
    greet(all_peers(z, x, c, y))

    def qkv_blk(r):
        return wqkv.at[pl.ds(pl.multiple_of(r * LANE, LANE), LANE), :]

    def wo_blk(r):
        return wo.at[:, lanes(r)]

    def ga_blk(r):
        return ga.at[:, lanes(r)]

    def ffn(r):
        return w3.at[:, :, lanes(r)]

    t_qkv = Tree(wire, qkv_l, qkv_blk, 0, 0)
    t_wo = Tree(wire, wo_l.at[0], wo_blk, 20, 16)
    t_ga = Tree(wire, ga_l, ga_blk, 40, 32)
    l_dres = Line(wire, dres_l, dres, 76, 64)
    l_norm = Line(wire, nrm, normed, 88, 72)
    mine = rid(z, x, c)
    t_ga.start()
    t_qkv.start()
    own = [
        pltpu.make_async_copy(qkv_l, qkv_blk(mine), ls.at[0]),
        pltpu.make_async_copy(wo_l.at[0], wo_blk(mine), ls.at[1]),
        pltpu.make_async_copy(ga_l, ga_blk(mine), ls.at[2]),
    ]
    for cp in own:
        cp.start()

    def round_cot(r):
        dres_l[r, :] = cot[r, :].astype(BF)

    def turn(i, carry):
        cut = lanes(i)
        w3_l[0, pl.ds(pl.multiple_of(i * LANE, LANE), LANE), :] = (
            wg_l[:, cut].astype(F32).T.astype(BF)
        )
        w3_l[1, pl.ds(pl.multiple_of(i * LANE, LANE), LANE), :] = (
            wu_l[:, cut].astype(F32).T.astype(BF)
        )
        return carry

    def turned(v):
        return v * cos_t[...] + swap_halves(v) * sin_t[...]

    def q_tile(j, carry):
        acc = dot_nn(n1[...], wqkv[:, lanes(j, 2 * LANE)])
        for h in (0, 1):
            q[:, lanes(2 * j + h)] = turned(acc[:, h * LANE : (h + 1) * LANE]).astype(BF)
        return carry

    def pair(p, carry):
        qp = q[:, lanes(p)]
        g = p // (pairs // 2)
        out = jnp.zeros((seq, LANE), F32)
        for h in (0, 1):
            s = dot_nt(qp, kx[2 * g + h]) * HD ** (-0.5)
            s = jnp.where(mask[...] > 0.0, s, masked_score)
            top = jnp.max(s, axis=-1, keepdims=True)
            lse = top + jnp.log(jnp.sum(jnp.exp(s - top), axis=-1, keepdims=True))
            out = out + dot_nn(jnp.exp(s - lse).astype(BF), vx[2 * g + h])
        ctx[:, lanes(p)] = out.astype(BF)
        return carry

    ids = jnp.broadcast_to(seg[...].astype(F32), (seq, seq))
    own_id = lax.broadcasted_iota(jnp.int32, (seq, seq), 0)
    key_id = lax.broadcasted_iota(jnp.int32, (seq, seq), 1)
    mine_id = jnp.sum(jnp.where(own_id == key_id, ids, 0.0), axis=1, keepdims=True)
    seen = jnp.where((ids == mine_id) & (key_id <= own_id), 1.0, 0.0)
    mask[...] = seen
    angles = (jnp.sum(seen, axis=1, keepdims=True) - 1.0) * freq[...]
    lane = lax.broadcasted_iota(jnp.int32, (seq, LANE), 1)
    cos_t[...] = jnp.cos(angles)
    sin_t[...] = jnp.where(lane % HD < HD // 2, -1.0, 1.0) * jnp.sin(angles)
    for o in range(ZN):
        gap = pl.ds(o * pitch + seq, pitch - seq)
        normed[gap, :] = jnp.zeros((pitch - seq, width), BF)
        dres[gap, :] = jnp.zeros((pitch - seq, width), BF)
    loads[0].wait()
    by_rows(seq, 16, round_cot)
    t_ga.relay(1)
    t_qkv.relay(1)
    t_ga.across(0)
    t_qkv.across(0)
    t_ga.relay(2)
    t_qkv.relay(2)
    t_wo.start_z()
    for cp in loads[1:]:
        cp.wait()
    lax.fori_loop(0, w3_l.shape[1] // LANE, turn, 0)
    t_ga.across(1)
    t_qkv.across(1)
    t_ga.relay(3)
    t_qkv.relay(3)
    t_wo.start_near()
    t_ga.across(2)
    t_ga.across(3)
    t_ga.finish()
    own[2].wait()
    gain_one = ga[pl.ds(0, 8), :].astype(F32)[0:1]
    gain_two = ga[pl.ds(0, 8), :].astype(F32)[1:2]

    def norm_one(r):
        v = resid[r, :]
        recip = lax.rsqrt(jnp.mean(v * v, axis=-1, keepdims=True) + epsilon)
        n1[r, :] = (v * recip * gain_one).astype(BF)

    by_rows(seq, 16, norm_one)
    t_wo.relay(1)
    t_qkv.across(2)
    t_wo.relay(2)
    for d in (2, 1, 3):
        zt = (z + d) % ZN
        wire.send(w3_l.at[:, rows(zt, units), :], ffn(mine), 60 + d - 1, 48 + z, dev(zt, x, c, y))
    l_dres.start()
    t_qkv.across(3)
    t_qkv.finish()
    own[0].wait()
    lax.fori_loop(0, pairs // 2, q_tile, 0)
    acc = dot_nn(n1[...], wqkv[:, pl.ds(q_width, 2 * LANE)])
    key = turned(acc[:, :LANE]).astype(BF)
    val = acc[:, LANE:].astype(BF)
    kv[:, pl.ds(0, LANE)] = key
    kv[:, pl.ds(LANE, LANE)] = val
    spread_pair(kx, key.astype(F32))
    spread_pair(vx, val.astype(F32))
    t_wo.across(0)
    t_wo.relay(3)
    mine3 = w3_l.at[:, rows(z, units), :]
    wire.send(mine3, ffn(mine), 64 + z, 52 + z, side)
    wire.send(mine3, ffn(mine), 68 + z * 2 + x, 56 + z * 2 + x, twin)
    own += [
        pltpu.make_async_copy(mine3, ffn(mine), ls.at[3]),
        pltpu.make_async_copy(dres_l, dres.at[tokens(z, pitch, seq), :], ls.at[4]),
    ]
    own[3].start()
    own[4].start()
    lax.fori_loop(0, pairs, pair, 0)
    for s in (1, 2, 3):
        t_wo.across(s)
    t_wo.finish()
    own[1].wait()

    def out_tile(j, carry):
        cut = lanes(j, 2 * LANE)
        attn[:, cut] = dot_nn(ctx[...], wo[:, cut]).astype(BF)
        return carry

    lax.fori_loop(0, width // (2 * LANE), out_tile, 0)
    wire.send(attn, part, 100, 80, other)
    kept = [
        pltpu.make_async_copy(a, b, ls.at[17 + i])
        for i, (a, b) in enumerate(
            ((wqkv, wqkv_o), (wo, wo_o), (n1, n1_o), (q, q_o), (ctx, ctx_o), (mid, mid_o))
        )
    ]
    for cp in kept[:5]:
        cp.start()

    def ffn_in(d):
        o = (z + ZN - d) % ZN
        b = ffn(rid(o, x, c))
        wire.arrived(b, 48 + o, dev(o, x, c, y))
        wire.send(b, b, 64 + o, 52 + o, side)
        wire.send(b, b, 68 + o * 2 + x, 56 + o * 2 + x, twin)

    def ffn_across(d):
        o = (z + ZN - d) % ZN
        b = ffn(rid(o, 1 - x, c))
        wire.arrived(b, 52 + o, side)
        k = o * 2 + 1 - x
        wire.send(b, b, 68 + k, 56 + k, twin)

    def second(r):
        m = resid[r, :] + (attn[r, :].astype(F32) + part[r, :].astype(F32))
        mid[r, :] = m
        recip = lax.rsqrt(jnp.mean(m * m, axis=-1, keepdims=True) + epsilon)
        nrm[r, :] = (m * recip * gain_two).astype(BF)

    ffn_in(2)
    wire.arrived(part, 80, other)
    by_rows(seq, 16, second)
    l_norm.start()
    kept[5].start()
    own.append(pltpu.make_async_copy(nrm, normed.at[tokens(z, pitch, seq), :], ls.at[5]))
    own[5].start()
    ffn_in(1)
    ffn_across(0)
    ffn_in(3)
    l_dres.relay(1)
    ffn_across(2)
    l_norm.relay(1)
    l_dres.relay(2)
    ffn_across(1)
    ffn_across(3)
    for o in range(ZN):
        for xx in (0, 1):
            wire.arrived(ffn(rid(o, xx, 1 - c)), 56 + o * 2 + xx, twin)
    for cp in own[3:]:
        cp.wait()
    step = units // 2

    def ffn_block(o):
        r = tokens(o, pitch, pitch)

        def some_units(i, carry):
            u = pl.ds(pl.multiple_of(i * step, 16), step)
            g = dot_nt(w3[0, u, :], normed[r, :])
            up = dot_nt(w3[1, u, :], normed[r, :])
            dh = dot_nt(w3[2, u, :], dres[r, :])
            s = jax.nn.sigmoid(g)
            hid_t[u, lanes(o, pitch)] = (g * s * up).astype(BF)
            dg_t[u, lanes(o, pitch)] = (dh * up * s * (1.0 + g * (1.0 - s))).astype(BF)
            du_t[u, lanes(o, pitch)] = (dh * (g * s)).astype(BF)
            return carry

        lax.fori_loop(0, units // step, some_units, 0)
        dg[...] = dg_t[:, lanes(o, pitch)].astype(F32).T[:seq].astype(BF)
        du[...] = du_t[:, lanes(o, pitch)].astype(F32).T[:seq].astype(BF)
        hid[rows(o, seq), :] = hid_t[:, lanes(o, pitch)].astype(F32).T[:seq].astype(BF)

        def some_lanes(j, carry):
            cut = lanes(j, 2 * LANE)
            dnp[o, :, cut] = (dot_nn(dg[...], w3[0, :, cut]) + dot_nn(du[...], w3[1, :, cut])).astype(BF)
            return carry

        lax.fori_loop(0, width // (2 * LANE), some_lanes, 0)

    def far_half(o):
        part = dnp.at[o].at[:, lanes(1 - y, half)]
        wire.send(part, yin.at[o], 101 + o, 81 + o, other)

    o1 = z + 1 - 2 * ((z + 3) // 4)
    o3 = 3 - 3 * (z // 2)
    o2 = 6 - z - o1 - o3

    def both_halves(o):
        l_dres.half_of(o)
        l_norm.half_of(o)

    ffn_block(z)
    l_norm.relay(2)
    l_dres.relay(3)
    both_halves(o1)
    ffn_block(o1)
    l_norm.relay(3)
    both_halves(o2)
    ffn_block(o2)
    far_half(o2)
    both_halves(o3)
    ffn_block(o3)
    for o in (o3, o1, z):
        far_half(o)

    wide = 4 * LANE
    tiles = width // wide

    def columns(first, value, dst):
        def one(j, carry):
            slot = j % 2
            cp = pltpu.make_async_copy(stage.at[slot], dst(j), ls.at[11 + slot])
            if first:
                pl.when(j >= 2)(cp.wait)
            else:
                cp.wait()
            stage[slot] = value(lanes(j, wide)).astype(BF)
            cp.start()
            return carry

        lax.fori_loop(0, tiles, one, 0)

    def over_tokens(act, kept):
        return lambda cut: dot_nn(act[...], kept[:, cut])

    def grad_dst(m):
        return lambda j: g3_out.at[m, :, lanes(j, wide)]

    line = Chain(wire, lambda o: yin.at[o], lambda k: zin.at[k], seq, 16, 105, 85)

    def dn_ready(o, cond):
        wire.arrived(yin.at[o], 81 + o, other, cond)

        @pl.when(cond)
        def _():
            add_into(yin.at[o], dnp.at[o].at[:, lanes(y, half)], seq, 16)

    columns(True, over_tokens(dg_t, normed), grad_dst(0))
    line.outward(3, dn_ready)
    columns(False, over_tokens(du_t, normed), grad_dst(1))
    line.outward(2, dn_ready)
    columns(False, over_tokens(hid_t, dres), grad_dst(2))
    line.outward(1, dn_ready)
    columns(False, lambda cut: dot_nn(hid[...], w3[2, :, cut]), lambda j: feed_out.at[:, lanes(j, wide)])
    dn_ready(z, z >= 0)
    line.home()

    def keep_dn(r):
        dn[r, lanes(y, half)] = yin[z, r, :]

    by_rows(seq, 16, keep_dn)
    blk = dn.at[:, lanes(y, half)]
    wire.send(blk, blk, 113, 90, other)
    wire.arrived(dn.at[:, lanes(1 - y, half)], 90, other)
    wire.drain()
    for slot in (0, 1):
        pltpu.make_async_copy(stage.at[slot], feed_out.at[:, lanes(slot, wide)], ls.at[11 + slot]).wait()
    for cp in kept:
        cp.wait()


def front(resid, w_query, w_key, w_value, w_out, g1, g2, w_gate, w_up, w_down, cot, seg):
    seq, width = resid.shape
    q_width, out_rows = w_query.shape[2], w_out.shape[1]
    total = q_width + 2 * LANE
    units = w_gate.shape[2] // ZN
    pair_shape = (4, seq, LANE)
    pitch = pl.cdiv(seq, LANE) * LANE
    freq = rope_base ** (-(np.arange(LANE) % (HD // 2)) * 2.0 / HD)
    freq = jnp.asarray(freq[None].astype(np.float32))
    vm, hb = vm_spec(), any_spec()
    return pl.pallas_call(
        front_kernel,
        name="front",
        out_shape=(
            jax.ShapeDtypeStruct((width, total), BF),
            jax.ShapeDtypeStruct((out_rows, width), BF),
            jax.ShapeDtypeStruct((16, width), BF),
            jax.ShapeDtypeStruct((seq, width), BF),
            jax.ShapeDtypeStruct((seq, q_width), BF),
            jax.ShapeDtypeStruct((seq, 2 * LANE), BF),
            jax.ShapeDtypeStruct((seq, q_width), BF),
            jax.ShapeDtypeStruct((seq, width), F32),
            jax.ShapeDtypeStruct((seq, LANE), F32),
            jax.ShapeDtypeStruct((seq, LANE), F32),
            jax.ShapeDtypeStruct((seq, seq), F32),
            jax.ShapeDtypeStruct((seq, width), BF),
            jax.ShapeDtypeStruct((seq * ZN, width), BF),
            jax.ShapeDtypeStruct((3, units, width), BF),
        ),
        in_specs=[hb] + [vm] * 6 + [hb] * 4 + [vm] * 2,
        out_specs=[hb] * 2 + [vm] + [hb] * 2 + [vm] + [hb] * 2 + [vm] * 4 + [hb] * 2,
        scratch_shapes=[
            pltpu.VMEM((width, total), BF),
            pltpu.VMEM((out_rows, width), BF),
            pltpu.VMEM((seq, width), BF),
            pltpu.VMEM((seq, q_width), BF),
            pltpu.VMEM((seq, q_width), BF),
            pltpu.VMEM((seq, width), F32),
            pltpu.VMEM((5, seq, width // 2), BF),
            pltpu.VMEM((3, units, width), BF),
            pltpu.VMEM((pitch * ZN, width), BF),
            pltpu.VMEM((pitch * ZN, width), BF),
            pltpu.VMEM((units, pitch * ZN), BF),
            pltpu.VMEM((units, pitch * ZN), BF),
            pltpu.VMEM((units, pitch * ZN), BF),
            pltpu.VMEM((seq * ZN, units), BF),
            pltpu.VMEM((seq, units), BF),
            pltpu.VMEM((seq, units), BF),
            pltpu.VMEM((ZN, seq, width), BF),
            pltpu.VMEM((ZN, seq, width // 2), BF),
            pltpu.VMEM((2, seq * ZN, 4 * LANE), BF),
            pltpu.VMEM((seq, width), F32),
            pltpu.VMEM((LANE, units * ZN), BF),
            pltpu.VMEM((LANE, units * ZN), BF),
            pltpu.VMEM((seq, width), F32),
            pltpu.VMEM((16, LANE), BF),
            pltpu.VMEM((LANE, total), BF),
            pltpu.VMEM((3, units * ZN, LANE), BF),
            pltpu.VMEM((seq, width), BF),
            pltpu.VMEM(pair_shape, BF),
            pltpu.VMEM(pair_shape, BF),
            pltpu.VMEM((seq, width), BF),
            pltpu.VMEM((seq, width), BF),
            pltpu.VMEM((seq, width), BF),
            sems(114),
            sems(91),
            sems(23),
        ],
        compiler_params=params(0),
    )(resid, w_query, w_key, w_value, w_out, g1, g2, w_gate, w_up, w_down, cot, seg, freq)


class Fold:
    def __init__(self, wire, part, cin, xin, zin, height, step, send_base, recv_base):
        self.wire, self.part, self.cin, self.xin = wire, part, cin, xin
        self.height, self.step = height, step
        self.s, self.r = send_base, recv_base
        self.z, self.x, self.c, y = place()
        z, x, c = self.z, self.x, self.c
        self.side, self.twin = dev(z, 1 - x, c, y), dev(z, x, 1 - c, y)
        self.chain = Chain(
            wire, lambda o: xin.at[o], lambda s: zin.at[s], height, step, self.s + 12, self.r + 12
        )

    def order(self):
        return [(self.z + d) % ZN for d in (2, 1, 3, 0)]

    def to_twin(self):
        for xx in (1 - self.x, self.x):
            for o in self.order():
                k = o * 2 + xx
                self.wire.send(
                    self.part(k * 2 + 1 - self.c), self.cin.at[k], self.s + k, self.r + k, self.twin
                )

    def from_twin(self, k):
        self.wire.arrived(self.cin.at[k], self.r + k, self.twin)
        add_into(self.cin.at[k], self.part(k * 2 + self.c), self.height, self.step)

    def from_twin_if(self, k, cond):
        self.wire.arrived(self.cin.at[k], self.r + k, self.twin, cond)

        @pl.when(cond)
        def _():
            add_into(self.cin.at[k], self.part(k * 2 + self.c), self.height, self.step)

    def across_one(self, o, cond=None):
        k = o * 2 + 1 - self.x
        if cond is None:
            self.from_twin(k)
        else:
            self.from_twin_if(k, cond)
        self.wire.send(
            self.cin.at[k], self.xin.at[o], self.s + 8 + o, self.r + 8 + o, self.side, cond
        )

    def across(self):
        z = self.z
        for t in (3, 2, 1):
            self.across_one(z + t, z + t < ZN)
            self.across_one(z - t, z >= t)
        self.across_one(z)

    def stay(self):
        for o in self.order():
            self.from_twin(o * 2 + self.x)

    def ready(self, o, cond):
        self.wire.arrived(self.xin.at[o], self.r + 8 + o, self.side, cond)

        @pl.when(cond)
        def _():
            add_into(self.xin.at[o], self.cin.at[o * 2 + self.x], self.height, self.step)

    def outward(self, t):
        self.chain.outward(t, self.ready)

    def home(self):
        self.ready(self.z, self.z >= 0)
        self.chain.home()
        return self.xin.at[self.z]


def back_kernel(
    feed_p, g3_p, wqkv, dn_h, mid_h, cot_h, resid_h, ga_h, n1_h, q_h, kv_h, ctx_h, wo_h, cos_h,
    sin_h, mask_h,
    feed_out, grad_out, g3, gq_out, go_out, gains_out,
    dn, mid, cot, resid, ga, n1, q, kv, ctx, wo, cos_t, sin_t, mask, grad_in, fown, yin, zin, gbuf, cin, xin, gq_p, go_p, gp, qc, qx, qz, oc, ox, oz, gc, gx, gz,
    feed, mid_b, dctx, dqkv, dn1, dn1_o, kx, vx, kacc, vacc, wbuf, gs, gr, ss, rs, ls,
):
    z, x, c, y = place()
    units = g3_p.shape[1]
    seq, width = mid.shape
    half = width // 2
    q_width = q.shape[1]
    pairs = q_width // LANE
    out_rows = wo.shape[0]
    wire = Wire(ss, rs)
    side, twin, other = dev(z, 1 - x, c, y), dev(z, x, 1 - c, y), dev(z, x, c, 1 - y)
    ring = [(z + d) % ZN for d in (2, 1, 3, 0)]
    greet(all_peers(z, x, c, y))

    def y_out(src, k, steps):
        for t in steps:
            todo = ((z + t, z + t < ZN), (z - t, z >= t)) if t else ((z, None),)
            for o, cond in todo:
                part = src.at[rows(o, seq), lanes(1 - y, half)]
                wire.send(part, yin.at[o], k * 4 + o, k * 4 + o, other, cond)

    def own_half(o):
        return pltpu.make_async_copy(
            feed_p.at[rows(o, seq), lanes(y, half)], fown.at[o], ls.at[3 + o]
        )

    for k in range(8):
        wire.send(g3_p.at[:, :, lanes(k * 2 + 1 - c)], cin.at[k], 26 + k, 20 + k, twin)
    ks = [o * 2 + 1 - x for o in ring] + [o * 2 + x for o in ring]

    def load(i):
        return pltpu.make_async_copy(
            g3_p.at[:, :, lanes(ks[i] * 2 + c)], gbuf.at[i % 2], ls.at[i % 2]
        )

    def add3(dst, src):
        for m in range(3):
            add_into(dst.at[m], src.at[m], units, 64)


    def ffn_add(i):
        if i < 7:
            load(i + 1).start()
        load(i).wait()
        wire.arrived(cin.at[ks[i]], 20 + ks[i], twin)
        add3(cin.at[ks[i]], gbuf.at[i % 2])
        if i < 4:
            o = ring[i]
            wire.send(cin.at[ks[i]], xin.at[o], 34 + o, 28 + o, side)

    load(0).start()
    pairs_in = (
        (dn_h, dn), (mid_h, mid), (cot_h, cot), (wo_h, wo), (ga_h, ga), (kv_h, kv), (mask_h, mask), (n1_h, n1),
        (q_h, q), (ctx_h, ctx), (cos_h, cos_t), (sin_h, sin_t), (resid_h, resid),
    )
    inward = [
        pltpu.make_async_copy(a, b, ls.at[13 + i]) for i, (a, b) in enumerate(pairs_in)
    ]
    for cp in inward:
        cp.start()
    for o in range(ZN):
        own_half(o).start()

    line = Chain(wire, lambda o: yin.at[o], lambda k: zin.at[k], seq, 16, 8, 8)

    def ffn_z(i):
        o = ring[i]
        wire.arrived(xin.at[o], 28 + o, side)
        add3(xin.at[o], cin.at[o * 2 + x])
        d = (2, 1, 3, 0)[i]
        if d:
            wire.send(xin.at[o], g3.at[:, rows(z, units), :], 38 + d - 1, 32 + z, dev(o, x, c, y))
        else:
            pltpu.make_async_copy(xin.at[o], g3.at[:, rows(z, units), :], ls.at[10]).start()

    y_out(feed_p, 1, (3, 2, 1, 0))
    for i in range(8):
        ffn_add(i)
    for cp in inward:
        cp.wait()
    spread_pair(kx, kv[:, pl.ds(0, LANE)].astype(F32))
    spread_pair(vx, kv[:, pl.ds(LANE, LANE)].astype(F32))
    kacc[...] = jnp.zeros_like(kacc)
    vacc[...] = jnp.zeros_like(vacc)
    gp[...] = jnp.zeros_like(gp)
    gain_one = ga[pl.ds(0, 8), :].astype(F32)[0:1]
    gain_two = ga[pl.ds(0, 8), :].astype(F32)[1:2]

    def norm_two(r):
        v, g = mid[r, :], dn[r, :].astype(F32)
        recip = lax.rsqrt(jnp.mean(v * v, axis=-1, keepdims=True) + epsilon)
        e = g * gain_two
        d = recip * e - v * (recip * recip * recip) * jnp.mean(e * v, axis=-1, keepdims=True)
        out = cot[r, :] + d
        grad_in[r, :] = out
        mid_b[r, :] = out.astype(BF)
        t = g * v * recip
        gp[pl.ds(8, 8), :] += t[:8] + t[8:]

    by_rows(seq, 16, norm_two)

    def out_grad(i, carry):
        cut = lanes(i, 2 * LANE)
        for h in range(2):
            hh = pl.ds(h * (out_rows // 2), out_rows // 2)
            go_p[hh, cut] = dot_tn(ctx[:, hh], mid_b[:, cut]).astype(BF)
        return carry

    lax.fori_loop(0, width // (2 * LANE), out_grad, 0)
    f_o = Fold(wire, lambda r: go_p.at[:, lanes(r)], oc, ox, oz, out_rows, 64, 61, 53)
    f_q = Fold(
        wire,
        lambda r: gq_p.at[pl.ds(pl.multiple_of(r * LANE, LANE), LANE), :],
        qc, qx, qz, LANE, 16, 41, 36,
    )
    f_g = Fold(wire, lambda r: gp.at[:, lanes(r)], gc, gx, gz, 16, 16, 81, 70)
    f_o.to_twin()

    def ctx_grad(j, carry):
        cut = lanes(j, 2 * LANE)
        dctx[:, cut] = dot_nt(mid_b[...], wo[cut, :]).astype(BF)
        return carry

    lax.fori_loop(0, q_width // (2 * LANE), ctx_grad, 0)
    ffn_z(0)
    f_o.across()

    def back_turned(v):
        return v * cos_t[...] - swap_halves(v) * sin_t[...]

    def pair(p, carry):
        qp, dc = q[:, lanes(p)], dctx[:, lanes(p)]
        g = p // (pairs // 2)
        prod = dc.astype(F32) * ctx[:, lanes(p)].astype(F32)
        low = lax.broadcasted_iota(jnp.int32, prod.shape, 1) < HD
        dq = jnp.zeros((seq, LANE), F32)
        for h in (0, 1):
            i = 2 * g + h
            s = dot_nt(qp, kx[i]) * HD ** (-0.5)
            s = jnp.where(mask[...] > 0.0, s, masked_score)
            top = jnp.max(s, axis=-1, keepdims=True)
            lse = top + jnp.log(jnp.sum(jnp.exp(s - top), axis=-1, keepdims=True))
            full = jnp.exp(s - lse)
            delta = jnp.sum(jnp.where(low if h == 0 else ~low, prod, 0.0), axis=-1, keepdims=True)
            ds = (full * (dot_nt(dc, vx[i]) - delta)).astype(BF)
            dq = dq + dot_nn(ds, kx[i])
            kacc[i] += dot_tn(ds, qp)
            vacc[i] += dot_tn(full.astype(BF), dc)
        dqkv[:, lanes(p)] = back_turned(dq * HD ** (-0.5)).astype(BF)
        return carry

    lax.fori_loop(0, pairs // 2, pair, 0)
    ffn_z(1)
    lax.fori_loop(pairs // 2, pairs, pair, 0)

    def joined(acc):
        low = lax.broadcasted_iota(jnp.int32, (seq, LANE), 1) < HD
        return jnp.where(
            low, acc[0] + pltpu.roll(acc[1], HD, 1), acc[3] + pltpu.roll(acc[2], HD, 1)
        )

    dqkv[:, pl.ds(q_width, LANE)] = back_turned(joined(kacc) * HD ** (-0.5)).astype(BF)
    dqkv[:, pl.ds(q_width + LANE, LANE)] = joined(vacc).astype(BF)

    def w_tile(j, slot):
        r = pl.ds(pl.multiple_of(j * 2 * LANE, 2 * LANE), 2 * LANE)
        return pltpu.make_async_copy(wqkv.at[r, :], wbuf.at[slot], ls.at[11 + slot])

    w_tile(0, 0).start()

    def in_grad(r, carry):
        gq_p[pl.ds(pl.multiple_of(r * LANE, LANE), LANE), :] = dot_tn(
            n1[:, lanes(r)], dqkv[...]
        ).astype(BF)
        return carry

    lax.fori_loop(0, width // LANE, in_grad, 0)
    f_q.to_twin()
    f_q.across()
    ffn_z(2)
    tiles = width // (2 * LANE)
    for j in range(tiles):
        if j + 1 < tiles:
            w_tile(j + 1, (j + 1) % 2).start()
        w_tile(j, j % 2).wait()
        dn1[:, pl.ds(j * 2 * LANE, 2 * LANE)] = dot_nt(dqkv[...], wbuf[j % 2]).astype(BF)
    wire.send(dn1, dn1_o, 101, 87, other)

    def gain_part(r):
        v = resid[r, :]
        recip = lax.rsqrt(jnp.mean(v * v, axis=-1, keepdims=True) + epsilon)
        t = dn1[r, :].astype(F32) * v * recip
        gp[pl.ds(0, 8), :] += t[:8] + t[8:]

    by_rows(seq, 16, gain_part)
    f_g.to_twin()
    f_g.across()
    ffn_z(3)
    f_o.stay()
    for t in (3, 2, 1):
        f_o.outward(t)

    for o in range(ZN):
        own_half(o).wait()

    def feed_ready(o, cond):
        wire.arrived(yin.at[o], 4 + o, other, cond)

        @pl.when(cond)
        def _():
            add_into(yin.at[o], fown.at[o], seq, 16)

    for t in (3, 2, 1):
        line.outward(t, feed_ready)
    f_q.stay()
    f_g.stay()
    for t in (3, 2, 1):
        f_q.outward(t)
        f_g.outward(t)
    feed_ready(z, z >= 0)
    line.home()
    fb = feed.at[:, lanes(y, half)]

    def keep_feed(r):
        feed[r, lanes(y, half)] = yin[z, r, :]

    by_rows(seq, 16, keep_feed)
    wire.send(fb, fb, 25, 19, other)
    wire.arrived(dn1_o, 87, other)

    def norm_one(r):
        v = resid[r, :]
        g = dn1[r, :].astype(F32) + dn1_o[r, :].astype(F32)
        recip = lax.rsqrt(jnp.mean(v * v, axis=-1, keepdims=True) + epsilon)
        e = g * gain_one
        d = recip * e - v * (recip * recip * recip) * jnp.mean(e * v, axis=-1, keepdims=True)
        grad_in[r, :] += d

    by_rows(seq, 16, norm_one)
    outward = [pltpu.make_async_copy(grad_in, grad_out, ls.at[26])]
    outward[0].start()
    done = f_o.home()
    outward.append(pltpu.make_async_copy(done, go_out, ls.at[27]))
    outward[1].start()
    mine = f_g.home()
    gs[...] = mine[...]
    wire.send(gs, gr, 102, 88, other)
    got = f_q.home()
    outward.append(pltpu.make_async_copy(got, gq_out, ls.at[28]))
    outward[2].start()
    wire.arrived(feed.at[:, lanes(1 - y, half)], 19, other)
    outward.append(pltpu.make_async_copy(feed, feed_out, ls.at[29]))
    outward[3].start()
    wire.arrived(gr, 88, other)
    first = jnp.sum(gs[pl.ds(0, 8), :] + gr[pl.ds(0, 8), :], axis=0, keepdims=True)
    second = jnp.sum(gs[pl.ds(8, 8), :], axis=0, keepdims=True)
    row = lax.broadcasted_iota(jnp.int32, (8, LANE), 0)
    gains_out[...] = jnp.where(row == 0, first, second)
    for d in (1, 2, 3):
        o = (z + ZN - d) % ZN
        wire.arrived(g3.at[:, rows(o, units), :], 32 + o, dev(o, x, c, y))
    wire.drain()
    pltpu.make_async_copy(xin.at[z], g3.at[:, rows(z, units), :], ls.at[10]).wait()
    for cp in outward:
        cp.wait()


def back(feed_p, g3_p, wqkv, dn, mid, cot, resid, ga, n1, q, kv, ctx, wo, cos_t, sin_t, mask):
    seq, width = mid.shape
    units = g3_p.shape[1]
    q_width, total = q.shape[1], wqkv.shape[1]
    out_rows = wo.shape[0]
    half = width // 2

    def vm(*shape, dtype=BF):
        return pltpu.VMEM(shape, dtype)

    held = (dn, mid, cot, resid, ga, n1, q, kv, ctx, wo, cos_t, sin_t, mask)
    return pl.pallas_call(
        back_kernel,
        name="back",
        out_shape=(
            jax.ShapeDtypeStruct((seq, width), BF),
            jax.ShapeDtypeStruct((seq, width), F32),
            jax.ShapeDtypeStruct((3, units * ZN, LANE), BF),
            jax.ShapeDtypeStruct((LANE, total), BF),
            jax.ShapeDtypeStruct((out_rows, LANE), BF),
            jax.ShapeDtypeStruct((8, LANE), F32),
        ),
        in_specs=[any_spec()] * 16,
        out_specs=[any_spec()] * 5 + [vm_spec()],
        scratch_shapes=[vm(*a.shape, dtype=a.dtype) for a in held]
        + [
            vm(seq, width, dtype=F32),
            vm(ZN, seq, half),
            vm(ZN, seq, half),
            vm(5, seq, half),
            vm(2, 3, units, LANE),
            vm(8, 3, units, LANE),
            vm(4, 3, units, LANE),
            vm(width, total),
            vm(out_rows, width),
            vm(16, width, dtype=F32),
            vm(8, LANE, total),
            vm(4, LANE, total),
            vm(5, LANE, total),
            vm(8, out_rows, LANE),
            vm(4, out_rows, LANE),
            vm(5, out_rows, LANE),
            vm(8, 16, LANE, dtype=F32),
            vm(4, 16, LANE, dtype=F32),
            vm(5, 16, LANE, dtype=F32),
            vm(seq, width),
            vm(seq, width),
            vm(seq, q_width),
            vm(seq, total),
            vm(seq, width),
            vm(seq, width),
            vm(4, seq, LANE),
            vm(4, seq, LANE),
            vm(4, seq, LANE, dtype=F32),
            vm(4, seq, LANE, dtype=F32),
            vm(2, 2 * LANE, total),
            vm(16, LANE, dtype=F32),
            vm(16, LANE, dtype=F32),
            sems(103),
            sems(89),
            sems(30),
        ],
        compiler_params=pltpu.CompilerParams(
            collective_id=1, has_side_effects=True, vmem_limit_bytes=67043328
        ),
    )(feed_p, g3_p, wqkv, *held)


def finish_kernel(
    mid_h, feed_h, grad_h, g3_h, gq_h, go_h, gains,
    hidden, grad_in, wg, wu, wd, wq, wk, wv, wo, first, second,
    mid, feed, grad, g3, gq, go, tg, td, tq, to, ls,
):
    q_width = wq.shape[2]
    units = td.shape[0]
    into = [
        pltpu.make_async_copy(a, b, ls.at[i])
        for i, (a, b) in enumerate(
            ((g3_h, g3), (mid_h, mid), (feed_h, feed), (gq_h, gq), (go_h, go), (grad_h, grad))
        )
    ]
    for cp in into:
        cp.start()
    first[...] = gains[pl.ds(0, 1), :]
    second[...] = gains[pl.ds(1, 1), :]
    out = []

    def put(src, dst):
        cp = pltpu.make_async_copy(src, dst, ls.at[6 + len(out)])
        cp.start()
        out.append(cp)

    into[0].wait()
    for m, dst in ((0, wg), (1, wu)):

        def turn(i, carry):
            r = pl.ds(pl.multiple_of(i * LANE, LANE), LANE)
            tg[m, :, lanes(i)] = g3[m, r, :].astype(F32).T
            return carry

        lax.fori_loop(0, units // LANE, turn, 0)
        put(tg.at[m], dst.at[0])

    def wide(r):
        td[r, :] = g3[2, r, :].astype(F32)

    by_rows(units, 64, wide)
    put(td, wd.at[0])
    into[1].wait()
    into[2].wait()

    def total(r):
        mid[r, :] += feed[r, :].astype(F32)

    by_rows(mid.shape[0], 16, total)
    put(mid, hidden)
    into[3].wait()

    def wide_q(r):
        tq[r, :] = gq[r, :].astype(F32)

    by_rows(LANE, 16, wide_q)
    put(tq.at[:, pl.ds(0, q_width)], wq.at[0])
    put(tq.at[:, pl.ds(q_width, LANE)], wk.at[0])
    put(tq.at[:, pl.ds(q_width + LANE, LANE)], wv.at[0])
    into[4].wait()

    def wide_o(r):
        to[r, :] = go[r, :].astype(F32)

    by_rows(to.shape[0], 64, wide_o)
    put(to, wo.at[0])
    into[5].wait()
    put(grad, grad_in)
    for cp in out:
        cp.wait()


def finish(mid, feed, grad, g3, gq, go, gains):
    seq, width = mid.shape
    units = g3.shape[1]
    q_width = gq.shape[1] - 2 * LANE
    f32 = lambda *shape: jax.ShapeDtypeStruct(shape, F32)
    ins = (mid, feed, grad, g3, gq, go)
    return pl.pallas_call(
        finish_kernel,
        name="finish",
        out_shape=(
            f32(seq, width),
            f32(seq, width),
            f32(1, LANE, units),
            f32(1, LANE, units),
            f32(1, units, LANE),
            f32(1, LANE, q_width),
            f32(1, LANE, LANE),
            f32(1, LANE, LANE),
            f32(1, go.shape[0], LANE),
            f32(1, LANE),
            f32(1, LANE),
        ),
        in_specs=[any_spec()] * 6 + [vm_spec()],
        out_specs=[any_spec()] * 9 + [vm_spec()] * 2,
        scratch_shapes=[pltpu.VMEM(a.shape, a.dtype) for a in ins]
        + [
            pltpu.VMEM((2, LANE, units), F32),
            pltpu.VMEM((units, LANE), F32),
            pltpu.VMEM(gq.shape, F32),
            pltpu.VMEM(go.shape, F32),
            sems(15),
        ],
        compiler_params=pltpu.CompilerParams(vmem_limit_bytes=67043328),
    )(*ins, gains)


def fast_body(
    hidden_in,
    segment_ids,
    gain_attn,
    w_query,
    w_key,
    w_value,
    w_out,
    gain_ffn,
    w_gate,
    w_up,
    w_down,
    cotangent,
):
    resid = hidden_in
    wqkv, wo, ga, n1, q, kv, ctx, middle, cos_w, sin_w, mask, dn, feed_p, g3_p = front(
        resid, w_query, w_key, w_value, w_out, gain_attn, gain_ffn, w_gate, w_up, w_down,
        cotangent, segment_ids,
    )
    feed, grad_b, g3, gq, go, gains_g = back(
        feed_p, g3_p, wqkv, dn, middle, cotangent, resid, ga, n1, q, kv, ctx, wo,
        cos_w, sin_w, mask,
    )
    hidden_out, grad_input, wg, wu, wd, wq, wk, wv, wo_g, first, second = finish(
        middle, feed, grad_b, g3, gq, go, gains_g
    )
    return (
        hidden_out,
        grad_input,
        first,
        wq,
        wk,
        wv,
        wo_g,
        second,
        wg,
        wu,
        wd,
    )


def solution(mesh):
    small = mesh.shape["dp"] == 16 and mesh.shape["tensor"] == 2
    chosen = fast_body if small else body
    return jax.shard_map(
        chosen,
        mesh=mesh,
        in_specs=(
            P("dp", None),
            P("dp", None),
            P(None, "dp"),
            P(None, "dp", "tensor"),
            P(None, "dp", "tensor"),
            P(None, "dp", "tensor"),
            P(None, "tensor", "dp"),
            P(None, "dp"),
            P(None, "dp", "tensor"),
            P(None, "dp", "tensor"),
            P(None, "tensor", "dp"),
            P("dp", None),
        ),
        out_specs=(
            P("dp", None),
            P("dp", None),
            P(None, "dp"),
            P(None, "dp", "tensor"),
            P(None, "dp", "tensor"),
            P(None, "dp", "tensor"),
            P(None, "tensor", "dp"),
            P(None, "dp"),
            P(None, "dp", "tensor"),
            P(None, "dp", "tensor"),
            P(None, "tensor", "dp"),
        ),
        check_vma=False,
    )
```

```python
import jax
import jax.numpy as jnp
import numpy as np
from jax import lax
from jax.experimental import pallas as pl
from jax.experimental.pallas import tpu as pltpu
from jax.sharding import PartitionSpec as P

HD = 64


epsilon = 1e-05
rope_base = 10000.0
masked_score = -1e30


def segment_positions(segment_ids):
    row_count, seq_len = segment_ids.shape
    index_grid = lax.broadcasted_iota(jnp.int32, (row_count, seq_len), 1)
    previous = jnp.concatenate([segment_ids[:, :1] - 1, segment_ids[:, :-1]], axis=1)
    starts = jnp.where(segment_ids != previous, index_grid, 0)
    return index_grid - lax.cummax(starts, axis=1)


def rope_tables(positions):
    half_dim = HD // 2
    inv_freq = rope_base ** (-(jnp.arange(half_dim, dtype=jnp.float32) * 2.0 / HD))
    angles = positions.astype(jnp.float32)[:, :, None] * inv_freq
    return (jnp.cos(angles), jnp.sin(angles))


def expand_table(table, values):
    extra_dims = values.ndim - 3
    return table.reshape(table.shape[:2] + (1,) * extra_dims + table.shape[2:])


def rotate_pairs(values, cos_t, sin_t):
    half_dim = values.shape[-1] // 2
    cos_e = expand_table(cos_t, values)
    sin_e = expand_table(sin_t, values)
    first, second = (values[..., :half_dim], values[..., half_dim:])
    return jnp.concatenate(
        [first * cos_e - second * sin_e, second * cos_e + first * sin_e], axis=-1
    )


def unrotate_pairs(values, cos_t, sin_t):
    half_dim = values.shape[-1] // 2
    cos_e = expand_table(cos_t, values)
    sin_e = expand_table(sin_t, values)
    first, second = (values[..., :half_dim], values[..., half_dim:])
    return jnp.concatenate(
        [first * cos_e + second * sin_e, second * cos_e - first * sin_e], axis=-1
    )


def attention_mask(segment_ids):
    seq_len = segment_ids.shape[1]
    same_seg = segment_ids[:, :, None] == segment_ids[:, None, :]
    query_pos = lax.broadcasted_iota(jnp.int32, (seq_len, seq_len), 0)
    key_pos = lax.broadcasted_iota(jnp.int32, (seq_len, seq_len), 1)
    return (same_seg & (key_pos <= query_pos))[:, None, None, :, :]


def score_block(query_heads, key_heads, allowed):
    scores = jnp.einsum(
        "rikgd,rjkd->rkgij", query_heads, key_heads, preferred_element_type=jnp.float32
    ) * HD ** (-0.5)
    return jnp.where(allowed, scores, masked_score)


def attend(query_heads, key_heads, value_heads, allowed):
    scores = score_block(query_heads, key_heads, allowed)
    row_max = jnp.max(scores, axis=-1, keepdims=True)
    log_norm = row_max + jnp.log(jnp.sum(jnp.exp(scores - row_max), axis=-1, keepdims=True))
    attn_probs = jnp.exp(scores - log_norm).astype(jnp.bfloat16)
    context = jnp.einsum(
        "rkgij,rjkd->rikgd", attn_probs, value_heads, preferred_element_type=jnp.float32
    )
    return (context.astype(jnp.bfloat16), log_norm)


def attend_back(query_heads, key_heads, value_heads, context, log_norm, grad_context, allowed):
    scores = score_block(query_heads, key_heads, allowed)
    probs_full = jnp.exp(scores - log_norm)
    probs_b = probs_full.astype(jnp.bfloat16)
    grad_v = jnp.einsum(
        "rkgij,rikgd->rjkd", probs_b, grad_context, preferred_element_type=jnp.float32
    )
    grad_probs = jnp.einsum(
        "rikgd,rjkd->rkgij", grad_context, value_heads, preferred_element_type=jnp.float32
    )
    delta = jnp.sum(grad_context.astype(jnp.float32) * context.astype(jnp.float32), axis=-1)
    delta = jnp.transpose(delta, (0, 2, 3, 1))[..., None]
    grad_scores = (probs_full * (grad_probs - delta)).astype(jnp.bfloat16)
    grad_q = jnp.einsum(
        "rkgij,rjkd->rikgd", grad_scores, key_heads, preferred_element_type=jnp.float32
    ) * HD ** (-0.5)
    grad_k = jnp.einsum(
        "rkgij,rikgd->rjkd", grad_scores, query_heads, preferred_element_type=jnp.float32
    ) * HD ** (-0.5)
    return (grad_q, grad_k, grad_v)


def contract_rows(left, right):
    return lax.dot_general(
        left, right, (((0,), (0,)), ((), ())), preferred_element_type=jnp.float32
    )


def contract_cols(left, right):
    return lax.dot_general(
        left, right, (((1,), (1,)), ((), ())), preferred_element_type=jnp.float32
    )


def norm_backward(resid, recip, gain, grad_normed):
    scaled = grad_normed * gain.astype(jnp.float32)
    grad_gain = jnp.sum(grad_normed * resid * recip, axis=0)
    grad_resid = recip * scaled - resid * (recip * recip * recip) * jnp.mean(
        scaled * resid, axis=-1, keepdims=True
    )
    return (grad_gain, grad_resid)


def layer_forward(resid, weights, cos_t, sin_t, allowed):
    gain_one, w_query, w_key, w_value, w_out, gain_two, w_gate, w_up, w_down = weights
    row_count, seq_len = (cos_t.shape[0], cos_t.shape[1])
    heads_here = w_query.shape[1] // HD
    kv_here = w_key.shape[1] // HD
    group_size = heads_here // kv_here
    recip_one = lax.rsqrt(jnp.mean(resid * resid, axis=-1, keepdims=True) + epsilon)
    normed_one = (resid * recip_one * gain_one.astype(jnp.float32)).astype(jnp.bfloat16)
    query_raw = jnp.dot(normed_one, w_query, preferred_element_type=jnp.float32)
    query_heads = rotate_pairs(
        query_raw.reshape(row_count, seq_len, kv_here, group_size, HD), cos_t, sin_t
    ).astype(jnp.bfloat16)
    key_raw = jnp.dot(normed_one, w_key, preferred_element_type=jnp.float32)
    key_heads = rotate_pairs(key_raw.reshape(row_count, seq_len, kv_here, HD), cos_t, sin_t).astype(
        jnp.bfloat16
    )
    value_raw = jnp.dot(normed_one, w_value, preferred_element_type=jnp.float32)
    value_heads = value_raw.reshape(row_count, seq_len, kv_here, HD).astype(jnp.bfloat16)
    context, log_norm = attend(query_heads, key_heads, value_heads, allowed)
    context_flat = context.reshape(row_count * seq_len, heads_here * HD)
    attn_sum = lax.psum(jnp.dot(context_flat, w_out, preferred_element_type=jnp.float32), "tensor")
    middle = resid + attn_sum
    recip_two = lax.rsqrt(jnp.mean(middle * middle, axis=-1, keepdims=True) + epsilon)
    normed_two = (middle * recip_two * gain_two.astype(jnp.float32)).astype(jnp.bfloat16)
    gate = jnp.dot(normed_two, w_gate, preferred_element_type=jnp.float32)
    up_proj = jnp.dot(normed_two, w_up, preferred_element_type=jnp.float32)
    hidden_act = (jax.nn.silu(gate) * up_proj).astype(jnp.bfloat16)
    feed_out = lax.psum(jnp.dot(hidden_act, w_down, preferred_element_type=jnp.float32), "tensor")
    kept_state = (
        resid,
        recip_one,
        normed_one,
        query_heads,
        key_heads,
        value_heads,
        context,
        log_norm,
        middle,
        recip_two,
        normed_two,
        gate,
        up_proj,
        hidden_act,
    )
    return (middle + feed_out, kept_state)


def backward_layer(grad_resid, kept_state, weights, cos_t, sin_t, allowed):
    (
        resid,
        recip_one,
        normed_one,
        query_heads,
        key_heads,
        value_heads,
        context,
        log_norm,
        middle,
        recip_two,
        normed_two,
        gate,
        up_proj,
        hidden_act,
    ) = kept_state
    gain_one, w_query, w_key, w_value, w_out, gain_two, w_gate, w_up, w_down = weights
    token_count = resid.shape[0]
    grad_b = grad_resid.astype(jnp.bfloat16)
    grad_down = contract_rows(hidden_act, grad_b)
    grad_hidden = contract_cols(grad_b, w_down)
    sigma = jax.nn.sigmoid(gate)
    grad_gate_b = (grad_hidden * up_proj * sigma * (1.0 + gate * (1.0 - sigma))).astype(
        jnp.bfloat16
    )
    grad_up_b = (grad_hidden * (gate * sigma)).astype(jnp.bfloat16)
    grad_gate_w = contract_rows(normed_two, grad_gate_b)
    grad_up_w = contract_rows(normed_two, grad_up_b)
    grad_normed_two = lax.psum(
        contract_cols(grad_gate_b, w_gate) + contract_cols(grad_up_b, w_up), "tensor"
    )
    grad_gain_two, grad_mid_norm = norm_backward(middle, recip_two, gain_two, grad_normed_two)
    grad_middle = grad_resid + grad_mid_norm
    middle_b = grad_middle.astype(jnp.bfloat16)
    context_flat = context.reshape(token_count, -1)
    grad_out_w = contract_rows(context_flat, middle_b)
    grad_context = contract_cols(middle_b, w_out).astype(jnp.bfloat16).reshape(context.shape)
    grad_q, grad_k, grad_v = attend_back(
        query_heads, key_heads, value_heads, context, log_norm, grad_context, allowed
    )
    grad_q = unrotate_pairs(grad_q, cos_t, sin_t).astype(jnp.bfloat16).reshape(token_count, -1)
    grad_k = unrotate_pairs(grad_k, cos_t, sin_t).astype(jnp.bfloat16).reshape(token_count, -1)
    grad_v = grad_v.astype(jnp.bfloat16).reshape(token_count, -1)
    grad_query_w = contract_rows(normed_one, grad_q)
    grad_key_w = contract_rows(normed_one, grad_k)
    grad_value_w = contract_rows(normed_one, grad_v)
    grad_normed_one = lax.psum(
        contract_cols(grad_q, w_query)
        + contract_cols(grad_k, w_key)
        + contract_cols(grad_v, w_value),
        "tensor",
    )
    grad_gain_one, grad_res_norm = norm_backward(resid, recip_one, gain_one, grad_normed_one)
    grad_input = grad_middle + grad_res_norm
    layer_grads = (
        lax.psum_scatter(grad_gain_one, "dp", scatter_dimension=0, tiled=True),
        lax.psum_scatter(grad_query_w, "dp", scatter_dimension=0, tiled=True),
        lax.psum_scatter(grad_key_w, "dp", scatter_dimension=0, tiled=True),
        lax.psum_scatter(grad_value_w, "dp", scatter_dimension=0, tiled=True),
        lax.psum_scatter(grad_out_w, "dp", scatter_dimension=1, tiled=True),
        lax.psum_scatter(grad_gain_two, "dp", scatter_dimension=0, tiled=True),
        lax.psum_scatter(grad_gate_w, "dp", scatter_dimension=0, tiled=True),
        lax.psum_scatter(grad_up_w, "dp", scatter_dimension=0, tiled=True),
        lax.psum_scatter(grad_down, "dp", scatter_dimension=1, tiled=True),
    )
    return (grad_input, tuple(layer_grads))


def body(
    hidden_in,
    segment_ids,
    gain_attn,
    w_query,
    w_key,
    w_value,
    w_out,
    gain_ffn,
    w_gate,
    w_up,
    w_down,
    cotangent,
):
    cos_t, sin_t = rope_tables(segment_positions(segment_ids))
    allowed = attention_mask(segment_ids)
    layer_count = w_query.shape[0]
    resid = hidden_in
    retained = []
    layer_no = 0
    gathered = (
        lax.all_gather(gain_attn[layer_no], "dp", axis=0, tiled=True),
        lax.all_gather(w_query[layer_no], "dp", axis=0, tiled=True),
        lax.all_gather(w_key[layer_no], "dp", axis=0, tiled=True),
        lax.all_gather(w_value[layer_no], "dp", axis=0, tiled=True),
        lax.all_gather(w_out[layer_no], "dp", axis=1, tiled=True),
        lax.all_gather(gain_ffn[layer_no], "dp", axis=0, tiled=True),
        lax.all_gather(w_gate[layer_no], "dp", axis=0, tiled=True),
        lax.all_gather(w_up[layer_no], "dp", axis=0, tiled=True),
        lax.all_gather(w_down[layer_no], "dp", axis=1, tiled=True),
    )
    retained.append(gathered)
    resid, kept_state = layer_forward(resid, gathered, cos_t, sin_t, allowed)
    states = [kept_state]
    grad_resid = cotangent
    collected = [None] * layer_count
    for layer_no in reversed(range(layer_count)):
        gathered = (
            lax.all_gather(gain_attn[layer_no], "dp", axis=0, tiled=True),
            lax.all_gather(w_query[layer_no], "dp", axis=0, tiled=True),
            lax.all_gather(w_key[layer_no], "dp", axis=0, tiled=True),
            lax.all_gather(w_value[layer_no], "dp", axis=0, tiled=True),
            lax.all_gather(w_out[layer_no], "dp", axis=1, tiled=True),
            lax.all_gather(gain_ffn[layer_no], "dp", axis=0, tiled=True),
            lax.all_gather(w_gate[layer_no], "dp", axis=0, tiled=True),
            lax.all_gather(w_up[layer_no], "dp", axis=0, tiled=True),
            lax.all_gather(w_down[layer_no], "dp", axis=1, tiled=True),
        )
        grad_resid, collected[layer_no] = backward_layer(
            grad_resid, states[layer_no], gathered, cos_t, sin_t, allowed
        )
    stacked = tuple((jnp.stack([collected[0][member]]) for member in range(9)))
    return (
        resid,
        grad_resid,
        stacked[0],
        stacked[1],
        stacked[2],
        stacked[3],
        stacked[4],
        stacked[5],
        stacked[6],
        stacked[7],
        stacked[8],
    )


ZN = 4
MESH = pl.DeviceIdType.MESH
BF = jnp.bfloat16
F32 = jnp.float32
LANE = 128


def place():
    dp = lax.axis_index("dp")
    return dp // 4, (dp // 2) % 2, dp % 2, lax.axis_index("tensor")


def dev(z, x, c, y):
    return (z * 4 + x * 2 + c, y)


def rid(z, x, c):
    return (z * 2 + x) * 2 + c


def lanes(r, width=LANE):
    return pl.ds(pl.multiple_of(r * width, LANE), width)


def rows(r, height):
    return pl.ds(pl.multiple_of(r * height, 16), height)


def tokens(o, pitch, count):
    return pl.ds(pl.multiple_of(o * pitch, 16), count)


def greet(peers):
    barrier = pltpu.get_barrier_semaphore()
    for peer in peers:
        pl.semaphore_signal(barrier, inc=1, device_id=peer, device_id_type=MESH)
    pl.semaphore_wait(barrier, len(peers))


class Wire:
    def __init__(self, send_sem, recv_sem):
        self.send_sem = send_sem
        self.recv_sem = recv_sem
        self.started = []

    def make(self, src, dst, si, ri, to):
        return pltpu.make_async_remote_copy(
            src_ref=src,
            dst_ref=dst,
            send_sem=self.send_sem.at[si],
            recv_sem=self.recv_sem.at[ri],
            device_id=to,
            device_id_type=MESH,
        )

    def send(self, src, dst, si, ri, to, cond=None):
        def go():
            self.make(src, dst, si, ri, to).start()

        def done():
            self.make(src, dst, si, ri, to).wait_send()

        if cond is None:
            go()
            self.started.append(done)
        else:
            pl.when(cond)(go)
            self.started.append(lambda: pl.when(cond)(done))

    def arrived(self, dst, ri, to, cond=None):
        def wait():
            self.make(dst, dst, 0, ri, to).wait_recv()

        if cond is None:
            wait()
        else:
            pl.when(cond)(wait)

    def drain(self):
        for done in self.started:
            done()


def all_peers(z, x, c, y):
    near = [dev(z, x, 1 - c, y), dev(z, 1 - x, c, y), dev(z, x, c, 1 - y)]
    return near + [dev((z + d) % ZN, x, c, y) for d in (1, 2, 3)]


def params(cid):
    return pltpu.CompilerParams(
        collective_id=cid, has_side_effects=True, vmem_limit_bytes=67043328
    )


def any_spec():
    return pl.BlockSpec(memory_space=pl.ANY)


def vm_spec():
    return pl.BlockSpec(memory_space=pltpu.VMEM)


def sems(n):
    return pltpu.SemaphoreType.DMA((n,))


def dot_nn(a, b):
    return lax.dot_general(a, b, (((1,), (0,)), ((), ())), preferred_element_type=F32)


def dot_nt(a, b):
    return lax.dot_general(a, b, (((1,), (1,)), ((), ())), preferred_element_type=F32)


def dot_tn(a, b):
    return lax.dot_general(a, b, (((0,), (0,)), ((), ())), preferred_element_type=F32)


def by_rows(height, step, one):
    def wrapped(i, carry):
        one(pl.ds(pl.multiple_of(i * step, step), step))
        return carry

    lax.fori_loop(0, height // step, wrapped, 0)


def add_into(dst, src, height, step):
    def one(r):
        dst[r, :] = (dst[r, :].astype(F32) + src[r, :].astype(F32)).astype(dst.dtype)

    by_rows(height, step, one)


def swap_halves(v):
    lane = lax.broadcasted_iota(jnp.int32, v.shape, 1)
    first = (lane % HD) < (HD // 2)
    return jnp.where(first, pltpu.roll(v, LANE - HD // 2, 1), pltpu.roll(v, HD // 2, 1))


def spread_pair(dst, pair):
    lane = lax.broadcasted_iota(jnp.int32, pair.shape, 1)
    low = lane < HD
    turned = pltpu.roll(pair, HD, 1)
    zero = jnp.zeros_like(pair)
    dst[0] = jnp.where(low, pair, zero).astype(BF)
    dst[1] = jnp.where(low, zero, turned).astype(BF)
    dst[2] = jnp.where(low, turned, zero).astype(BF)
    dst[3] = jnp.where(low, zero, pair).astype(BF)


class Line:
    def __init__(self, wire, own, buf, send_base, recv_base):
        self.wire, self.own, self.buf = wire, own, buf
        self.s, self.r = send_base, recv_base
        self.pitch = buf.shape[0] // ZN
        z, x, c, y = place()
        self.z, self.y = z, y
        self.up, self.down = dev(z + 1, x, c, y), dev(z - 1, x, c, y)
        self.other = dev(z, x, c, 1 - y)
        self.seq, self.half = own.shape[0], own.shape[1] // 2

    def blk(self, o, h):
        return self.buf.at[tokens(o, self.pitch, self.seq), lanes(h, self.half)]

    def start(self):
        z, wire = self.z, self.wire
        src = self.own.at[:, lanes(self.y, self.half)]
        dst = self.blk(z, self.y)
        wire.send(src, dst, self.s + z, self.r + z, self.up, z < ZN - 1)
        wire.send(src, dst, self.s + 4 + z, self.r + z, self.down, z > 0)

    def relay(self, s):
        z, wire = self.z, self.wire
        for o, cond, fwd, to, frm, base in (
            (z - s, z >= s, z < ZN - 1, self.up, self.down, 0),
            (z + s, z + s < ZN, z > 0, self.down, self.up, 4),
        ):
            b = self.blk(o, self.y)
            wire.arrived(b, self.r + o, frm, cond)
            wire.send(b, b, self.s + base + o, self.r + o, to, cond & fwd)
            wire.send(b, b, self.s + 8 + o, self.r + 4 + o, self.other, cond)

    def half_of(self, o):
        self.wire.arrived(self.blk(o, 1 - self.y), self.r + 4 + o, self.other)


class Chain:
    def __init__(self, wire, held, zin, height, step, send_base, recv_base):
        self.wire, self.held, self.zin = wire, held, zin
        self.height, self.step = height, step
        self.s, self.r = send_base, recv_base
        self.z, x, c, y = place()
        self.up, self.down = dev(self.z + 1, x, c, y), dev(self.z - 1, x, c, y)

    def inbound(self, o, slot, frm, cond):
        self.wire.arrived(self.zin(slot), self.r + slot, frm, cond)

        @pl.when(cond)
        def _():
            add_into(self.held(o), self.zin(slot), self.height, self.step)

    def outward(self, t, ready):
        z = self.z
        for o, cond, more, to, frm, base, slot in (
            (z + t, z + t < ZN, z > 0, self.up, self.down, 0, z + t),
            (z - t, z >= t, z < ZN - 1, self.down, self.up, 4, 4 if t == 1 else z - t),
        ):
            ready(o, cond)
            self.inbound(o, o, frm, cond & more)
            self.wire.send(
                self.held(o), self.zin(slot), self.s + base + o, self.r + slot, to, cond
            )

    def home(self):
        z = self.z
        self.inbound(z, z, self.down, z > 0)
        self.inbound(z, 4, self.up, z < ZN - 1)


class Tree:
    def __init__(self, wire, own, blk, send_base, recv_base):
        self.wire, self.own, self.blk = wire, own, blk
        self.s, self.r = send_base, recv_base
        self.z, self.x, self.c, y = place()
        z, x, c = self.z, self.x, self.c
        self.up, self.down = dev(z + 1, x, c, y), dev(z - 1, x, c, y)
        self.side, self.twin = dev(z, 1 - x, c, y), dev(z, x, 1 - c, y)

    def start_z(self):
        z, wire = self.z, self.wire
        d = self.blk(rid(z, self.x, self.c))
        wire.send(self.own, d, self.s + z, self.r + z, self.up, z < ZN - 1)
        wire.send(self.own, d, self.s + 4 + z, self.r + z, self.down, z > 0)

    def start_near(self):
        z, wire = self.z, self.wire
        d = self.blk(rid(z, self.x, self.c))
        wire.send(self.own, d, self.s + 8 + z, self.r + 4 + z, self.side)
        k = z * 2 + self.x
        wire.send(self.own, d, self.s + 12 + k, self.r + 8 + k, self.twin)

    def start(self):
        self.start_z()
        self.start_near()

    def relay(self, s):
        z, wire = self.z, self.wire
        for o, cond, fwd, to, frm, base in (
            (z - s, z >= s, z < ZN - 1, self.up, self.down, 0),
            (z + s, z + s < ZN, z > 0, self.down, self.up, 4),
        ):
            b = self.blk(rid(o, self.x, self.c))
            wire.arrived(b, self.r + o, frm, cond)
            wire.send(b, b, self.s + base + o, self.r + o, to, cond & fwd)
            wire.send(b, b, self.s + 8 + o, self.r + 4 + o, self.side, cond)
            k = o * 2 + self.x
            wire.send(b, b, self.s + 12 + k, self.r + 8 + k, self.twin, cond)

    def across(self, s):
        z = self.z
        todo = ((z, None),) if s == 0 else ((z - s, z >= s), (z + s, z + s < ZN))
        for o, cond in todo:
            b = self.blk(rid(o, 1 - self.x, self.c))
            self.wire.arrived(b, self.r + 4 + o, self.side, cond)
            k = o * 2 + 1 - self.x
            self.wire.send(b, b, self.s + 12 + k, self.r + 8 + k, self.twin, cond)

    def finish(self):
        for o in range(ZN):
            for xx in (0, 1):
                b = self.blk(rid(o, xx, 1 - self.c))
                self.wire.arrived(b, self.r + 8 + o * 2 + xx, self.twin)


def front_kernel(
    resid_h, wq_l, wk_l, wv_l, wo_l, g1_l, g2_l, wg_h, wu_h, wd_h, cot_h, seg, freq,
    wqkv_o, wo_o, ga, n1_o, q_o, kv, ctx_o, mid_o, cos_t, sin_t, mask, dn, feed_out, g3_out,
    wqkv, wo, n1, q, ctx, mid, zin, w3, dres, normed, hid_t, dg_t, du_t, hid, dg, du, dnp, yin, stage,
    resid, wg_l, wu_l, cot, ga_l, qkv_l, w3_l, dres_l, kx, vx, attn, part, nrm, ss, rs, ls,
):
    z, x, c, y = place()
    units = w3.shape[1]
    seq, width = resid.shape
    half = width // 2
    pitch = normed.shape[0] // ZN
    q_width = q.shape[1]
    pairs = q_width // LANE
    loads = [
        pltpu.make_async_copy(cot_h, cot, ls.at[6]),
        pltpu.make_async_copy(wg_h.at[0], wg_l, ls.at[7]),
        pltpu.make_async_copy(wu_h.at[0], wu_l, ls.at[8]),
        pltpu.make_async_copy(wd_h.at[0], w3_l.at[2], ls.at[9]),
        pltpu.make_async_copy(resid_h, resid, ls.at[10]),
    ]
    for cp in loads:
        cp.start()
    wire = Wire(ss, rs)
    side, twin, other = dev(z, 1 - x, c, y), dev(z, x, 1 - c, y), dev(z, x, c, 1 - y)
    qkv_l[:, pl.ds(0, q_width)] = wq_l[0]
    qkv_l[:, pl.ds(q_width, LANE)] = wk_l[0]
    qkv_l[:, pl.ds(q_width + LANE, LANE)] = wv_l[0]
    row = lax.broadcasted_iota(jnp.int32, (16, LANE), 0)
    two = jnp.where(row == 0, g1_l[...].astype(F32), g2_l[...].astype(F32))
    ga_l[...] = jnp.where(row < 2, two, 0.0).astype(BF)
    greet(all_peers(z, x, c, y))

    def qkv_blk(r):
        return wqkv.at[pl.ds(pl.multiple_of(r * LANE, LANE), LANE), :]

    def wo_blk(r):
        return wo.at[:, lanes(r)]

    def ga_blk(r):
        return ga.at[:, lanes(r)]

    def ffn(r):
        return w3.at[:, :, lanes(r)]

    t_qkv = Tree(wire, qkv_l, qkv_blk, 0, 0)
    t_wo = Tree(wire, wo_l.at[0], wo_blk, 20, 16)
    t_ga = Tree(wire, ga_l, ga_blk, 40, 32)
    l_dres = Line(wire, dres_l, dres, 76, 64)
    l_norm = Line(wire, nrm, normed, 88, 72)
    mine = rid(z, x, c)
    t_ga.start()
    t_qkv.start()
    own = [
        pltpu.make_async_copy(qkv_l, qkv_blk(mine), ls.at[0]),
        pltpu.make_async_copy(wo_l.at[0], wo_blk(mine), ls.at[1]),
        pltpu.make_async_copy(ga_l, ga_blk(mine), ls.at[2]),
    ]
    for cp in own:
        cp.start()

    def round_cot(r):
        dres_l[r, :] = cot[r, :].astype(BF)

    def turn(i, carry):
        cut = lanes(i)
        w3_l[0, pl.ds(pl.multiple_of(i * LANE, LANE), LANE), :] = (
            wg_l[:, cut].astype(F32).T.astype(BF)
        )
        w3_l[1, pl.ds(pl.multiple_of(i * LANE, LANE), LANE), :] = (
            wu_l[:, cut].astype(F32).T.astype(BF)
        )
        return carry

    def turned(v):
        return v * cos_t[...] + swap_halves(v) * sin_t[...]

    def q_tile(j, carry):
        acc = dot_nn(n1[...], wqkv[:, lanes(j, 2 * LANE)])
        for h in (0, 1):
            q[:, lanes(2 * j + h)] = turned(acc[:, h * LANE : (h + 1) * LANE]).astype(BF)
        return carry

    def pair(p, carry):
        qp = q[:, lanes(p)]
        g = p // (pairs // 2)
        out = jnp.zeros((seq, LANE), F32)
        for h in (0, 1):
            s = dot_nt(qp, kx[2 * g + h]) * HD ** (-0.5)
            s = jnp.where(mask[...] > 0.0, s, masked_score)
            top = jnp.max(s, axis=-1, keepdims=True)
            lse = top + jnp.log(jnp.sum(jnp.exp(s - top), axis=-1, keepdims=True))
            out = out + dot_nn(jnp.exp(s - lse).astype(BF), vx[2 * g + h])
        ctx[:, lanes(p)] = out.astype(BF)
        return carry

    ids = jnp.broadcast_to(seg[...].astype(F32), (seq, seq))
    own_id = lax.broadcasted_iota(jnp.int32, (seq, seq), 0)
    key_id = lax.broadcasted_iota(jnp.int32, (seq, seq), 1)
    mine_id = jnp.sum(jnp.where(own_id == key_id, ids, 0.0), axis=1, keepdims=True)
    seen = jnp.where((ids == mine_id) & (key_id <= own_id), 1.0, 0.0)
    mask[...] = seen
    angles = (jnp.sum(seen, axis=1, keepdims=True) - 1.0) * freq[...]
    lane = lax.broadcasted_iota(jnp.int32, (seq, LANE), 1)
    cos_t[...] = jnp.cos(angles)
    sin_t[...] = jnp.where(lane % HD < HD // 2, -1.0, 1.0) * jnp.sin(angles)
    for o in range(ZN):
        gap = pl.ds(o * pitch + seq, pitch - seq)
        normed[gap, :] = jnp.zeros((pitch - seq, width), BF)
        dres[gap, :] = jnp.zeros((pitch - seq, width), BF)
    loads[0].wait()
    by_rows(seq, 16, round_cot)
    t_ga.relay(1)
    t_qkv.relay(1)
    t_ga.across(0)
    t_qkv.across(0)
    t_ga.relay(2)
    t_qkv.relay(2)
    t_wo.start_z()
    for cp in loads[1:]:
        cp.wait()
    lax.fori_loop(0, w3_l.shape[1] // LANE, turn, 0)
    t_ga.across(1)
    t_qkv.across(1)
    t_ga.relay(3)
    t_qkv.relay(3)
    t_wo.start_near()
    t_ga.across(2)
    t_ga.across(3)
    t_ga.finish()
    own[2].wait()
    gain_one = ga[pl.ds(0, 8), :].astype(F32)[0:1]
    gain_two = ga[pl.ds(0, 8), :].astype(F32)[1:2]

    def norm_one(r):
        v = resid[r, :]
        recip = lax.rsqrt(jnp.mean(v * v, axis=-1, keepdims=True) + epsilon)
        n1[r, :] = (v * recip * gain_one).astype(BF)

    by_rows(seq, 16, norm_one)
    t_wo.relay(1)
    t_qkv.across(2)
    t_wo.relay(2)
    for d in (2, 1, 3):
        zt = (z + d) % ZN
        wire.send(w3_l.at[:, rows(zt, units), :], ffn(mine), 60 + d - 1, 48 + z, dev(zt, x, c, y))
    l_dres.start()
    t_qkv.across(3)
    t_qkv.finish()
    own[0].wait()
    lax.fori_loop(0, pairs // 2, q_tile, 0)
    acc = dot_nn(n1[...], wqkv[:, pl.ds(q_width, 2 * LANE)])
    key = turned(acc[:, :LANE]).astype(BF)
    val = acc[:, LANE:].astype(BF)
    kv[:, pl.ds(0, LANE)] = key
    kv[:, pl.ds(LANE, LANE)] = val
    spread_pair(kx, key.astype(F32))
    spread_pair(vx, val.astype(F32))
    t_wo.across(0)
    t_wo.relay(3)
    mine3 = w3_l.at[:, rows(z, units), :]
    wire.send(mine3, ffn(mine), 64 + z, 52 + z, side)
    wire.send(mine3, ffn(mine), 68 + z * 2 + x, 56 + z * 2 + x, twin)
    own += [
        pltpu.make_async_copy(mine3, ffn(mine), ls.at[3]),
        pltpu.make_async_copy(dres_l, dres.at[tokens(z, pitch, seq), :], ls.at[4]),
    ]
    own[3].start()
    own[4].start()
    lax.fori_loop(0, pairs, pair, 0)
    for s in (1, 2, 3):
        t_wo.across(s)
    t_wo.finish()
    own[1].wait()

    def out_tile(j, carry):
        cut = lanes(j, 2 * LANE)
        attn[:, cut] = dot_nn(ctx[...], wo[:, cut]).astype(BF)
        return carry

    lax.fori_loop(0, width // (2 * LANE), out_tile, 0)
    wire.send(attn, part, 100, 80, other)
    kept = [
        pltpu.make_async_copy(a, b, ls.at[17 + i])
        for i, (a, b) in enumerate(
            ((wqkv, wqkv_o), (wo, wo_o), (n1, n1_o), (q, q_o), (ctx, ctx_o), (mid, mid_o))
        )
    ]
    for cp in kept[:5]:
        cp.start()

    def ffn_in(d):
        o = (z + ZN - d) % ZN
        b = ffn(rid(o, x, c))
        wire.arrived(b, 48 + o, dev(o, x, c, y))
        wire.send(b, b, 64 + o, 52 + o, side)
        wire.send(b, b, 68 + o * 2 + x, 56 + o * 2 + x, twin)

    def ffn_across(d):
        o = (z + ZN - d) % ZN
        b = ffn(rid(o, 1 - x, c))
        wire.arrived(b, 52 + o, side)
        k = o * 2 + 1 - x
        wire.send(b, b, 68 + k, 56 + k, twin)

    def second(r):
        m = resid[r, :] + (attn[r, :].astype(F32) + part[r, :].astype(F32))
        mid[r, :] = m
        recip = lax.rsqrt(jnp.mean(m * m, axis=-1, keepdims=True) + epsilon)
        nrm[r, :] = (m * recip * gain_two).astype(BF)

    ffn_in(2)
    wire.arrived(part, 80, other)
    by_rows(seq, 16, second)
    l_norm.start()
    kept[5].start()
    own.append(pltpu.make_async_copy(nrm, normed.at[tokens(z, pitch, seq), :], ls.at[5]))
    own[5].start()
    ffn_in(1)
    ffn_across(0)
    ffn_in(3)
    l_dres.relay(1)
    ffn_across(2)
    l_norm.relay(1)
    l_dres.relay(2)
    ffn_across(1)
    ffn_across(3)
    for o in range(ZN):
        for xx in (0, 1):
            wire.arrived(ffn(rid(o, xx, 1 - c)), 56 + o * 2 + xx, twin)
    for cp in own[3:]:
        cp.wait()
    step = units // 2

    def ffn_block(o):
        r = tokens(o, pitch, pitch)

        def some_units(i, carry):
            u = pl.ds(pl.multiple_of(i * step, 16), step)
            g = dot_nt(w3[0, u, :], normed[r, :])
            up = dot_nt(w3[1, u, :], normed[r, :])
            dh = dot_nt(w3[2, u, :], dres[r, :])
            s = jax.nn.sigmoid(g)
            hid_t[u, lanes(o, pitch)] = (g * s * up).astype(BF)
            dg_t[u, lanes(o, pitch)] = (dh * up * s * (1.0 + g * (1.0 - s))).astype(BF)
            du_t[u, lanes(o, pitch)] = (dh * (g * s)).astype(BF)
            return carry

        lax.fori_loop(0, units // step, some_units, 0)
        dg[...] = dg_t[:, lanes(o, pitch)].astype(F32).T[:seq].astype(BF)
        du[...] = du_t[:, lanes(o, pitch)].astype(F32).T[:seq].astype(BF)
        hid[rows(o, seq), :] = hid_t[:, lanes(o, pitch)].astype(F32).T[:seq].astype(BF)

        def some_lanes(j, carry):
            cut = lanes(j, 2 * LANE)
            dnp[o, :, cut] = (dot_nn(dg[...], w3[0, :, cut]) + dot_nn(du[...], w3[1, :, cut])).astype(BF)
            return carry

        lax.fori_loop(0, width // (2 * LANE), some_lanes, 0)

    def far_half(o):
        part = dnp.at[o].at[:, lanes(1 - y, half)]
        wire.send(part, yin.at[o], 101 + o, 81 + o, other)

    o1 = z + 1 - 2 * ((z + 3) // 4)
    o3 = 3 - 3 * (z // 2)
    o2 = 6 - z - o1 - o3

    def both_halves(o):
        l_dres.half_of(o)
        l_norm.half_of(o)

    ffn_block(z)
    l_norm.relay(2)
    l_dres.relay(3)
    both_halves(o1)
    ffn_block(o1)
    l_norm.relay(3)
    both_halves(o2)
    ffn_block(o2)
    far_half(o2)
    both_halves(o3)
    ffn_block(o3)
    for o in (o3, o1, z):
        far_half(o)

    wide = 4 * LANE
    tiles = width // wide

    def columns(first, value, dst):
        def one(j, carry):
            slot = j % 2
            cp = pltpu.make_async_copy(stage.at[slot], dst(j), ls.at[11 + slot])
            if first:
                pl.when(j >= 2)(cp.wait)
            else:
                cp.wait()
            stage[slot] = value(lanes(j, wide)).astype(BF)
            cp.start()
            return carry

        lax.fori_loop(0, tiles, one, 0)

    def over_tokens(act, kept):
        return lambda cut: dot_nn(act[...], kept[:, cut])

    def grad_dst(m):
        return lambda j: g3_out.at[m, :, lanes(j, wide)]

    quarter = half // 2

    def part_chain(h):
        cut = pl.ds(h * quarter, quarter)
        return Chain(
            wire,
            lambda o: yin.at[o].at[:, cut],
            lambda k: zin.at[k].at[:, cut],
            seq, 16, 105 + 8 * h, 85 + 5 * h,
        )

    lines = [part_chain(0), part_chain(1)]

    def outward(t):
        lines[0].outward(t, dn_ready)
        lines[1].outward(t, lambda o, cond: None)


    def dn_ready(o, cond):
        wire.arrived(yin.at[o], 81 + o, other, cond)

        @pl.when(cond)
        def _():
            add_into(yin.at[o], dnp.at[o].at[:, lanes(y, half)], seq, 16)

    columns(True, over_tokens(dg_t, normed), grad_dst(0))
    outward(3)
    columns(False, over_tokens(du_t, normed), grad_dst(1))
    outward(2)
    columns(False, over_tokens(hid_t, dres), grad_dst(2))
    outward(1)
    columns(False, lambda cut: dot_nn(hid[...], w3[2, :, cut]), lambda j: feed_out.at[:, lanes(j, wide)])
    dn_ready(z, z >= 0)
    for line in lines:
        line.home()

    keep_dn = pltpu.make_async_copy(yin.at[z], dn, ls.at[13])
    keep_dn.start()
    wire.drain()
    for slot in (0, 1):
        pltpu.make_async_copy(stage.at[slot], feed_out.at[:, lanes(slot, wide)], ls.at[11 + slot]).wait()
    for cp in kept:
        cp.wait()
    keep_dn.wait()


def front(resid, w_query, w_key, w_value, w_out, g1, g2, w_gate, w_up, w_down, cot, seg):
    seq, width = resid.shape
    q_width, out_rows = w_query.shape[2], w_out.shape[1]
    total = q_width + 2 * LANE
    units = w_gate.shape[2] // ZN
    pair_shape = (4, seq, LANE)
    pitch = pl.cdiv(seq, LANE) * LANE
    freq = rope_base ** (-(np.arange(LANE) % (HD // 2)) * 2.0 / HD)
    freq = jnp.asarray(freq[None].astype(np.float32))
    vm, hb = vm_spec(), any_spec()
    return pl.pallas_call(
        front_kernel,
        name="front",
        out_shape=(
            jax.ShapeDtypeStruct((width, total), BF),
            jax.ShapeDtypeStruct((out_rows, width), BF),
            jax.ShapeDtypeStruct((16, width), BF),
            jax.ShapeDtypeStruct((seq, width), BF),
            jax.ShapeDtypeStruct((seq, q_width), BF),
            jax.ShapeDtypeStruct((seq, 2 * LANE), BF),
            jax.ShapeDtypeStruct((seq, q_width), BF),
            jax.ShapeDtypeStruct((seq, width), F32),
            jax.ShapeDtypeStruct((seq, LANE), F32),
            jax.ShapeDtypeStruct((seq, LANE), F32),
            jax.ShapeDtypeStruct((seq, seq), F32),
            jax.ShapeDtypeStruct((seq, width // 2), BF),
            jax.ShapeDtypeStruct((seq * ZN, width), BF),
            jax.ShapeDtypeStruct((3, units, width), BF),
        ),
        in_specs=[hb] + [vm] * 6 + [hb] * 4 + [vm] * 2,
        out_specs=[hb] * 2 + [vm] + [hb] * 2 + [vm] + [hb] * 2 + [vm] * 3 + [hb] * 3,
        scratch_shapes=[
            pltpu.VMEM((width, total), BF),
            pltpu.VMEM((out_rows, width), BF),
            pltpu.VMEM((seq, width), BF),
            pltpu.VMEM((seq, q_width), BF),
            pltpu.VMEM((seq, q_width), BF),
            pltpu.VMEM((seq, width), F32),
            pltpu.VMEM((5, seq, width // 2), BF),
            pltpu.VMEM((3, units, width), BF),
            pltpu.VMEM((pitch * ZN, width), BF),
            pltpu.VMEM((pitch * ZN, width), BF),
            pltpu.VMEM((units, pitch * ZN), BF),
            pltpu.VMEM((units, pitch * ZN), BF),
            pltpu.VMEM((units, pitch * ZN), BF),
            pltpu.VMEM((seq * ZN, units), BF),
            pltpu.VMEM((seq, units), BF),
            pltpu.VMEM((seq, units), BF),
            pltpu.VMEM((ZN, seq, width), BF),
            pltpu.VMEM((ZN, seq, width // 2), BF),
            pltpu.VMEM((2, seq * ZN, 4 * LANE), BF),
            pltpu.VMEM((seq, width), F32),
            pltpu.VMEM((LANE, units * ZN), BF),
            pltpu.VMEM((LANE, units * ZN), BF),
            pltpu.VMEM((seq, width), F32),
            pltpu.VMEM((16, LANE), BF),
            pltpu.VMEM((LANE, total), BF),
            pltpu.VMEM((3, units * ZN, LANE), BF),
            pltpu.VMEM((seq, width), BF),
            pltpu.VMEM(pair_shape, BF),
            pltpu.VMEM(pair_shape, BF),
            pltpu.VMEM((seq, width), BF),
            pltpu.VMEM((seq, width), BF),
            pltpu.VMEM((seq, width), BF),
            sems(121),
            sems(95),
            sems(23),
        ],
        compiler_params=params(0),
    )(resid, w_query, w_key, w_value, w_out, g1, g2, w_gate, w_up, w_down, cot, seg, freq)


class Fold:
    def __init__(self, wire, part, cin, xin, zin, height, step, send_base, recv_base):
        self.wire, self.part, self.cin, self.xin = wire, part, cin, xin
        self.height, self.step = height, step
        self.s, self.r = send_base, recv_base
        self.z, self.x, self.c, y = place()
        z, x, c = self.z, self.x, self.c
        self.side, self.twin = dev(z, 1 - x, c, y), dev(z, x, 1 - c, y)
        self.chain = Chain(
            wire, lambda o: xin.at[o], lambda s: zin.at[s], height, step, self.s + 12, self.r + 12
        )

    def order(self):
        return [(self.z + d) % ZN for d in (2, 1, 3, 0)]

    def to_twin(self):
        for xx in (1 - self.x, self.x):
            for o in self.order():
                k = o * 2 + xx
                self.wire.send(
                    self.part(k * 2 + 1 - self.c), self.cin.at[k], self.s + k, self.r + k, self.twin
                )

    def from_twin(self, k):
        self.wire.arrived(self.cin.at[k], self.r + k, self.twin)
        add_into(self.cin.at[k], self.part(k * 2 + self.c), self.height, self.step)

    def from_twin_if(self, k, cond):
        self.wire.arrived(self.cin.at[k], self.r + k, self.twin, cond)

        @pl.when(cond)
        def _():
            add_into(self.cin.at[k], self.part(k * 2 + self.c), self.height, self.step)

    def across_one(self, o, cond=None):
        k = o * 2 + 1 - self.x
        if cond is None:
            self.from_twin(k)
        else:
            self.from_twin_if(k, cond)
        self.wire.send(
            self.cin.at[k], self.xin.at[o], self.s + 8 + o, self.r + 8 + o, self.side, cond
        )

    def across(self):
        z = self.z
        for t in (3, 2, 1):
            self.across_one(z + t, z + t < ZN)
            self.across_one(z - t, z >= t)
        self.across_one(z)

    def stay(self):
        for o in self.order():
            self.from_twin(o * 2 + self.x)

    def ready(self, o, cond):
        self.wire.arrived(self.xin.at[o], self.r + 8 + o, self.side, cond)

        @pl.when(cond)
        def _():
            add_into(self.xin.at[o], self.cin.at[o * 2 + self.x], self.height, self.step)

    def outward(self, t):
        self.chain.outward(t, self.ready)

    def home(self):
        self.ready(self.z, self.z >= 0)
        self.chain.home()
        return self.xin.at[self.z]


def back_kernel(
    feed_p, g3_p, wqkv, dn_h, mid_h, cot_h, resid_h, ga_h, n1_h, q_h, kv_h, ctx_h, wo_h, cos_h,
    sin_h, mask_h,
    feed_out, grad_out, g3, gq_out, go_out, gains_out,
    dn, mid, cot, resid, ga, n1, q, kv, ctx, wo, cos_t, sin_t, mask, grad_in, fown, yin, zin, gbuf, cin, xin, gq_p, go_p, gp, qc, qx, qz, oc, ox, oz, gc, gx, gz,
    feed, mid_b, dctx, dqkv, dn1, dn1_o, kx, vx, kacc, vacc, wbuf, gs, gr, ss, rs, ls,
):
    z, x, c, y = place()
    units = g3_p.shape[1]
    seq, width = mid.shape
    half = width // 2
    q_width = q.shape[1]
    pairs = q_width // LANE
    out_rows = wo.shape[0]
    wire = Wire(ss, rs)
    side, twin, other = dev(z, 1 - x, c, y), dev(z, x, 1 - c, y), dev(z, x, c, 1 - y)
    ring = [(z + d) % ZN for d in (2, 1, 3, 0)]
    greet(all_peers(z, x, c, y))

    def y_out(src, k, steps):
        for t in steps:
            todo = ((z + t, z + t < ZN), (z - t, z >= t)) if t else ((z, None),)
            for o, cond in todo:
                part = src.at[rows(o, seq), lanes(1 - y, half)]
                wire.send(part, yin.at[o], k * 4 + o, k * 4 + o, other, cond)

    def own_half(o):
        return pltpu.make_async_copy(
            feed_p.at[rows(o, seq), lanes(y, half)], fown.at[o], ls.at[3 + o]
        )

    wire.send(dn_h, dn.at[:, lanes(y, half)], 24, 18, other)
    for k in range(8):
        wire.send(g3_p.at[:, :, lanes(k * 2 + 1 - c)], cin.at[k], 26 + k, 20 + k, twin)
    ks = [o * 2 + 1 - x for o in ring] + [o * 2 + x for o in ring]

    def load(i):
        return pltpu.make_async_copy(
            g3_p.at[:, :, lanes(ks[i] * 2 + c)], gbuf.at[i % 2], ls.at[i % 2]
        )

    def add3(dst, src):
        for m in range(3):
            add_into(dst.at[m], src.at[m], units, 64)


    def ffn_add(i):
        if i < 7:
            load(i + 1).start()
        load(i).wait()
        wire.arrived(cin.at[ks[i]], 20 + ks[i], twin)
        add3(cin.at[ks[i]], gbuf.at[i % 2])
        if i < 4:
            o = ring[i]
            wire.send(cin.at[ks[i]], xin.at[o], 34 + o, 28 + o, side)

    load(0).start()
    pairs_in = (
        (dn_h, dn.at[:, lanes(y, half)]), (mid_h, mid), (cot_h, cot), (wo_h, wo), (ga_h, ga), (kv_h, kv), (mask_h, mask), (n1_h, n1),
        (q_h, q), (ctx_h, ctx), (cos_h, cos_t), (sin_h, sin_t), (resid_h, resid),
    )
    inward = [
        pltpu.make_async_copy(a, b, ls.at[13 + i]) for i, (a, b) in enumerate(pairs_in)
    ]
    for cp in inward:
        cp.start()
    for o in range(ZN):
        own_half(o).start()

    line = Chain(wire, lambda o: yin.at[o], lambda k: zin.at[k], seq, 16, 8, 8)

    def ffn_z(i):
        o = ring[i]
        wire.arrived(xin.at[o], 28 + o, side)
        add3(xin.at[o], cin.at[o * 2 + x])
        d = (2, 1, 3, 0)[i]
        if d:
            wire.send(xin.at[o], g3.at[:, rows(z, units), :], 38 + d - 1, 32 + z, dev(o, x, c, y))
        else:
            pltpu.make_async_copy(xin.at[o], g3.at[:, rows(z, units), :], ls.at[10]).start()

    y_out(feed_p, 1, (3, 2, 1, 0))
    for i in range(8):
        ffn_add(i)
    for cp in inward:
        cp.wait()
    spread_pair(kx, kv[:, pl.ds(0, LANE)].astype(F32))
    spread_pair(vx, kv[:, pl.ds(LANE, LANE)].astype(F32))
    kacc[...] = jnp.zeros_like(kacc)
    vacc[...] = jnp.zeros_like(vacc)
    gp[...] = jnp.zeros_like(gp)
    gain_one = ga[pl.ds(0, 8), :].astype(F32)[0:1]
    gain_two = ga[pl.ds(0, 8), :].astype(F32)[1:2]

    def norm_two(r):
        v, g = mid[r, :], dn[r, :].astype(F32)
        recip = lax.rsqrt(jnp.mean(v * v, axis=-1, keepdims=True) + epsilon)
        e = g * gain_two
        d = recip * e - v * (recip * recip * recip) * jnp.mean(e * v, axis=-1, keepdims=True)
        out = cot[r, :] + d
        grad_in[r, :] = out
        mid_b[r, :] = out.astype(BF)
        t = g * v * recip
        gp[pl.ds(8, 8), :] += t[:8] + t[8:]

    wire.arrived(dn.at[:, lanes(1 - y, half)], 18, other)
    by_rows(seq, 16, norm_two)

    def out_grad(i, carry):
        cut = lanes(i, 2 * LANE)
        for h in range(2):
            hh = pl.ds(h * (out_rows // 2), out_rows // 2)
            go_p[hh, cut] = dot_tn(ctx[:, hh], mid_b[:, cut]).astype(BF)
        return carry

    lax.fori_loop(0, width // (2 * LANE), out_grad, 0)
    f_o = Fold(wire, lambda r: go_p.at[:, lanes(r)], oc, ox, oz, out_rows, 64, 61, 53)
    f_q = Fold(
        wire,
        lambda r: gq_p.at[pl.ds(pl.multiple_of(r * LANE, LANE), LANE), :],
        qc, qx, qz, LANE, 16, 41, 36,
    )
    f_g = Fold(wire, lambda r: gp.at[:, lanes(r)], gc, gx, gz, 16, 16, 81, 70)
    f_o.to_twin()

    def ctx_grad(j, carry):
        cut = lanes(j, 2 * LANE)
        dctx[:, cut] = dot_nt(mid_b[...], wo[cut, :]).astype(BF)
        return carry

    lax.fori_loop(0, q_width // (2 * LANE), ctx_grad, 0)
    ffn_z(0)
    f_o.across()

    def back_turned(v):
        return v * cos_t[...] - swap_halves(v) * sin_t[...]

    def pair(p, carry):
        qp, dc = q[:, lanes(p)], dctx[:, lanes(p)]
        g = p // (pairs // 2)
        prod = dc.astype(F32) * ctx[:, lanes(p)].astype(F32)
        low = lax.broadcasted_iota(jnp.int32, prod.shape, 1) < HD
        dq = jnp.zeros((seq, LANE), F32)
        for h in (0, 1):
            i = 2 * g + h
            s = dot_nt(qp, kx[i]) * HD ** (-0.5)
            s = jnp.where(mask[...] > 0.0, s, masked_score)
            top = jnp.max(s, axis=-1, keepdims=True)
            lse = top + jnp.log(jnp.sum(jnp.exp(s - top), axis=-1, keepdims=True))
            full = jnp.exp(s - lse)
            delta = jnp.sum(jnp.where(low if h == 0 else ~low, prod, 0.0), axis=-1, keepdims=True)
            ds = (full * (dot_nt(dc, vx[i]) - delta)).astype(BF)
            dq = dq + dot_nn(ds, kx[i])
            kacc[i] += dot_tn(ds, qp)
            vacc[i] += dot_tn(full.astype(BF), dc)
        dqkv[:, lanes(p)] = back_turned(dq * HD ** (-0.5)).astype(BF)
        return carry

    lax.fori_loop(0, pairs // 2, pair, 0)
    ffn_z(1)
    lax.fori_loop(pairs // 2, pairs, pair, 0)

    def joined(acc):
        low = lax.broadcasted_iota(jnp.int32, (seq, LANE), 1) < HD
        return jnp.where(
            low, acc[0] + pltpu.roll(acc[1], HD, 1), acc[3] + pltpu.roll(acc[2], HD, 1)
        )

    dqkv[:, pl.ds(q_width, LANE)] = back_turned(joined(kacc) * HD ** (-0.5)).astype(BF)
    dqkv[:, pl.ds(q_width + LANE, LANE)] = joined(vacc).astype(BF)

    def w_tile(j, slot):
        r = pl.ds(pl.multiple_of(j * 2 * LANE, 2 * LANE), 2 * LANE)
        return pltpu.make_async_copy(wqkv.at[r, :], wbuf.at[slot], ls.at[11 + slot])

    w_tile(0, 0).start()

    def in_grad(r, carry):
        gq_p[pl.ds(pl.multiple_of(r * LANE, LANE), LANE), :] = dot_tn(
            n1[:, lanes(r)], dqkv[...]
        ).astype(BF)
        return carry

    lax.fori_loop(0, width // LANE, in_grad, 0)
    f_q.to_twin()
    f_q.across()
    ffn_z(2)
    tiles = width // (2 * LANE)
    for j in range(tiles):
        if j + 1 < tiles:
            w_tile(j + 1, (j + 1) % 2).start()
        w_tile(j, j % 2).wait()
        dn1[:, pl.ds(j * 2 * LANE, 2 * LANE)] = dot_nt(dqkv[...], wbuf[j % 2]).astype(BF)
    wire.send(dn1, dn1_o, 101, 87, other)

    def gain_part(r):
        v = resid[r, :]
        recip = lax.rsqrt(jnp.mean(v * v, axis=-1, keepdims=True) + epsilon)
        t = dn1[r, :].astype(F32) * v * recip
        gp[pl.ds(0, 8), :] += t[:8] + t[8:]

    by_rows(seq, 16, gain_part)
    f_g.to_twin()
    f_g.across()
    ffn_z(3)
    f_o.stay()
    for t in (3, 2, 1):
        f_o.outward(t)

    for o in range(ZN):
        own_half(o).wait()

    def feed_ready(o, cond):
        wire.arrived(yin.at[o], 4 + o, other, cond)

        @pl.when(cond)
        def _():
            add_into(yin.at[o], fown.at[o], seq, 16)

    for t in (3, 2, 1):
        line.outward(t, feed_ready)
    f_q.stay()
    f_g.stay()
    for t in (3, 2, 1):
        f_q.outward(t)
        f_g.outward(t)
    feed_ready(z, z >= 0)
    line.home()
    fb = feed.at[:, lanes(y, half)]

    def keep_feed(r):
        feed[r, lanes(y, half)] = yin[z, r, :]

    by_rows(seq, 16, keep_feed)
    wire.send(fb, fb, 25, 19, other)
    wire.arrived(dn1_o, 87, other)

    def norm_one(r):
        v = resid[r, :]
        g = dn1[r, :].astype(F32) + dn1_o[r, :].astype(F32)
        recip = lax.rsqrt(jnp.mean(v * v, axis=-1, keepdims=True) + epsilon)
        e = g * gain_one
        d = recip * e - v * (recip * recip * recip) * jnp.mean(e * v, axis=-1, keepdims=True)
        grad_in[r, :] += d

    by_rows(seq, 16, norm_one)
    outward = [pltpu.make_async_copy(grad_in, grad_out, ls.at[26])]
    outward[0].start()
    done = f_o.home()
    outward.append(pltpu.make_async_copy(done, go_out, ls.at[27]))
    outward[1].start()
    mine = f_g.home()
    gs[...] = mine[...]
    wire.send(gs, gr, 102, 88, other)
    got = f_q.home()
    outward.append(pltpu.make_async_copy(got, gq_out, ls.at[28]))
    outward[2].start()
    wire.arrived(feed.at[:, lanes(1 - y, half)], 19, other)
    outward.append(pltpu.make_async_copy(feed, feed_out, ls.at[29]))
    outward[3].start()
    wire.arrived(gr, 88, other)
    first = jnp.sum(gs[pl.ds(0, 8), :] + gr[pl.ds(0, 8), :], axis=0, keepdims=True)
    second = jnp.sum(gs[pl.ds(8, 8), :], axis=0, keepdims=True)
    row = lax.broadcasted_iota(jnp.int32, (8, LANE), 0)
    gains_out[...] = jnp.where(row == 0, first, second)
    for d in (1, 2, 3):
        o = (z + ZN - d) % ZN
        wire.arrived(g3.at[:, rows(o, units), :], 32 + o, dev(o, x, c, y))
    wire.drain()
    pltpu.make_async_copy(xin.at[z], g3.at[:, rows(z, units), :], ls.at[10]).wait()
    for cp in outward:
        cp.wait()


def back(feed_p, g3_p, wqkv, dn, mid, cot, resid, ga, n1, q, kv, ctx, wo, cos_t, sin_t, mask):
    seq, width = mid.shape
    units = g3_p.shape[1]
    q_width, total = q.shape[1], wqkv.shape[1]
    out_rows = wo.shape[0]
    half = width // 2

    def vm(*shape, dtype=BF):
        return pltpu.VMEM(shape, dtype)

    held = (dn, mid, cot, resid, ga, n1, q, kv, ctx, wo, cos_t, sin_t, mask)
    return pl.pallas_call(
        back_kernel,
        name="back",
        out_shape=(
            jax.ShapeDtypeStruct((seq, width), BF),
            jax.ShapeDtypeStruct((seq, width), F32),
            jax.ShapeDtypeStruct((3, units * ZN, LANE), BF),
            jax.ShapeDtypeStruct((LANE, total), BF),
            jax.ShapeDtypeStruct((out_rows, LANE), BF),
            jax.ShapeDtypeStruct((8, LANE), F32),
        ),
        in_specs=[any_spec()] * 16,
        out_specs=[any_spec()] * 5 + [vm_spec()],
        scratch_shapes=[vm(seq, width)]
        + [vm(*a.shape, dtype=a.dtype) for a in held[1:]]
        + [
            vm(seq, width, dtype=F32),
            vm(ZN, seq, half),
            vm(ZN, seq, half),
            vm(5, seq, half),
            vm(2, 3, units, LANE),
            vm(8, 3, units, LANE),
            vm(4, 3, units, LANE),
            vm(width, total),
            vm(out_rows, width),
            vm(16, width, dtype=F32),
            vm(8, LANE, total),
            vm(4, LANE, total),
            vm(5, LANE, total),
            vm(8, out_rows, LANE),
            vm(4, out_rows, LANE),
            vm(5, out_rows, LANE),
            vm(8, 16, LANE, dtype=F32),
            vm(4, 16, LANE, dtype=F32),
            vm(5, 16, LANE, dtype=F32),
            vm(seq, width),
            vm(seq, width),
            vm(seq, q_width),
            vm(seq, total),
            vm(seq, width),
            vm(seq, width),
            vm(4, seq, LANE),
            vm(4, seq, LANE),
            vm(4, seq, LANE, dtype=F32),
            vm(4, seq, LANE, dtype=F32),
            vm(2, 2 * LANE, total),
            vm(16, LANE, dtype=F32),
            vm(16, LANE, dtype=F32),
            sems(103),
            sems(89),
            sems(30),
        ],
        compiler_params=pltpu.CompilerParams(
            collective_id=1, has_side_effects=True, vmem_limit_bytes=67043328
        ),
    )(feed_p, g3_p, wqkv, *held)


def finish_kernel(
    mid_h, feed_h, grad_h, g3_h, gq_h, go_h, gains,
    hidden, grad_in, wg, wu, wd, wq, wk, wv, wo, first, second,
    mid, feed, grad, g3, gq, go, tg, td, tq, to, ls,
):
    q_width = wq.shape[2]
    units = td.shape[0]
    into = [
        pltpu.make_async_copy(a, b, ls.at[i])
        for i, (a, b) in enumerate(
            ((g3_h, g3), (mid_h, mid), (feed_h, feed), (gq_h, gq), (go_h, go), (grad_h, grad))
        )
    ]
    for cp in into:
        cp.start()
    first[...] = gains[pl.ds(0, 1), :]
    second[...] = gains[pl.ds(1, 1), :]
    out = []

    def put(src, dst):
        cp = pltpu.make_async_copy(src, dst, ls.at[6 + len(out)])
        cp.start()
        out.append(cp)

    into[0].wait()
    for m, dst in ((0, wg), (1, wu)):

        def turn(i, carry):
            r = pl.ds(pl.multiple_of(i * LANE, LANE), LANE)
            tg[m, :, lanes(i)] = g3[m, r, :].astype(F32).T
            return carry

        lax.fori_loop(0, units // LANE, turn, 0)
        put(tg.at[m], dst.at[0])

    def wide(r):
        td[r, :] = g3[2, r, :].astype(F32)

    by_rows(units, 64, wide)
    put(td, wd.at[0])
    into[1].wait()
    into[2].wait()

    def total(r):
        mid[r, :] += feed[r, :].astype(F32)

    by_rows(mid.shape[0], 16, total)
    put(mid, hidden)
    into[3].wait()

    def wide_q(r):
        tq[r, :] = gq[r, :].astype(F32)

    by_rows(LANE, 16, wide_q)
    put(tq.at[:, pl.ds(0, q_width)], wq.at[0])
    put(tq.at[:, pl.ds(q_width, LANE)], wk.at[0])
    put(tq.at[:, pl.ds(q_width + LANE, LANE)], wv.at[0])
    into[4].wait()

    def wide_o(r):
        to[r, :] = go[r, :].astype(F32)

    by_rows(to.shape[0], 64, wide_o)
    put(to, wo.at[0])
    into[5].wait()
    put(grad, grad_in)
    for cp in out:
        cp.wait()


def finish(mid, feed, grad, g3, gq, go, gains):
    seq, width = mid.shape
    units = g3.shape[1]
    q_width = gq.shape[1] - 2 * LANE
    f32 = lambda *shape: jax.ShapeDtypeStruct(shape, F32)
    ins = (mid, feed, grad, g3, gq, go)
    return pl.pallas_call(
        finish_kernel,
        name="finish",
        out_shape=(
            f32(seq, width),
            f32(seq, width),
            f32(1, LANE, units),
            f32(1, LANE, units),
            f32(1, units, LANE),
            f32(1, LANE, q_width),
            f32(1, LANE, LANE),
            f32(1, LANE, LANE),
            f32(1, go.shape[0], LANE),
            f32(1, LANE),
            f32(1, LANE),
        ),
        in_specs=[any_spec()] * 6 + [vm_spec()],
        out_specs=[any_spec()] * 9 + [vm_spec()] * 2,
        scratch_shapes=[pltpu.VMEM(a.shape, a.dtype) for a in ins]
        + [
            pltpu.VMEM((2, LANE, units), F32),
            pltpu.VMEM((units, LANE), F32),
            pltpu.VMEM(gq.shape, F32),
            pltpu.VMEM(go.shape, F32),
            sems(15),
        ],
        compiler_params=pltpu.CompilerParams(vmem_limit_bytes=67043328),
    )(*ins, gains)


def fast_body(
    hidden_in,
    segment_ids,
    gain_attn,
    w_query,
    w_key,
    w_value,
    w_out,
    gain_ffn,
    w_gate,
    w_up,
    w_down,
    cotangent,
):
    resid = hidden_in
    wqkv, wo, ga, n1, q, kv, ctx, middle, cos_w, sin_w, mask, dn, feed_p, g3_p = front(
        resid, w_query, w_key, w_value, w_out, gain_attn, gain_ffn, w_gate, w_up, w_down,
        cotangent, segment_ids,
    )
    feed, grad_b, g3, gq, go, gains_g = back(
        feed_p, g3_p, wqkv, dn, middle, cotangent, resid, ga, n1, q, kv, ctx, wo,
        cos_w, sin_w, mask,
    )
    hidden_out, grad_input, wg, wu, wd, wq, wk, wv, wo_g, first, second = finish(
        middle, feed, grad_b, g3, gq, go, gains_g
    )
    return (
        hidden_out,
        grad_input,
        first,
        wq,
        wk,
        wv,
        wo_g,
        second,
        wg,
        wu,
        wd,
    )


def solution(mesh):
    small = mesh.shape["dp"] == 16 and mesh.shape["tensor"] == 2
    chosen = fast_body if small else body
    return jax.shard_map(
        chosen,
        mesh=mesh,
        in_specs=(
            P("dp", None),
            P("dp", None),
            P(None, "dp"),
            P(None, "dp", "tensor"),
            P(None, "dp", "tensor"),
            P(None, "dp", "tensor"),
            P(None, "tensor", "dp"),
            P(None, "dp"),
            P(None, "dp", "tensor"),
            P(None, "dp", "tensor"),
            P(None, "tensor", "dp"),
            P("dp", None),
        ),
        out_specs=(
            P("dp", None),
            P("dp", None),
            P(None, "dp"),
            P(None, "dp", "tensor"),
            P(None, "dp", "tensor"),
            P(None, "dp", "tensor"),
            P(None, "tensor", "dp"),
            P(None, "dp"),
            P(None, "dp", "tensor"),
            P(None, "dp", "tensor"),
            P(None, "tensor", "dp"),
        ),
        check_vma=False,
    )
```
